128 devices in a mesh: pod: 1, dp: 16 (over z, y), tp: 8 (over x, core).
Axes of the slice: x: 4, y: 4, z: 4, core: 2. Of those that a mesh axis runs over, the one named last changes fastest.
Arguments:
- x_in: bfloat16 [128, 512, 1536], P(('pod', 'dp'))
- seg_ids: int32 [128, 512], P(('pod', 'dp'))
- gain_one: bfloat16 [1536], replicated
- gain_two: bfloat16 [1536], replicated
- w_qkv: bfloat16 [1536, 4608], P(None, 'tp')
- w_out: bfloat16 [16, 96, 1536], P('tp')
- w_up: bfloat16 [1536, 6144], P(None, 'tp')
- w_down: bfloat16 [6144, 1536], P('tp')
- grad_y: bfloat16 [128, 512, 1536], P(('pod', 'dp'))
Outputs:
- output 1: bfloat16 [128, 512, 1536], P(('pod', 'dp'))
- output 2: bfloat16 [128, 512, 1536], P(('pod', 'dp'))
- output 3: bfloat16 [1536], P('pod')
- output 4: bfloat16 [1536], P('pod')
- output 5: bfloat16 [1536, 4608], P('pod', 'tp')
- output 6: bfloat16 [16, 96, 1536], P(('pod', 'tp'))
- output 7: bfloat16 [1536, 6144], P('pod', 'tp')
- output 8: bfloat16 [6144, 1536], P(('pod', 'tp'))
All inputs are finite; a program needn't handle non-finite values.
Results may differ from the reference program's by a relative error of at most 0.02.
Values are sent between devices in bfloat16 or wider.
A program may use at most 1 GiB of HBM per device.

```python
import functools
import jax
import jax.numpy as jnp
from jax import lax

BATCH_ROWS = 128
SEQ_LEN = 512
HIDDEN_DIM = 1536
NUM_HEADS = 16
HEAD_DIM = 96
FFN_DIM = 6144
EPS_NORM = 1e-5


def setup_inputs(seed: int = 0, part: int = 0) -> dict:
    own_key = jax.random.fold_in(jax.random.key(seed), part)
    own_keys = jax.random.split(own_key, 3)
    shared_keys = jax.random.split(jax.random.key(seed + 1), 5)
    x_in = jax.random.normal(own_keys[0], (BATCH_ROWS, SEQ_LEN, HIDDEN_DIM), jnp.float32)
    cut_points = jax.random.randint(own_keys[1], (BATCH_ROWS, 3), 1, SEQ_LEN)
    positions = jnp.arange(SEQ_LEN)
    seg_ids = jnp.sum((positions[None, :, None] >= cut_points[:, None, :]).astype(jnp.int32), axis=-1)
    grad_y = jax.random.normal(own_keys[2], (BATCH_ROWS, SEQ_LEN, HIDDEN_DIM), jnp.float32)
    gain_pair = 1.0 + 0.3 * jax.random.normal(shared_keys[0], (2, HIDDEN_DIM), jnp.float32)
    qk_boost = jnp.array([1.5, 1.5, 1.0], jnp.float32)[None, None, :, None]
    w_qkv = jax.random.normal(shared_keys[1], (HIDDEN_DIM, NUM_HEADS, 3, HEAD_DIM), jnp.float32) * qk_boost * HIDDEN_DIM ** -0.5
    w_out = jax.random.normal(shared_keys[2], (NUM_HEADS, HEAD_DIM, HIDDEN_DIM), jnp.float32) * (2.0 * (NUM_HEADS * HEAD_DIM) ** -0.5)
    w_up = jax.random.normal(shared_keys[3], (HIDDEN_DIM, FFN_DIM), jnp.float32) * HIDDEN_DIM ** -0.5
    w_down = jax.random.normal(shared_keys[4], (FFN_DIM, HIDDEN_DIM), jnp.float32) * FFN_DIM ** -0.5
    return {
        "x_in": x_in.astype(jnp.bfloat16),
        "seg_ids": seg_ids,
        "gain_one": gain_pair[0].astype(jnp.bfloat16),
        "gain_two": gain_pair[1].astype(jnp.bfloat16),
        "w_qkv": w_qkv.reshape(HIDDEN_DIM, 3 * NUM_HEADS * HEAD_DIM).astype(jnp.bfloat16),
        "w_out": w_out.astype(jnp.bfloat16),
        "w_up": w_up.astype(jnp.bfloat16),
        "w_down": w_down.astype(jnp.bfloat16),
        "grad_y": grad_y.astype(jnp.bfloat16),
    }


def layer_norm(x_rows, gain_vec):
    x_f32 = x_rows.astype(jnp.float32)
    centered = x_f32 - jnp.mean(x_f32, axis=-1, keepdims=True)
    variance = jnp.mean(centered * centered, axis=-1, keepdims=True)
    return (centered * lax.rsqrt(variance + EPS_NORM) * gain_vec.astype(jnp.float32)).astype(jnp.bfloat16)


def head_attention(qkv_item, seg_row):
    scores = jnp.dot(qkv_item[0], qkv_item[1].T, preferred_element_type=jnp.float32) * (HEAD_DIM ** -0.5)
    positions = jnp.arange(SEQ_LEN)
    allowed = (positions[:, None] >= positions[None, :]) & (seg_row[:, None] == seg_row[None, :])
    attn_probs = jax.nn.softmax(jnp.where(allowed, scores, -1e30), axis=-1)
    return jnp.dot(attn_probs.astype(jnp.bfloat16), qkv_item[2], preferred_element_type=jnp.float32).astype(jnp.bfloat16)


def layer_forward(seg_ids, x_in, gain_one, gain_two, w_qkv, w_out, w_up, w_down):
    tokens = BATCH_ROWS * SEQ_LEN
    x_rows = x_in.reshape(tokens, HIDDEN_DIM)
    normed_a = layer_norm(x_rows, gain_one)
    qkv_rows = jnp.dot(normed_a, w_qkv, preferred_element_type=jnp.float32).astype(jnp.bfloat16)
    qkv_rows = qkv_rows.reshape(BATCH_ROWS, SEQ_LEN, NUM_HEADS, 3, HEAD_DIM)
    qkv_rows = jnp.transpose(qkv_rows, (0, 2, 3, 1, 4)).reshape(BATCH_ROWS * NUM_HEADS, 3, SEQ_LEN, HEAD_DIM)
    seg_rep = jnp.repeat(seg_ids, NUM_HEADS, axis=0)
    attn_out = lax.map(lambda map_item: jax.checkpoint(head_attention)(map_item[0], map_item[1]), (qkv_rows, seg_rep))
    attn_out = jnp.transpose(attn_out.reshape(BATCH_ROWS, NUM_HEADS, SEQ_LEN, HEAD_DIM), (0, 2, 1, 3)).reshape(tokens, NUM_HEADS * HEAD_DIM)
    part_one = jnp.dot(attn_out, w_out.reshape(NUM_HEADS * HEAD_DIM, HIDDEN_DIM), preferred_element_type=jnp.float32).astype(jnp.bfloat16)
    x_one = (x_rows.astype(jnp.float32) + part_one.astype(jnp.float32)).astype(jnp.bfloat16)
    normed_b = layer_norm(x_one, gain_two)
    pre_act = jnp.dot(normed_b, w_up, preferred_element_type=jnp.float32)
    hidden_act = jax.nn.gelu(pre_act, approximate=True).astype(jnp.bfloat16)
    part_two = jnp.dot(hidden_act, w_down, preferred_element_type=jnp.float32).astype(jnp.bfloat16)
    y_rows = (x_one.astype(jnp.float32) + part_two.astype(jnp.float32)).astype(jnp.bfloat16)
    return y_rows.reshape(BATCH_ROWS, SEQ_LEN, HIDDEN_DIM)


def reference(x_in, seg_ids, gain_one, gain_two, w_qkv, w_out, w_up, w_down, grad_y):
    y_out, pullback = jax.vjp(functools.partial(layer_forward, seg_ids), x_in, gain_one, gain_two, w_qkv, w_out, w_up, w_down)
    grad_list = pullback(grad_y)
    return (y_out, grad_list[0], grad_list[1], grad_list[2], grad_list[3], grad_list[4], grad_list[5], grad_list[6])
```

```python
import jax
import jax.numpy as jnp
from jax import lax
from jax.experimental import pallas as pl
from jax.experimental.pallas import tpu as pltpu
from jax.sharding import PartitionSpec as P

EPS_NORM = 1e-5
NEG_LARGE = -1e30
F32 = jnp.float32
BF16 = jnp.bfloat16
RING = 4


def gelu_tanh(values):
    return jax.nn.gelu(values, approximate=True)


def norm_forward(x_rows, gain_vec):
    x_f32 = x_rows.astype(F32)
    centered = x_f32 - jnp.mean(x_f32, axis=-1, keepdims=True)
    inv_std = lax.rsqrt(jnp.mean(centered * centered, axis=-1, keepdims=True) + EPS_NORM)
    x_hat = centered * inv_std
    return (x_hat * gain_vec.astype(F32)).astype(BF16), x_hat, inv_std


def norm_backward(grad_out, x_hat, inv_std, gain_vec):
    grad_f32 = grad_out.astype(F32)
    grad_gain = jnp.sum(grad_f32 * x_hat, axis=0)
    grad_hat = grad_f32 * gain_vec.astype(F32)
    mean_one = jnp.mean(grad_hat, axis=-1, keepdims=True)
    mean_two = jnp.mean(grad_hat * x_hat, axis=-1, keepdims=True)
    return inv_std * (grad_hat - mean_one - x_hat * mean_two), grad_gain


def dot_nt(lhs, rhs):
    return lax.dot_general(lhs, rhs, (((lhs.ndim - 1,), (rhs.ndim - 1,)), ((), ())), preferred_element_type=F32)


def dot_tn(lhs, rhs):
    return lax.dot_general(lhs, rhs, (((0,), (0,)), ((), ())), preferred_element_type=F32)


def dot_nn(lhs, rhs):
    return lax.dot_general(lhs, rhs, (((lhs.ndim - 1,), (0,)), ((), ())), preferred_element_type=F32)


def core_swap(array):
    return lax.ppermute(array, "tp", [(i, i ^ 1) for i in range(8)])


THIRD = 512
PIECE = 48
WIDTH = 1536
HALF = WIDTH // 2
MESH_ID = pl.DeviceIdType.MESH


class Place:
    def __init__(self):
        plane = lax.axis_index("dp")
        column = lax.axis_index("tp")
        self.pos = {"z": lax.div(plane, RING), "y": lax.rem(plane, RING), "x": lax.div(column, 2)}
        self.core = lax.rem(column, 2)

    def ahead(self, axis, step):
        return lax.rem(self.pos[axis] + step, RING)

    def peer(self, axis, step):
        if axis == "x":
            return {"tp": self.ahead("x", step) * 2 + self.core}
        if axis == "y":
            return {"dp": self.pos["z"] * RING + self.ahead("y", step)}
        return {"dp": self.ahead("z", step) * RING + self.pos["y"]}

    def block(self, axis, step):
        return step if axis == "x" else self.ahead(axis, step)

    def enter(self):
        barrier = pltpu.get_barrier_semaphore()
        for axis in "xyz":
            for step in range(1, RING):
                pl.semaphore_signal(barrier, inc=1, device_id=self.peer(axis, step), device_id_type=MESH_ID)
        pl.semaphore_wait(barrier, 9)


class Sender:
    def __init__(self, place, send_sems, recv_sems):
        self.place, self.send_sems, self.recv_sems = place, send_sems, recv_sems
        self.used = 0
        self.copies = []

    def ring(self, axis, source, target):
        started = []
        for step in range(1, RING):
            copy = pltpu.make_async_remote_copy(
                src_ref=source(step), dst_ref=target(step),
                send_sem=self.send_sems.at[self.used], recv_sem=self.recv_sems.at[self.used],
                device_id=self.place.peer(axis, step), device_id_type=MESH_ID,
            )
            copy.start()
            self.used += 1
            started.append(copy)
        self.copies += started
        return started

    def drain(self):
        for copy in self.copies:
            copy.wait_send()


def wait_all(copies):
    for copy in copies:
        copy.wait_recv()


class WeightGather:
    COPIES = 21

    def __init__(self, place, sender, own, out):
        self.place, self.sender, self.own, self.out = place, sender, own, out

    def spot(self, cols):
        z, y = self.place.pos["z"], self.place.pos["y"]
        return lambda step: self.out.at[pl.ds(1, 3), z, y, :, cols]

    def start(self):
        z, y = self.place.pos["z"], self.place.pos["y"]
        self.near = []
        for part in range(2):
            cols = pl.ds(part * THIRD, THIRD)
            self.near.append(self.sender.ring(
                "x", lambda step: self.own.at[z, y, :, cols], lambda step: self.out.at[RING - step, z, y, :, cols]))
        cols = pl.ds(2 * THIRD, THIRD)
        self.whole = self.sender.ring(
            "x", lambda step: self.own.at[:, :, :, cols], lambda step: self.out.at[RING - step, :, :, :, cols])

    def second(self):
        self.mid = []
        for part, axis in enumerate("yz"):
            wait_all(self.near[part])
            spot = self.spot(pl.ds(part * THIRD, THIRD))
            self.mid.append(self.sender.ring(axis, spot, spot))

    def third(self):
        z, y = self.place.pos["z"], self.place.pos["y"]
        wait_all(self.mid[0])
        line = lambda step: self.out.at[pl.ds(1, 3), z, :, :, pl.ds(0, THIRD)]
        self.far = self.sender.ring("z", line, line)
        wait_all(self.mid[1])
        row = lambda step: self.out.at[pl.ds(1, 3), :, y, :, pl.ds(THIRD, THIRD)]
        self.far += self.sender.ring("y", row, row)

    def finish(self):
        wait_all(self.far)
        wait_all(self.whole)


def gather_kernel(count, *refs):
    owns, outs = refs[:count], refs[count : 2 * count]
    stage, send_sems, recv_sems, local_sems = refs[2 * count :]
    place = Place()
    sender = Sender(place, send_sems, recv_sems)
    gathers = [WeightGather(place, sender, own, out) for own, out in zip(owns, outs)]
    loads = [pltpu.make_async_copy(own, stage.at[i], local_sems.at[i]) for i, own in enumerate(owns)]
    for load in loads:
        load.start()
    place.enter()
    for gather in gathers:
        gather.start()
    stores = []
    for i in range(count):
        loads[i].wait()
        store = pltpu.make_async_copy(stage.at[i], outs[i].at[0], local_sems.at[count + i])
        store.start()
        stores.append(store)
    for gather in gathers:
        gather.second()
    for gather in gathers:
        gather.third()
    for gather in gathers:
        gather.finish()
    for store in stores:
        store.wait()
    sender.drain()


def gather_weights(owns, collective_id):
    count = len(owns)
    copies = WeightGather.COPIES * count
    return pl.pallas_call(
        lambda *refs: gather_kernel(count, *refs),
        out_shape=[jax.ShapeDtypeStruct((RING,) + own.shape, own.dtype) for own in owns],
        in_specs=[pl.BlockSpec(memory_space=pl.ANY)] * count,
        out_specs=[pl.BlockSpec(memory_space=pl.ANY)] * count,
        scratch_shapes=[
            pltpu.VMEM((count,) + owns[0].shape, owns[0].dtype),
            pltpu.SemaphoreType.DMA((copies,)),
            pltpu.SemaphoreType.DMA((copies,)),
            pltpu.SemaphoreType.DMA((2 * count,)),
        ],
        compiler_params=pltpu.CompilerParams(collective_id=collective_id, has_side_effects=True),
        name=f"gather_weights_{collective_id}",
    )(*owns)


ORDERS = (("z", "y", "x", 1), ("y", "x", "z", 0), ("x", "z", "y", 0))


class GradScatter:
    COPIES = 27

    def __init__(self, place, sender, grads, mine, first, second, third, final, local_sems):
        self.place, self.sender, self.grads = place, sender, grads
        self.mine, self.bufs, self.final, self.local_sems = mine, (first, second, third), final, local_sems

    def cut(self, part, step):
        axis = ORDERS[part][0]
        index = self.place.block(axis, step)
        cols = pl.ds(part * THIRD, THIRD)
        if axis == "x":
            return self.grads.at[index, :, :, :, cols]
        if axis == "z":
            return self.grads.at[:, index, :, :, cols]
        return self.grads.at[:, :, index, :, cols]

    def start(self):
        self.loads, self.one, self.two, self.three = [], [], [None] * 3, [None] * 3
        for part in range(3):
            self.one.append(self.sender.ring(
                ORDERS[part][0], lambda step: self.cut(part, step), lambda step: self.bufs[0].at[part, step - 1]))
        for part in range(3):
            load = pltpu.make_async_copy(self.cut(part, 0), self.mine.at[part], self.local_sems.at[part])
            load.start()
            self.loads.append(load)

    def second(self, part):
        self.loads[part].wait()
        wait_all(self.one[part])

        @pl.loop(0, RING)
        def _(a):
            for b in range(RING):
                total = self.mine[part, a, b].astype(F32)
                for k in range(3):
                    total = total + self.bufs[0][part, k, a, b].astype(F32)
                self.mine[part, a, b] = total.astype(BF16)

        axis, spot = ORDERS[part][1], ORDERS[part][3]

        def source(step):
            index = self.place.block(axis, step)
            return self.mine.at[part, :, index] if spot else self.mine.at[part, index]

        self.two[part] = self.sender.ring(axis, source, lambda step: self.bufs[1].at[part, step - 1])

    def third(self, part):
        wait_all(self.two[part])
        axis, spot = ORDERS[part][1], ORDERS[part][3]
        own = self.place.block(axis, 0)
        for other in range(RING):
            at = (part, other, own) if spot else (part, own, other)
            total = self.mine[at].astype(F32)
            for k in range(3):
                total = total + self.bufs[1][part, k, other].astype(F32)
            self.bufs[1][part, 3, other] = total.astype(BF16)
        axis = ORDERS[part][2]
        self.three[part] = self.sender.ring(
            axis, lambda step: self.bufs[1].at[part, 3, self.place.block(axis, step)], lambda step: self.bufs[2].at[part, step - 1])

    def finish(self, part):
        wait_all(self.three[part])
        own = self.place.block(ORDERS[part][2], 0)
        total = self.bufs[1][part, 3, own].astype(F32)
        for k in range(3):
            total = total + self.bufs[2][part, k].astype(F32)
        self.final[:, part * THIRD : (part + 1) * THIRD] = total.astype(BF16)


class PlaneGather:
    COPIES = 12

    def __init__(self, place, sender, final, out, local_sem):
        self.place, self.sender, self.final, self.out, self.local_sem = place, sender, final, out, local_sem

    def start(self):
        z, y = self.place.pos["z"], self.place.pos["y"]
        self.store = pltpu.make_async_copy(self.final, self.out.at[z, y], self.local_sem)
        self.store.start()
        self.near = []
        for part, axis in enumerate("yz"):
            cols = pl.ds(part * HALF, HALF)
            self.near.append(self.sender.ring(
                axis, lambda step: self.final.at[:, cols], lambda step: self.out.at[z, y, :, cols]))

    def second(self):
        z, y = self.place.pos["z"], self.place.pos["y"]
        self.store.wait()
        wait_all(self.near[0])
        line = lambda step: self.out.at[z, :, :, pl.ds(0, HALF)]
        self.far = self.sender.ring("z", line, line)
        wait_all(self.near[1])
        row = lambda step: self.out.at[:, y, :, pl.ds(HALF, HALF)]
        self.far += self.sender.ring("y", row, row)

    def finish(self):
        wait_all(self.far)


def gain_step(place, sender, gains, bufs, index, axis):
    copies = sender.ring(axis, lambda step: gains.at[index], lambda step: bufs.at[index, step - 1])

    def finish():
        wait_all(copies)
        gains[index + 1] = (gains[index] + bufs[index, 1]) + (bufs[index, 0] + bufs[index, 2])

    return finish


def scatter_kernel(count, with_gains, *refs):
    grads, refs = refs[:count], refs[count:]
    if with_gains:
        gain_in, refs = refs[0], refs[1:]
    outs, refs = refs[:count], refs[count:]
    if with_gains:
        gain_out, refs = refs[0], refs[1:]
    mine, first, second, third, final, send_sems, recv_sems, local_sems = refs[:8]
    place = Place()
    sender = Sender(place, send_sems, recv_sems)
    place.enter()
    works = []
    for i in range(count):
        works.append(GradScatter(place, sender, grads[i], mine.at[i], first.at[i], second.at[i], third.at[i], final.at[i], local_sems.at[i]))
    planes = [PlaneGather(place, sender, final.at[i], outs[i], local_sems.at[i, 3]) for i in range(count)]
    if with_gains:
        gains, gain_bufs = refs[8:]
        gains[0] = gain_in[...]
        gain_finish = gain_step(place, sender, gains, gain_bufs, 0, "z")
    for work in works:
        work.start()
    for work in works:
        for part in range(3):
            work.second(part)
    if with_gains:
        gain_finish()
        gain_finish = gain_step(place, sender, gains, gain_bufs, 1, "y")
    for work in works:
        for part in range(3):
            work.third(part)
    if with_gains:
        gain_finish()
        gain_finish = gain_step(place, sender, gains, gain_bufs, 2, "x")
    for work, plane in zip(works, planes):
        for part in range(3):
            work.finish(part)
        plane.start()
    if with_gains:
        gain_finish()
        gain_out[...] = gains[3]
    for plane in planes:
        plane.second()
    for plane in planes:
        plane.finish()
    sender.drain()


def scatter_grads(grads, gains, collective_id):
    count = len(grads)
    with_gains = gains is not None
    copies = (GradScatter.COPIES + PlaneGather.COPIES) * count + 9 * with_gains
    block = (RING, RING, PIECE, THIRD)
    any_spec = pl.BlockSpec(memory_space=pl.ANY)
    vmem_spec = pl.BlockSpec(memory_space=pltpu.VMEM)
    scratch = [
        pltpu.VMEM((count, 3) + block, BF16),
        pltpu.VMEM((count, 3, 3) + block, BF16),
        pltpu.VMEM((count, 3, 4) + block[1:], BF16),
        pltpu.VMEM((count, 3, 3) + block[2:], BF16),
        pltpu.VMEM((count, PIECE, WIDTH), BF16),
        pltpu.SemaphoreType.DMA((copies,)),
        pltpu.SemaphoreType.DMA((copies,)),
        pltpu.SemaphoreType.DMA((count, 4)),
    ]
    out_shape = [jax.ShapeDtypeStruct(grad.shape[1:], BF16) for grad in grads]
    operands = list(grads)
    if with_gains:
        scratch += [pltpu.VMEM((4,) + gains.shape, F32), pltpu.VMEM((3, 3) + gains.shape, F32)]
        out_shape.append(jax.ShapeDtypeStruct(gains.shape, F32))
        operands.append(gains)
    return pl.pallas_call(
        lambda *refs: scatter_kernel(count, with_gains, *refs),
        out_shape=out_shape,
        in_specs=[any_spec] * count + [vmem_spec] * with_gains,
        out_specs=[any_spec] * count + [vmem_spec] * with_gains,
        scratch_shapes=scratch,
        compiler_params=pltpu.CompilerParams(collective_id=collective_id, has_side_effects=True, vmem_limit_bytes=56 << 20),
        name=f"scatter_grads_{collective_id}",
    )(*operands)


def attention_forward(q_t, k_t, v_t, allowed, score_scale):
    scores = jnp.einsum("ndbq,ndbk->bnqk", q_t, k_t, preferred_element_type=F32) * score_scale
    attn_probs = jax.nn.softmax(jnp.where(allowed, scores, NEG_LARGE), axis=-1)
    attn_out = jnp.einsum("bnqk,ndbk->ndbq", attn_probs.astype(BF16), v_t, preferred_element_type=F32)
    return attn_out.astype(BF16), attn_probs


def attention_backward(grad_out, q_t, k_t, v_t, attn_probs, score_scale):
    grad_v = jnp.einsum("bnqk,ndbq->ndbk", attn_probs.astype(BF16), grad_out, preferred_element_type=F32)
    grad_probs = jnp.einsum("ndbq,ndbk->bnqk", grad_out, v_t, preferred_element_type=F32)
    grad_scores = attn_probs * (grad_probs - jnp.sum(grad_probs * attn_probs, axis=-1, keepdims=True))
    grad_low = (grad_scores * score_scale).astype(BF16)
    grad_q = jnp.einsum("bnqk,ndbk->ndbq", grad_low, k_t, preferred_element_type=F32)
    grad_k = jnp.einsum("bnqk,ndbq->ndbk", grad_low, q_t, preferred_element_type=F32)
    return grad_q, grad_k, grad_v


def solution(mesh):
    batch_spec = P(("pod", "dp"), None, None)
    seg_spec = P(("pod", "dp"), None)

    def local_step(x_in, seg_ids, gain_one, gain_two, w_qkv, w_out, w_up, w_down, grad_y):
        batch_loc, seq_len, hidden = x_in.shape
        heads_loc, head_dim = w_out.shape[:2]
        score_scale = head_dim ** -0.5
        rows_loc = batch_loc // RING
        tokens = rows_loc * seq_len
        shard_rows = w_up.shape[1]
        qkv_cols = w_qkv.shape[1]
        x_pos = lax.axis_index("tp") // 2

        def own_rows(array):
            return lax.dynamic_slice_in_dim(array, x_pos * rows_loc, rows_loc, axis=0)

        def grid_of(own):
            return own.reshape(RING, RING, PIECE, hidden)

        own_att = grid_of(jnp.concatenate([w_qkv.T, w_out.reshape(heads_loc * head_dim, hidden)], axis=0))
        own_up = grid_of(w_up.T)
        own_down = grid_of(w_down)
        (w_att,) = gather_weights([own_att], 1)
        up_t, down = gather_weights([own_up, own_down], 2)
        w_att = w_att.reshape(RING, shard_rows, hidden)
        up_t = up_t.reshape(RING * shard_rows, hidden)
        down = down.reshape(RING * shard_rows, hidden)
        w_qkv_t = w_att[:, :qkv_cols]
        w_out_all = w_att[:, qkv_cols:].reshape(RING * heads_loc * head_dim, hidden)

        x_rows = own_rows(x_in).reshape(tokens, hidden)
        seg_rows = own_rows(seg_ids)
        grad_rows = own_rows(grad_y).reshape(tokens, hidden)
        positions = jnp.arange(seq_len)
        allowed = (positions[:, None] >= positions[None, :])[None, None] & (seg_rows[:, None, :, None] == seg_rows[:, None, None, :])
        normed_a, hat_a, inv_a = norm_forward(x_rows, gain_one)
        qkv_t = dot_nt(w_qkv_t, normed_a).astype(BF16)
        qkv_t = qkv_t.reshape(RING * heads_loc, 3, head_dim, rows_loc, seq_len)
        q_t, k_t, v_t = qkv_t[:, 0], qkv_t[:, 1], qkv_t[:, 2]
        attn_t, attn_probs = attention_forward(q_t, k_t, v_t, allowed, score_scale)
        attn_flat = attn_t.reshape(RING * heads_loc * head_dim, tokens)

        def pair_sum(part):
            return part.astype(F32) + core_swap(part).astype(F32)

        part_one = dot_tn(attn_flat, w_out_all).astype(BF16)
        sum_one = pair_sum(part_one).astype(BF16)
        x_one = (x_rows.astype(F32) + sum_one.astype(F32)).astype(BF16)
        normed_b, hat_b, inv_b = norm_forward(x_one, gain_two)
        pre_act = dot_nt(up_t, normed_b)
        act_val, gelu_pull = jax.vjp(gelu_tanh, pre_act)
        hidden_act = act_val.astype(BF16)
        part_two = dot_tn(hidden_act, down).astype(BF16)
        sum_two = pair_sum(part_two).astype(BF16)
        y_rows = (x_one.astype(F32) + sum_two.astype(F32)).astype(BF16)

        grad_hidden = dot_nt(down, grad_rows).astype(BF16)
        grad_pre = gelu_pull(grad_hidden.astype(F32))[0].astype(BF16)

        grid_shape = (RING, RING, RING, PIECE, hidden)
        grad_down_w = dot_nn(hidden_act, grad_rows).astype(BF16).reshape(grid_shape)
        grad_up_w = dot_nn(grad_pre, normed_b).astype(BF16).reshape(grid_shape)
        grad_up_own, grad_down_own = scatter_grads([grad_up_w, grad_down_w], None, 3)

        part_b = dot_tn(grad_pre, up_t).astype(BF16)
        grad_norm_b = pair_sum(part_b).astype(BF16)
        back_b, gain_grad_two = norm_backward(grad_norm_b, hat_b, inv_b, gain_two)
        grad_x_one = (grad_rows.astype(F32) + back_b).astype(BF16)
        grad_out_w = dot_nn(attn_flat, grad_x_one).astype(BF16)
        grad_attn = dot_nt(w_out_all, grad_x_one).astype(BF16)
        grad_q, grad_k, grad_v = attention_backward(grad_attn.reshape(attn_t.shape), q_t, k_t, v_t, attn_probs, score_scale)
        grad_qkv_t = jnp.stack([grad_q, grad_k, grad_v], axis=1).astype(BF16).reshape(RING * qkv_cols, tokens)
        part_a = dot_tn(grad_qkv_t, w_qkv_t.reshape(RING * qkv_cols, hidden)).astype(BF16)
        grad_norm_a = pair_sum(part_a).astype(BF16)
        back_a, gain_grad_one = norm_backward(grad_norm_a, hat_a, inv_a, gain_one)
        grad_x = (grad_x_one.astype(F32) + back_a).astype(BF16)

        grad_qkv_w = dot_nn(grad_qkv_t, normed_a).astype(BF16)
        grad_att = jnp.concatenate([grad_qkv_w.reshape(RING, qkv_cols, hidden), grad_out_w.reshape(RING, shard_rows - qkv_cols, hidden)], axis=1)
        gains = jnp.concatenate([gain_grad_one[None], gain_grad_two[None], jnp.zeros((6, hidden), F32)], axis=0)
        grad_att_own, gains = scatter_grads([grad_att.reshape(grid_shape)], gains, 4)
        grad_att_own = grad_att_own.reshape(shard_rows, hidden)

        def spread(rows):
            core = lax.axis_index("tp") % 2
            mine = lax.dynamic_slice_in_dim(rows.reshape(rows_loc, seq_len, hidden), core, 1, axis=0)
            return lax.all_gather(mine, "tp", axis=0, tiled=True)

        return (
            spread(y_rows),
            spread(grad_x),
            gains[0].astype(BF16),
            gains[1].astype(BF16),
            grad_att_own[:qkv_cols].T,
            grad_att_own[qkv_cols:].reshape(heads_loc, head_dim, hidden),
            grad_up_own.reshape(shard_rows, hidden).T,
            grad_down_own.reshape(shard_rows, hidden),
        )

    return jax.shard_map(
        local_step,
        mesh=mesh,
        in_specs=(batch_spec, seg_spec, P(None), P(None), P(None, "tp"), P("tp", None, None), P(None, "tp"), P("tp", None), batch_spec),
        out_specs=(batch_spec, batch_spec, P("pod"), P("pod"), P("pod", "tp"), P(("pod", "tp"), None, None), P("pod", "tp"), P(("pod", "tp"), None)),
        check_vma=False,
    )
```

```python
import functools

import jax
import jax.numpy as jnp
from jax import lax
from jax.experimental import pallas as pl
from jax.experimental.pallas import tpu as pltpu
from jax.sharding import PartitionSpec as P

EPS_NORM = 1e-5
NEG_LARGE = -1e30
F32 = jnp.float32
BF16 = jnp.bfloat16
RING = 4


def gelu_tanh(values):
    return jax.nn.gelu(values, approximate=True)


def norm_forward(x_rows, gain_vec):
    x_f32 = x_rows.astype(F32)
    centered = x_f32 - jnp.mean(x_f32, axis=-1, keepdims=True)
    inv_std = lax.rsqrt(jnp.mean(centered * centered, axis=-1, keepdims=True) + EPS_NORM)
    x_hat = centered * inv_std
    return (x_hat * gain_vec.astype(F32)).astype(BF16), x_hat, inv_std


def norm_backward(grad_out, x_hat, inv_std, gain_vec):
    grad_f32 = grad_out.astype(F32)
    grad_gain = jnp.sum(grad_f32 * x_hat, axis=0)
    grad_hat = grad_f32 * gain_vec.astype(F32)
    mean_one = jnp.mean(grad_hat, axis=-1, keepdims=True)
    mean_two = jnp.mean(grad_hat * x_hat, axis=-1, keepdims=True)
    return inv_std * (grad_hat - mean_one - x_hat * mean_two), grad_gain


def dot_nt(lhs, rhs):
    return lax.dot_general(lhs, rhs, (((lhs.ndim - 1,), (rhs.ndim - 1,)), ((), ())), preferred_element_type=F32)


def dot_tn(lhs, rhs):
    return lax.dot_general(lhs, rhs, (((0,), (0,)), ((), ())), preferred_element_type=F32)


def dot_nn(lhs, rhs):
    return lax.dot_general(lhs, rhs, (((lhs.ndim - 1,), (0,)), ((), ())), preferred_element_type=F32)


def core_swap(array):
    return lax.ppermute(array, "tp", [(i, i ^ 1) for i in range(8)])


THIRD = 512
PIECE = 48
WIDTH = 1536
HALF = WIDTH // 2
MESH_ID = pl.DeviceIdType.MESH


class Place:
    def __init__(self):
        plane = lax.axis_index("dp")
        column = lax.axis_index("tp")
        self.pos = {"z": lax.div(plane, RING), "y": lax.rem(plane, RING), "x": lax.div(column, 2)}
        self.core = lax.rem(column, 2)

    def ahead(self, axis, step):
        return lax.rem(self.pos[axis] + step, RING)

    def peer(self, axis, step):
        if axis == "x":
            return {"tp": self.ahead("x", step) * 2 + self.core}
        if axis == "y":
            return {"dp": self.pos["z"] * RING + self.ahead("y", step)}
        return {"dp": self.ahead("z", step) * RING + self.pos["y"]}

    def block(self, axis, step):
        return step if axis == "x" else self.ahead(axis, step)

    def enter(self):
        barrier = pltpu.get_barrier_semaphore()
        for axis in "xyz":
            for step in range(1, RING):
                pl.semaphore_signal(barrier, inc=1, device_id=self.peer(axis, step), device_id_type=MESH_ID)
        pl.semaphore_wait(barrier, 9)


class Sender:
    def __init__(self, place, send_sems, recv_sems):
        self.place, self.send_sems, self.recv_sems = place, send_sems, recv_sems
        self.used = 0
        self.copies = []

    def ring(self, axis, source, target):
        started = []
        for step in range(1, RING):
            copy = pltpu.make_async_remote_copy(
                src_ref=source(step), dst_ref=target(step),
                send_sem=self.send_sems.at[self.used], recv_sem=self.recv_sems.at[self.used],
                device_id=self.place.peer(axis, step), device_id_type=MESH_ID,
            )
            copy.start()
            self.used += 1
            started.append(copy)
        self.copies += started
        return started

    def drain(self):
        for copy in self.copies:
            copy.wait_send()


def wait_all(copies):
    for copy in copies:
        copy.wait_recv()


SEQ = 512
BLOCK = 256
HEAD = 96
SCALE = HEAD ** -0.5


def head_slice(ref, index, kind, lo, hi, kinds=3):
    head, row = lax.div(index, 2), lax.rem(index, 2)
    start = pl.multiple_of((head * kinds + kind) * HEAD, 32)
    return ref.at[pl.ds(start, HEAD), pl.ds(pl.multiple_of(row * SEQ + lo, 128), hi - lo)]


def dot_cols(lhs, rhs):
    return lax.dot_general(lhs, rhs, (((0,), (0,)), ((), ())), preferred_element_type=F32)


def dot_rows(lhs, rhs):
    return lax.dot_general(lhs, rhs, (((1,), (1,)), ((), ())), preferred_element_type=F32)


def probs_block(k_t, q_t, seg, seg_col, row, first):
    keys = first + BLOCK
    scores = dot_cols(k_t, q_t) * SCALE
    query = lax.broadcasted_iota(jnp.int32, (keys, BLOCK), 1) + first
    key = lax.broadcasted_iota(jnp.int32, (keys, BLOCK), 0)
    same = seg[row, :, first : first + BLOCK] == seg_col[row, :keys, :]
    scores = jnp.where((query >= key) & same, scores, NEG_LARGE)
    weights = jnp.exp(scores - jnp.max(scores, axis=0, keepdims=True))
    return weights * (1.0 / jnp.sum(weights, axis=0, keepdims=True))


def attention_forward(qkv, seg, seg_col, out, start, stop):
    @pl.loop(start, stop)
    def _(index):
        row = lax.rem(index, 2)
        for first in range(0, SEQ, BLOCK):
            keys = first + BLOCK
            probs = probs_block(
                head_slice(qkv, index, 1, 0, keys)[...], head_slice(qkv, index, 0, first, keys)[...], seg, seg_col, row, first)
            value = lax.dot_general(
                head_slice(qkv, index, 2, 0, keys)[...], probs.astype(BF16), (((1,), (0,)), ((), ())), preferred_element_type=F32)
            head_slice(out, index, 0, first, keys, kinds=1)[...] = value.astype(BF16)


def attention_backward(qkv, seg, seg_col, grad, out, start, stop):
    @pl.loop(start, stop)
    def _(index):
        row = lax.rem(index, 2)
        grads = []
        for first in range(0, SEQ, BLOCK):
            keys = first + BLOCK
            q_t = head_slice(qkv, index, 0, first, keys)[...]
            k_t = head_slice(qkv, index, 1, 0, keys)[...]
            g_t = head_slice(grad, index, 0, first, keys, kinds=1)[...]
            probs = probs_block(k_t, q_t, seg, seg_col, row, first)
            grad_probs = dot_cols(head_slice(qkv, index, 2, 0, keys)[...], g_t)
            grad_scores = probs * (grad_probs - jnp.sum(grad_probs * probs, axis=0, keepdims=True))
            low = (grad_scores * SCALE).astype(BF16)
            grad_q = lax.dot_general(k_t, low, (((1,), (0,)), ((), ())), preferred_element_type=F32)
            head_slice(out, index, 0, first, keys)[...] = grad_q.astype(BF16)
            grads.append((dot_rows(q_t, low), dot_rows(g_t, probs.astype(BF16))))
        for i in range(2):
            whole = grads[1][i]
            head_slice(out, index, 1 + i, 0, BLOCK)[...] = (grads[0][i] + whole[:, :BLOCK]).astype(BF16)
            head_slice(out, index, 1 + i, BLOCK, SEQ)[...] = whole[:, BLOCK:].astype(BF16)


class WeightGather:
    COPIES = 21

    def __init__(self, place, sender, own, out):
        self.place, self.sender, self.own, self.out = place, sender, own, out

    def spot(self, cols):
        z, y = self.place.pos["z"], self.place.pos["y"]
        return lambda step: self.out.at[pl.ds(1, 3), z, y, :, cols]

    def start(self):
        z, y = self.place.pos["z"], self.place.pos["y"]
        self.near = []
        for part in range(2):
            cols = pl.ds(part * THIRD, THIRD)
            self.near.append(self.sender.ring(
                "x", lambda step: self.own.at[z, y, :, cols], lambda step: self.out.at[RING - step, z, y, :, cols]))

    def start_whole(self):
        cols = pl.ds(2 * THIRD, THIRD)
        self.whole = self.sender.ring(
            "x", lambda step: self.own.at[:, :, :, cols], lambda step: self.out.at[RING - step, :, :, :, cols])

    def second(self):
        self.mid = []
        for part, axis in enumerate("yz"):
            wait_all(self.near[part])
            spot = self.spot(pl.ds(part * THIRD, THIRD))
            self.mid.append(self.sender.ring(axis, spot, spot))

    def third(self):
        z, y = self.place.pos["z"], self.place.pos["y"]
        wait_all(self.mid[0])
        line = lambda step: self.out.at[pl.ds(1, 3), z, :, :, pl.ds(0, THIRD)]
        self.far = self.sender.ring("z", line, line)
        wait_all(self.mid[1])
        row = lambda step: self.out.at[pl.ds(1, 3), :, y, :, pl.ds(THIRD, THIRD)]
        self.far += self.sender.ring("y", row, row)

    def finish(self):
        wait_all(self.far)
        wait_all(self.whole)


def gather_kernel(count, attention, *refs):
    owns, refs = refs[:count], refs[count:]
    work = None
    if attention:
        work = functools.partial(attention_forward, refs[0], refs[1], refs[2], refs[count + 3])
        refs = refs[3 : count + 3] + refs[count + 4 :]
    outs = refs[:count]
    stage, send_sems, recv_sems, local_sems = refs[count:]
    place = Place()
    sender = Sender(place, send_sems, recv_sems)
    gathers = [WeightGather(place, sender, own, out) for own, out in zip(owns, outs)]
    loads = [pltpu.make_async_copy(own, stage.at[i], local_sems.at[i]) for i, own in enumerate(owns)]
    for load in loads:
        load.start()
    place.enter()
    for gather in gathers:
        gather.start()
    for gather in gathers:
        gather.start_whole()
    stores = []
    for i in range(count):
        loads[i].wait()
        store = pltpu.make_async_copy(stage.at[i], outs[i].at[0], local_sems.at[count + i])
        store.start()
        stores.append(store)
    if work is not None:
        work(0, 4)
    for gather in gathers:
        gather.second()
    if work is not None:
        work(4, 10)
    for gather in gathers:
        gather.third()
    if work is not None:
        work(10, 16)
    for gather in gathers:
        gather.finish()
    for store in stores:
        store.wait()
    sender.drain()


def gather_weights(owns, collective_id, attention=()):
    count = len(owns)
    copies = WeightGather.COPIES * count
    any_spec = pl.BlockSpec(memory_space=pl.ANY)
    vmem_spec = pl.BlockSpec(memory_space=pltpu.VMEM)
    out_shape = [jax.ShapeDtypeStruct((RING,) + own.shape, own.dtype) for own in owns]
    out_specs = [any_spec] * count
    if attention:
        rows, tokens = attention[0].shape
        out_shape.append(jax.ShapeDtypeStruct((rows // 3, tokens), BF16))
        out_specs.append(vmem_spec)
    return pl.pallas_call(
        lambda *refs: gather_kernel(count, bool(attention), *refs),
        out_shape=out_shape,
        in_specs=[any_spec] * count + [vmem_spec] * len(attention),
        out_specs=out_specs,
        scratch_shapes=[
            pltpu.VMEM((count,) + owns[0].shape, owns[0].dtype),
            pltpu.SemaphoreType.DMA((copies,)),
            pltpu.SemaphoreType.DMA((copies,)),
            pltpu.SemaphoreType.DMA((2 * count,)),
        ],
        compiler_params=pltpu.CompilerParams(collective_id=collective_id, has_side_effects=True, vmem_limit_bytes=(40 if attention else 16) << 20),
        name=f"gather_weights_{collective_id}",
    )(*owns, *attention)


ORDERS = (("z", "y", "x", 1), ("y", "x", "z", 0), ("x", "z", "y", 0))


class GradScatter:
    COPIES = 27

    def __init__(self, place, sender, grads, mine, first, second, third, final, local_sems):
        self.place, self.sender, self.grads = place, sender, grads
        self.mine, self.bufs, self.final, self.local_sems = mine, (first, second, third), final, local_sems

    def cut(self, part, step):
        axis = ORDERS[part][0]
        index = self.place.block(axis, step)
        cols = pl.ds(part * THIRD, THIRD)
        if axis == "x":
            return self.grads.at[index, :, :, :, cols]
        if axis == "z":
            return self.grads.at[:, index, :, :, cols]
        return self.grads.at[:, :, index, :, cols]

    def start(self):
        self.loads, self.one, self.two, self.three = [], [], [None] * 3, [None] * 3
        for part in range(3):
            self.one.append(self.sender.ring(
                ORDERS[part][0], lambda step: self.cut(part, step), lambda step: self.bufs[0].at[part, step - 1]))
        for part in range(3):
            load = pltpu.make_async_copy(self.cut(part, 0), self.mine.at[part], self.local_sems.at[part])
            load.start()
            self.loads.append(load)

    def second(self, part):
        self.loads[part].wait()
        wait_all(self.one[part])

        @pl.loop(0, RING)
        def _(a):
            for b in range(RING):
                total = self.mine[part, a, b].astype(F32)
                for k in range(3):
                    total = total + self.bufs[0][part, k, a, b].astype(F32)
                self.mine[part, a, b] = total.astype(BF16)

        axis, spot = ORDERS[part][1], ORDERS[part][3]

        def source(step):
            index = self.place.block(axis, step)
            return self.mine.at[part, :, index] if spot else self.mine.at[part, index]

        self.two[part] = self.sender.ring(axis, source, lambda step: self.bufs[1].at[part, step - 1])

    def third(self, part):
        wait_all(self.two[part])
        axis, spot = ORDERS[part][1], ORDERS[part][3]
        own = self.place.block(axis, 0)
        for other in range(RING):
            at = (part, other, own) if spot else (part, own, other)
            total = self.mine[at].astype(F32)
            for k in range(3):
                total = total + self.bufs[1][part, k, other].astype(F32)
            self.bufs[1][part, 3, other] = total.astype(BF16)
        axis = ORDERS[part][2]
        self.three[part] = self.sender.ring(
            axis, lambda step: self.bufs[1].at[part, 3, self.place.block(axis, step)], lambda step: self.bufs[2].at[part, step - 1])

    def finish(self, part):
        wait_all(self.three[part])
        own = self.place.block(ORDERS[part][2], 0)
        total = self.bufs[1][part, 3, own].astype(F32)
        for k in range(3):
            total = total + self.bufs[2][part, k].astype(F32)
        self.final[:, part * THIRD : (part + 1) * THIRD] = total.astype(BF16)


class PlaneGather:
    COPIES = 12

    def __init__(self, place, sender, final, out, local_sem):
        self.place, self.sender, self.final, self.out, self.local_sem = place, sender, final, out, local_sem

    def start(self):
        z, y = self.place.pos["z"], self.place.pos["y"]
        self.store = pltpu.make_async_copy(self.final, self.out.at[z, y], self.local_sem)
        self.store.start()
        self.near = []
        for part, axis in enumerate("yz"):
            cols = pl.ds(part * HALF, HALF)
            self.near.append(self.sender.ring(
                axis, lambda step: self.final.at[:, cols], lambda step: self.out.at[z, y, :, cols]))

    def second(self):
        z, y = self.place.pos["z"], self.place.pos["y"]
        self.store.wait()
        wait_all(self.near[0])
        line = lambda step: self.out.at[z, :, :, pl.ds(0, HALF)]
        self.far = self.sender.ring("z", line, line)
        wait_all(self.near[1])
        row = lambda step: self.out.at[:, y, :, pl.ds(HALF, HALF)]
        self.far += self.sender.ring("y", row, row)

    def finish(self):
        wait_all(self.far)


def gain_step(place, sender, gains, bufs, index, axis):
    copies = sender.ring(axis, lambda step: gains.at[index], lambda step: bufs.at[index, step - 1])

    def finish():
        wait_all(copies)
        gains[index + 1] = (gains[index] + bufs[index, 1]) + (bufs[index, 0] + bufs[index, 2])

    return finish


def scatter_kernel(count, with_gains, attention, *refs):
    grads, refs = refs[:count], refs[count:]
    if with_gains:
        gain_in, refs = refs[0], refs[1:]
    work = None
    if attention:
        work = functools.partial(attention_backward, *refs[:4], refs[4 + count])
        refs = refs[4 : 4 + count] + refs[5 + count :]
    outs, refs = refs[:count], refs[count:]
    if with_gains:
        gain_out, refs = refs[0], refs[1:]
    mine, first, second, third, final, send_sems, recv_sems, local_sems = refs[:8]
    place = Place()
    sender = Sender(place, send_sems, recv_sems)
    place.enter()
    works = []
    for i in range(count):
        works.append(GradScatter(place, sender, grads[i], mine.at[i], first.at[i], second.at[i], third.at[i], final.at[i], local_sems.at[i]))
    planes = [PlaneGather(place, sender, final.at[i], outs[i], local_sems.at[i, 3]) for i in range(count)]
    if with_gains:
        gains, gain_bufs = refs[8:]
        gains[0] = gain_in[...]
        gain_finish = gain_step(place, sender, gains, gain_bufs, 0, "z")
    for item in works:
        item.start()
    if work is not None:
        work(0, 14)
    for i, item in enumerate(works):
        for part in range(3):
            item.second(part)
        if work is not None and i == 0:
            work(14, 16)
    if with_gains:
        gain_finish()
        gain_finish = gain_step(place, sender, gains, gain_bufs, 1, "y")
    for item in works:
        for part in range(3):
            item.third(part)
    if with_gains:
        gain_finish()
        gain_finish = gain_step(place, sender, gains, gain_bufs, 2, "x")
    for item, plane in zip(works, planes):
        for part in range(3):
            item.finish(part)
        plane.start()
    if with_gains:
        gain_finish()
        gain_out[...] = gains[3]
    for plane in planes:
        plane.second()
    for plane in planes:
        plane.finish()
    sender.drain()


def scatter_grads(grads, gains, collective_id, attention=()):
    count = len(grads)
    with_gains = gains is not None
    copies = (GradScatter.COPIES + PlaneGather.COPIES) * count + 9 * with_gains
    block = (RING, RING, PIECE, THIRD)
    any_spec = pl.BlockSpec(memory_space=pl.ANY)
    vmem_spec = pl.BlockSpec(memory_space=pltpu.VMEM)
    scratch = [
        pltpu.VMEM((count, 3) + block, BF16),
        pltpu.VMEM((count, 3, 3) + block, BF16),
        pltpu.VMEM((count, 3, 4) + block[1:], BF16),
        pltpu.VMEM((count, 3, 3) + block[2:], BF16),
        pltpu.VMEM((count, PIECE, WIDTH), BF16),
        pltpu.SemaphoreType.DMA((copies,)),
        pltpu.SemaphoreType.DMA((copies,)),
        pltpu.SemaphoreType.DMA((count, 4)),
    ]
    out_shape = [jax.ShapeDtypeStruct(grad.shape[1:], BF16) for grad in grads]
    operands = list(grads)
    extra_outs = 0
    if with_gains:
        scratch += [pltpu.VMEM((4,) + gains.shape, F32), pltpu.VMEM((3, 3) + gains.shape, F32)]
        out_shape.append(jax.ShapeDtypeStruct(gains.shape, F32))
        operands.append(gains)
        extra_outs = 1
    if attention:
        out_shape.append(jax.ShapeDtypeStruct(attention[0].shape, BF16))
        operands += attention
        extra_outs = 1
    return pl.pallas_call(
        lambda *refs: scatter_kernel(count, with_gains, bool(attention), *refs),
        out_shape=out_shape,
        in_specs=[any_spec] * count + [vmem_spec] * (len(operands) - count),
        out_specs=[any_spec] * count + [vmem_spec] * extra_outs,
        scratch_shapes=scratch,
        compiler_params=pltpu.CompilerParams(collective_id=collective_id, has_side_effects=True, vmem_limit_bytes=60 << 20),
        name=f"scatter_grads_{collective_id}",
    )(*operands)


def solution(mesh):
    batch_spec = P(("pod", "dp"), None, None)
    seg_spec = P(("pod", "dp"), None)

    def local_step(x_in, seg_ids, gain_one, gain_two, w_qkv, w_out, w_up, w_down, grad_y):
        batch_loc, seq_len, hidden = x_in.shape
        heads_loc, head_dim = w_out.shape[:2]
        rows_loc = batch_loc // RING
        tokens = rows_loc * seq_len
        shard_rows = w_up.shape[1]
        qkv_cols = w_qkv.shape[1]
        x_pos = lax.axis_index("tp") // 2

        def own_rows(array):
            return lax.dynamic_slice_in_dim(array, x_pos * rows_loc, rows_loc, axis=0)

        def grid_of(own):
            return own.reshape(RING, RING, PIECE, hidden)

        own_att = grid_of(jnp.concatenate([w_qkv.T, w_out.reshape(heads_loc * head_dim, hidden)], axis=0))
        own_up = grid_of(w_up.T)
        own_down = grid_of(w_down)
        (w_att,) = gather_weights([own_att], 1)
        w_att = w_att.reshape(RING, shard_rows, hidden)
        w_qkv_t = w_att[:, :qkv_cols]
        w_out_all = w_att[:, qkv_cols:].reshape(RING * heads_loc * head_dim, hidden)

        x_rows = own_rows(x_in).reshape(tokens, hidden)
        seg_rows = own_rows(seg_ids)
        grad_rows = own_rows(grad_y).reshape(tokens, hidden)
        seg_row, seg_col = seg_rows[:, None, :], seg_rows[:, :, None]
        normed_a, hat_a, inv_a = norm_forward(x_rows, gain_one)
        qkv_t = dot_nt(w_qkv_t, normed_a).astype(BF16)
        qkv_t = qkv_t.reshape(RING * qkv_cols, tokens)
        up_t, down, attn_flat = gather_weights([own_up, own_down], 2, (qkv_t, seg_row, seg_col))
        up_t = up_t.reshape(RING * shard_rows, hidden)
        down = down.reshape(RING * shard_rows, hidden)

        def pair_sum(part):
            return part.astype(F32) + core_swap(part).astype(F32)

        part_one = dot_tn(attn_flat, w_out_all).astype(BF16)
        sum_one = pair_sum(part_one).astype(BF16)
        x_one = (x_rows.astype(F32) + sum_one.astype(F32)).astype(BF16)
        normed_b, hat_b, inv_b = norm_forward(x_one, gain_two)
        pre_act = dot_nt(up_t, normed_b)
        act_val, gelu_pull = jax.vjp(gelu_tanh, pre_act)
        hidden_act = act_val.astype(BF16)
        part_two = dot_tn(hidden_act, down).astype(BF16)
        sum_two = pair_sum(part_two).astype(BF16)
        y_rows = (x_one.astype(F32) + sum_two.astype(F32)).astype(BF16)

        grad_hidden = dot_nt(down, grad_rows).astype(BF16)
        grad_pre = gelu_pull(grad_hidden.astype(F32))[0].astype(BF16)

        grid_shape = (RING, RING, RING, PIECE, hidden)
        grad_down_w = dot_nn(hidden_act, grad_rows).astype(BF16).reshape(grid_shape)
        grad_up_w = dot_nn(grad_pre, normed_b).astype(BF16).reshape(grid_shape)
        part_b = dot_tn(grad_pre, up_t).astype(BF16)
        grad_norm_b = pair_sum(part_b).astype(BF16)
        back_b, gain_grad_two = norm_backward(grad_norm_b, hat_b, inv_b, gain_two)
        grad_x_one = (grad_rows.astype(F32) + back_b).astype(BF16)
        grad_out_w = dot_nn(attn_flat, grad_x_one).astype(BF16)
        grad_attn = dot_nt(w_out_all, grad_x_one).astype(BF16)
        grad_up_own, grad_down_own, grad_qkv_t = scatter_grads(
            [grad_up_w, grad_down_w], None, 3, (qkv_t, seg_row, seg_col, grad_attn))
        part_a = dot_tn(grad_qkv_t, w_qkv_t.reshape(RING * qkv_cols, hidden)).astype(BF16)
        grad_norm_a = pair_sum(part_a).astype(BF16)
        back_a, gain_grad_one = norm_backward(grad_norm_a, hat_a, inv_a, gain_one)
        grad_x = (grad_x_one.astype(F32) + back_a).astype(BF16)

        grad_qkv_w = dot_nn(grad_qkv_t, normed_a).astype(BF16)
        grad_att = jnp.concatenate([grad_qkv_w.reshape(RING, qkv_cols, hidden), grad_out_w.reshape(RING, shard_rows - qkv_cols, hidden)], axis=1)
        gains = jnp.concatenate([gain_grad_one[None], gain_grad_two[None], jnp.zeros((6, hidden), F32)], axis=0)
        grad_att_own, gains = scatter_grads([grad_att.reshape(grid_shape)], gains, 4)
        grad_att_own = grad_att_own.reshape(shard_rows, hidden)

        def spread(rows):
            core = lax.axis_index("tp") % 2
            mine = lax.dynamic_slice_in_dim(rows.reshape(rows_loc, seq_len, hidden), core, 1, axis=0)
            return lax.all_gather(mine, "tp", axis=0, tiled=True)

        return (
            spread(y_rows),
            spread(grad_x),
            gains[0].astype(BF16),
            gains[1].astype(BF16),
            grad_att_own[:qkv_cols].T,
            grad_att_own[qkv_cols:].reshape(heads_loc, head_dim, hidden),
            grad_up_own.reshape(shard_rows, hidden).T,
            grad_down_own.reshape(shard_rows, hidden),
        )

    return jax.shard_map(
        local_step,
        mesh=mesh,
        in_specs=(batch_spec, seg_spec, P(None), P(None), P(None, "tp"), P("tp", None, None), P(None, "tp"), P("tp", None), batch_spec),
        out_specs=(batch_spec, batch_spec, P("pod"), P("pod"), P("pod", "tp"), P(("pod", "tp"), None, None), P("pod", "tp"), P(("pod", "tp"), None)),
        check_vma=False,
    )
```

```python
import functools

import jax
import jax.numpy as jnp
from jax import lax
from jax.experimental import pallas as pl
from jax.experimental.pallas import tpu as pltpu
from jax.sharding import PartitionSpec as P

EPS_NORM = 1e-5
NEG_LARGE = -1e30
F32 = jnp.float32
BF16 = jnp.bfloat16
RING = 4


def gelu_tanh(values):
    return jax.nn.gelu(values, approximate=True)


def norm_forward(x_rows, gain_vec):
    x_f32 = x_rows.astype(F32)
    centered = x_f32 - jnp.mean(x_f32, axis=-1, keepdims=True)
    inv_std = lax.rsqrt(jnp.mean(centered * centered, axis=-1, keepdims=True) + EPS_NORM)
    x_hat = centered * inv_std
    return (x_hat * gain_vec.astype(F32)).astype(BF16), x_hat, inv_std


def norm_backward(grad_out, x_hat, inv_std, gain_vec):
    grad_f32 = grad_out.astype(F32)
    grad_gain = jnp.sum(grad_f32 * x_hat, axis=0)
    grad_hat = grad_f32 * gain_vec.astype(F32)
    mean_one = jnp.mean(grad_hat, axis=-1, keepdims=True)
    mean_two = jnp.mean(grad_hat * x_hat, axis=-1, keepdims=True)
    return inv_std * (grad_hat - mean_one - x_hat * mean_two), grad_gain


def dot_nt(lhs, rhs):
    return lax.dot_general(lhs, rhs, (((lhs.ndim - 1,), (rhs.ndim - 1,)), ((), ())), preferred_element_type=F32)


def dot_tn(lhs, rhs):
    return lax.dot_general(lhs, rhs, (((0,), (0,)), ((), ())), preferred_element_type=F32)


def dot_nn(lhs, rhs):
    return lax.dot_general(lhs, rhs, (((lhs.ndim - 1,), (0,)), ((), ())), preferred_element_type=F32)


def core_swap(array):
    return lax.ppermute(array, "tp", [(i, i ^ 1) for i in range(8)])


THIRD = 512
PIECE = 48
WIDTH = 1536
HALF = WIDTH // 2
MESH_ID = pl.DeviceIdType.MESH


class Place:
    def __init__(self):
        plane = lax.axis_index("dp")
        column = lax.axis_index("tp")
        self.pos = {"z": lax.div(plane, RING), "y": lax.rem(plane, RING), "x": lax.div(column, 2)}
        self.core = lax.rem(column, 2)

    def ahead(self, axis, step):
        return lax.rem(self.pos[axis] + step, RING)

    def peer(self, axis, step):
        if axis == "x":
            return {"tp": self.ahead("x", step) * 2 + self.core}
        if axis == "y":
            return {"dp": self.pos["z"] * RING + self.ahead("y", step)}
        return {"dp": self.ahead("z", step) * RING + self.pos["y"]}

    def block(self, axis, step):
        return step if axis == "x" else self.ahead(axis, step)

    def sibling(self):
        return {"tp": self.pos["x"] * 2 + 1 - self.core}

    def enter(self, core=False):
        barrier = pltpu.get_barrier_semaphore()
        if core:
            pl.semaphore_signal(barrier, inc=1, device_id=self.sibling(), device_id_type=MESH_ID)
        for axis in "xyz":
            for step in range(1, RING):
                pl.semaphore_signal(barrier, inc=1, device_id=self.peer(axis, step), device_id_type=MESH_ID)
        pl.semaphore_wait(barrier, 9 + core)


class Sender:
    def __init__(self, place, send_sems, recv_sems):
        self.place, self.send_sems, self.recv_sems = place, send_sems, recv_sems
        self.used = 0
        self.copies = []

    def ring(self, axis, source, target):
        started = []
        for step in range(1, RING):
            copy = pltpu.make_async_remote_copy(
                src_ref=source(step), dst_ref=target(step),
                send_sem=self.send_sems.at[self.used], recv_sem=self.recv_sems.at[self.used],
                device_id=self.place.peer(axis, step), device_id_type=MESH_ID,
            )
            copy.start()
            self.used += 1
            started.append(copy)
        self.copies += started
        return started

    def swap(self, source, target):
        copy = pltpu.make_async_remote_copy(
            src_ref=source, dst_ref=target,
            send_sem=self.send_sems.at[self.used], recv_sem=self.recv_sems.at[self.used],
            device_id=self.place.sibling(), device_id_type=MESH_ID,
        )
        copy.start()
        self.used += 1
        return copy

    def drain(self):
        for copy in self.copies:
            copy.wait_send()


def wait_all(copies):
    for copy in copies:
        copy.wait_recv()


SEQ = 512
BLOCK = 256
HEAD = 96
SCALE = HEAD ** -0.5


def head_slice(ref, index, kind, lo, hi, kinds=3):
    head, row = lax.div(index, 2), lax.rem(index, 2)
    start = pl.multiple_of((head * kinds + kind) * HEAD, 32)
    return ref.at[pl.ds(start, HEAD), pl.ds(pl.multiple_of(row * SEQ + lo, 128), hi - lo)]


def dot_cols(lhs, rhs):
    return lax.dot_general(lhs, rhs, (((0,), (0,)), ((), ())), preferred_element_type=F32)


def dot_rows(lhs, rhs):
    return lax.dot_general(lhs, rhs, (((1,), (1,)), ((), ())), preferred_element_type=F32)


def dot_plain(lhs, rhs):
    return lax.dot_general(lhs, rhs, (((1,), (0,)), ((), ())), preferred_element_type=F32)


def probs_block(k_t, q_t, seg, seg_col, row, first):
    keys = first + BLOCK
    scores = dot_cols(k_t, q_t) * SCALE
    query = lax.broadcasted_iota(jnp.int32, (keys, BLOCK), 1) + first
    key = lax.broadcasted_iota(jnp.int32, (keys, BLOCK), 0)
    same = seg[row, :, first : first + BLOCK] == seg_col[row, :keys, :]
    scores = jnp.where((query >= key) & same, scores, NEG_LARGE)
    weights = jnp.exp(scores - jnp.max(scores, axis=0, keepdims=True))
    return weights * (1.0 / jnp.sum(weights, axis=0, keepdims=True))


def attention_forward(qkv, seg, seg_col, out, start, stop):
    @pl.loop(start, stop)
    def _(index):
        row = lax.rem(index, 2)
        for first in range(0, SEQ, BLOCK):
            keys = first + BLOCK
            probs = probs_block(
                head_slice(qkv, index, 1, 0, keys)[...], head_slice(qkv, index, 0, first, keys)[...], seg, seg_col, row, first)
            value = lax.dot_general(
                head_slice(qkv, index, 2, 0, keys)[...], probs.astype(BF16), (((1,), (0,)), ((), ())), preferred_element_type=F32)
            head_slice(out, index, 0, first, keys, kinds=1)[...] = value.astype(BF16)


def attention_backward(qkv, seg, seg_col, grad, out, start, stop):
    @pl.loop(start, stop)
    def _(index):
        row = lax.rem(index, 2)
        grads = []
        for first in range(0, SEQ, BLOCK):
            keys = first + BLOCK
            q_t = head_slice(qkv, index, 0, first, keys)[...]
            k_t = head_slice(qkv, index, 1, 0, keys)[...]
            g_t = head_slice(grad, index, 0, first, keys, kinds=1)[...]
            probs = probs_block(k_t, q_t, seg, seg_col, row, first)
            grad_probs = dot_cols(head_slice(qkv, index, 2, 0, keys)[...], g_t)
            grad_scores = probs * (grad_probs - jnp.sum(grad_probs * probs, axis=0, keepdims=True))
            low = (grad_scores * SCALE).astype(BF16)
            grad_q = lax.dot_general(k_t, low, (((1,), (0,)), ((), ())), preferred_element_type=F32)
            head_slice(out, index, 0, first, keys)[...] = grad_q.astype(BF16)
            grads.append((dot_rows(q_t, low), dot_rows(g_t, probs.astype(BF16))))
        for i in range(2):
            whole = grads[1][i]
            head_slice(out, index, 1 + i, 0, BLOCK)[...] = (grads[0][i] + whole[:, :BLOCK]).astype(BF16)
            head_slice(out, index, 1 + i, BLOCK, SEQ)[...] = whole[:, BLOCK:].astype(BF16)


class WeightGather:
    COPIES = 21

    def __init__(self, place, sender, own, out):
        self.place, self.sender, self.own, self.out = place, sender, own, out

    def spot(self, cols):
        z, y = self.place.pos["z"], self.place.pos["y"]
        return lambda step: self.out.at[pl.ds(1, 3), z, y, :, cols]

    def start(self):
        z, y = self.place.pos["z"], self.place.pos["y"]
        self.near = []
        for part in range(2):
            cols = pl.ds(part * THIRD, THIRD)
            self.near.append(self.sender.ring(
                "x", lambda step: self.own.at[z, y, :, cols], lambda step: self.out.at[RING - step, z, y, :, cols]))

    def start_whole(self):
        cols = pl.ds(2 * THIRD, THIRD)
        self.whole = self.sender.ring(
            "x", lambda step: self.own.at[:, :, :, cols], lambda step: self.out.at[RING - step, :, :, :, cols])

    def second(self):
        self.mid = []
        for part, axis in enumerate("yz"):
            wait_all(self.near[part])
            spot = self.spot(pl.ds(part * THIRD, THIRD))
            self.mid.append(self.sender.ring(axis, spot, spot))

    def third(self):
        z, y = self.place.pos["z"], self.place.pos["y"]
        wait_all(self.mid[0])
        line = lambda step: self.out.at[pl.ds(1, 3), z, :, :, pl.ds(0, THIRD)]
        self.far = self.sender.ring("z", line, line)
        wait_all(self.mid[1])
        row = lambda step: self.out.at[pl.ds(1, 3), :, y, :, pl.ds(THIRD, THIRD)]
        self.far += self.sender.ring("y", row, row)

    def finish(self):
        wait_all(self.far)
        wait_all(self.whole)


def gather_kernel(count, attention, *refs):
    owns, refs = refs[:count], refs[count:]
    work = None
    if attention:
        work = functools.partial(attention_forward, refs[0], refs[1], refs[2], refs[count + 3])
        refs = refs[3 : count + 3] + refs[count + 4 :]
    outs = refs[:count]
    stage, send_sems, recv_sems, local_sems = refs[count:]
    place = Place()
    sender = Sender(place, send_sems, recv_sems)
    gathers = [WeightGather(place, sender, own, out) for own, out in zip(owns, outs)]
    loads = [pltpu.make_async_copy(own, stage.at[i], local_sems.at[i]) for i, own in enumerate(owns)]
    for load in loads:
        load.start()
    place.enter()
    for gather in gathers:
        gather.start()
    for gather in gathers:
        gather.start_whole()
    stores = []
    for i in range(count):
        loads[i].wait()
        store = pltpu.make_async_copy(stage.at[i], outs[i].at[0], local_sems.at[count + i])
        store.start()
        stores.append(store)
    if work is not None:
        work(0, 4)
    for gather in gathers:
        gather.second()
    if work is not None:
        work(4, 10)
    for gather in gathers:
        gather.third()
    if work is not None:
        work(10, 16)
    for gather in gathers:
        gather.finish()
    for store in stores:
        store.wait()
    sender.drain()


def gather_weights(owns, collective_id, attention=()):
    count = len(owns)
    copies = WeightGather.COPIES * count
    any_spec = pl.BlockSpec(memory_space=pl.ANY)
    vmem_spec = pl.BlockSpec(memory_space=pltpu.VMEM)
    out_shape = [jax.ShapeDtypeStruct((RING,) + own.shape, own.dtype) for own in owns]
    out_specs = [any_spec] * count
    if attention:
        rows, tokens = attention[0].shape
        out_shape.append(jax.ShapeDtypeStruct((rows // 3, tokens), BF16))
        out_specs.append(vmem_spec)
    return pl.pallas_call(
        lambda *refs: gather_kernel(count, bool(attention), *refs),
        out_shape=out_shape,
        in_specs=[any_spec] * count + [vmem_spec] * len(attention),
        out_specs=out_specs,
        scratch_shapes=[
            pltpu.VMEM((count,) + owns[0].shape, owns[0].dtype),
            pltpu.SemaphoreType.DMA((copies,)),
            pltpu.SemaphoreType.DMA((copies,)),
            pltpu.SemaphoreType.DMA((2 * count,)),
        ],
        compiler_params=pltpu.CompilerParams(collective_id=collective_id, has_side_effects=True, vmem_limit_bytes=(40 if attention else 16) << 20),
        name=f"gather_weights_{collective_id}",
    )(*owns, *attention)


ORDERS = (("z", "y", "x", 1), ("y", "x", "z", 0), ("x", "z", "y", 0))


class GradScatter:
    def __init__(self, place, sender, grads, widths, bufs, final, local_sems):
        self.place, self.sender, self.grads = place, sender, grads
        self.bufs, self.final, self.local_sems = bufs, final, local_sems
        self.parts = range(len(widths))
        self.cols = [(sum(widths[:part]), widths[part]) for part in self.parts]

    @staticmethod
    def scratch(widths):
        shapes = []
        for width in widths:
            shapes += [
                pltpu.VMEM((RING, RING, PIECE, width), BF16),
                pltpu.VMEM((3, RING, RING, PIECE, width), BF16),
                pltpu.VMEM((RING, RING, PIECE, width), BF16),
                pltpu.VMEM((3, PIECE, width), BF16),
            ]
        return shapes

    def cut(self, part, step):
        axis = ORDERS[part][0]
        index = self.place.block(axis, step)
        cols = pl.ds(*self.cols[part])
        if axis == "x":
            return self.grads.at[index, :, :, :, cols]
        if axis == "z":
            return self.grads.at[:, index, :, :, cols]
        return self.grads.at[:, :, index, :, cols]

    def start(self):
        self.loads, self.one, self.two, self.three = [], [], {}, {}
        for part in self.parts:
            self.one.append(self.sender.ring(
                ORDERS[part][0], lambda step: self.cut(part, step), lambda step: self.bufs[part][1].at[step - 1]))
        for part in self.parts:
            load = pltpu.make_async_copy(self.cut(part, 0), self.bufs[part][0], self.local_sems.at[part])
            load.start()
            self.loads.append(load)

    def second(self):
        for part in self.parts:
            self.loads[part].wait()
            wait_all(self.one[part])
            mine, first, second, _ = self.bufs[part]

            @pl.loop(0, RING)
            def _(a):
                for b in range(RING):
                    total = mine[a, b].astype(F32)
                    for k in range(3):
                        total = total + first[k, a, b].astype(F32)
                    mine[a, b] = total.astype(BF16)

            axis, spot = ORDERS[part][1], ORDERS[part][3]

            def source(step):
                index = self.place.block(axis, step)
                return mine.at[:, index] if spot else mine.at[index]

            self.two[part] = self.sender.ring(axis, source, lambda step: second.at[step - 1])

    def third(self):
        for part in self.parts:
            wait_all(self.two[part])
            mine, _, second, third = self.bufs[part]
            axis, spot = ORDERS[part][1], ORDERS[part][3]
            own = self.place.block(axis, 0)
            for other in range(RING):
                total = mine[(other, own) if spot else (own, other)].astype(F32)
                for k in range(3):
                    total = total + second[k, other].astype(F32)
                second[3, other] = total.astype(BF16)
            axis = ORDERS[part][2]
            self.three[part] = self.sender.ring(
                axis, lambda step: second.at[3, self.place.block(axis, step)], lambda step: third.at[step - 1])

    def finish(self):
        for part in self.parts:
            wait_all(self.three[part])
            _, _, second, third = self.bufs[part]
            total = second[3, self.place.block(ORDERS[part][2], 0)].astype(F32)
            for k in range(3):
                total = total + third[k].astype(F32)
            start, width = self.cols[part]
            self.final[:, start : start + width] = total.astype(BF16)


class PlaneGather:
    COPIES = 12

    def __init__(self, place, sender, final, out, local_sem):
        self.place, self.sender, self.final, self.out, self.local_sem = place, sender, final, out, local_sem

    def start(self):
        z, y = self.place.pos["z"], self.place.pos["y"]
        self.store = pltpu.make_async_copy(self.final, self.out.at[z, y], self.local_sem)
        self.store.start()
        self.near = []
        for part, axis in enumerate("yz"):
            cols = pl.ds(part * HALF, HALF)
            self.near.append(self.sender.ring(
                axis, lambda step: self.final.at[:, cols], lambda step: self.out.at[z, y, :, cols]))

    def second(self):
        z, y = self.place.pos["z"], self.place.pos["y"]
        self.store.wait()
        wait_all(self.near[0])
        line = lambda step: self.out.at[z, :, :, pl.ds(0, HALF)]
        self.far = self.sender.ring("z", line, line)
        wait_all(self.near[1])
        row = lambda step: self.out.at[:, y, :, pl.ds(HALF, HALF)]
        self.far += self.sender.ring("y", row, row)

    def finish(self):
        wait_all(self.far)


def gain_step(place, sender, gains, bufs, index, axis):
    copies = sender.ring(axis, lambda step: gains.at[index], lambda step: bufs.at[index, step - 1])

    def finish():
        wait_all(copies)
        gains[index + 1] = (gains[index] + bufs[index, 1]) + (bufs[index, 0] + bufs[index, 2])

    return finish


def grad_works(place, sender, grads, widths, bufs, finals, outs, local_sems):
    parts = len(widths)
    works, planes = [], []
    for i, grad in enumerate(grads):
        mine = bufs[4 * parts * i : 4 * parts * (i + 1)]
        mine = [mine[4 * part : 4 * part + 4] for part in range(parts)]
        works.append(GradScatter(place, sender, grad, widths, mine, finals.at[i], local_sems.at[i]))
        planes.append(PlaneGather(place, sender, finals.at[i], outs[i], local_sems.at[i, 3]))
    return works, planes


def comm_scratch(count, widths, extra):
    copies = (9 * len(widths) + PlaneGather.COPIES) * count + extra
    scratch = [
        pltpu.VMEM((count, PIECE, WIDTH), BF16),
        pltpu.SemaphoreType.DMA((copies,)),
        pltpu.SemaphoreType.DMA((copies,)),
        pltpu.SemaphoreType.DMA((count, 4)),
    ]
    for _ in range(count):
        scratch += GradScatter.scratch(widths)
    return scratch


ANY_SPEC = pl.BlockSpec(memory_space=pl.ANY)
VMEM_SPEC = pl.BlockSpec(memory_space=pltpu.VMEM)
ATT_WIDTHS = (768, 768)
MLP_WIDTHS = (640, 512, 384)


def last_kernel(grad, gain_in, out, gain_out, gains, gain_bufs, finals, send_sems, recv_sems, local_sems, *bufs):
    place = Place()
    sender = Sender(place, send_sems, recv_sems)
    place.enter()
    (work,), (plane,) = grad_works(place, sender, [grad], ATT_WIDTHS, bufs, finals, [out], local_sems)
    gains[0] = gain_in[...]
    gain_finish = gain_step(place, sender, gains, gain_bufs, 0, "z")
    work.start()
    gain_finish()
    gain_finish = gain_step(place, sender, gains, gain_bufs, 1, "y")
    work.second()
    gain_finish()
    gain_finish = gain_step(place, sender, gains, gain_bufs, 2, "x")
    work.third()
    work.finish()
    plane.start()
    gain_finish()
    gain_out[...] = gains[3]
    plane.second()
    plane.finish()
    sender.drain()


def scatter_last(grad, gains):
    return pl.pallas_call(
        last_kernel,
        out_shape=[jax.ShapeDtypeStruct(grad.shape[1:], BF16), jax.ShapeDtypeStruct(gains.shape, F32)],
        in_specs=[ANY_SPEC, VMEM_SPEC],
        out_specs=[ANY_SPEC, VMEM_SPEC],
        scratch_shapes=[pltpu.VMEM((4,) + gains.shape, F32), pltpu.VMEM((3, 3) + gains.shape, F32)] + comm_scratch(1, ATT_WIDTHS, 9),
        compiler_params=pltpu.CompilerParams(collective_id=4, has_side_effects=True, vmem_limit_bytes=32 << 20),
        name="scatter_last",
    )(grad, gains)


QKV_ROWS = 576
OUT_ROWS = 192
TOKENS = 2 * SEQ
STEP = 256
NORM_STEP = 128


def back_kernel(
    grad_up, grad_down, qkv_in, seg, seg_col, attn, grad_one_in, w_att, normed_in, x_in, gain,
    out_up, out_down, grad_att, grad_x, gain_grad,
    qkv, grad_attn, grad_one, normed, w_qkv, w_out, part, other, stage, load_sems, stage_sems,
    finals, send_sems, recv_sems, local_sems, *bufs,
):
    place = Place()
    sender = Sender(place, send_sems, recv_sems)
    loads = {}

    def load(name, source, target, index):
        copy = pltpu.make_async_copy(source, target, load_sems.at[index])
        copy.start()
        loads.setdefault(name, []).append(copy)

    def ready(name):
        for copy in loads[name]:
            copy.wait()

    load("one", grad_one_in, grad_one, 0)
    for shard in range(RING):
        load("out", w_att.at[shard, pl.ds(QKV_ROWS, OUT_ROWS)], w_out.at[pl.ds(shard * OUT_ROWS, OUT_ROWS)], 1 + shard)
    load("qkv", qkv_in, qkv, 5)
    load("normed", normed_in, normed, 6)
    for shard in range(RING):
        load("w", w_att.at[shard, pl.ds(0, QKV_ROWS)], w_qkv.at[pl.ds(shard * QKV_ROWS, QKV_ROWS)], 7 + shard)
    place.enter(core=True)
    works, planes = grad_works(place, sender, [grad_up, grad_down], MLP_WIDTHS, bufs, finals, [out_up, out_down], local_sems)
    for work in works:
        work.start()

    stores = []

    def put(rows, shard, start):
        slot = len(stores) % 2
        if len(stores) >= 2:
            stores[-2].wait()
        stage[slot] = rows.astype(BF16)
        copy = pltpu.make_async_copy(stage.at[slot], grad_att.at[shard, pl.ds(start, OUT_ROWS)], stage_sems.at[slot])
        copy.start()
        stores.append(copy)

    ready("one")
    ready("out")
    for shard in range(RING):
        rows = pl.ds(shard * OUT_ROWS, OUT_ROWS)
        grad_attn[rows] = dot_rows(w_out[rows], grad_one[...]).astype(BF16)
    ready("qkv")
    attention_backward(qkv, seg, seg_col, grad_attn, qkv, 0, 16)
    works[0].second()

    ready("w")
    swaps = []
    for index in range(TOKENS // STEP):
        rows = pl.ds(index * STEP, STEP)
        part[rows] = dot_cols(qkv[:, index * STEP : (index + 1) * STEP], w_qkv[...]).astype(BF16)
        swaps.append(sender.swap(part.at[rows], other.at[rows]))
    works[1].second()
    for shard in range(RING):
        put(dot_plain(attn[shard * OUT_ROWS : (shard + 1) * OUT_ROWS], grad_one[...]), shard, QKV_ROWS)
    ready("normed")
    for shard in range(RING):
        for block in range(3):
            start = shard * QKV_ROWS + block * OUT_ROWS
            put(dot_plain(qkv[start : start + OUT_ROWS], normed[...]), shard, block * OUT_ROWS)
    for store in stores[-2:]:
        store.wait()
    load("x", x_in, normed, 11)
    for work in works:
        work.third()
    ready("x")
    gain_grad[...] = jnp.zeros_like(gain_grad)
    wait_all(swaps)
    for copy in swaps:
        copy.wait_send()

    @pl.loop(0, TOKENS // NORM_STEP)
    def _(index):
        rows = pl.ds(pl.multiple_of(index * NORM_STEP, NORM_STEP), NORM_STEP)
        x_f32 = normed[rows].astype(F32)
        centered = x_f32 - jnp.mean(x_f32, axis=-1, keepdims=True)
        inv_std = lax.rsqrt(jnp.mean(centered * centered, axis=-1, keepdims=True) + EPS_NORM)
        x_hat = centered * inv_std
        grad = (part[rows].astype(F32) + other[rows].astype(F32)).astype(BF16).astype(F32)
        gain_grad[...] += jnp.sum(grad * x_hat, axis=0, keepdims=True)
        grad_hat = grad * gain[...].astype(F32)
        mean_one = jnp.mean(grad_hat, axis=-1, keepdims=True)
        mean_two = jnp.mean(grad_hat * x_hat, axis=-1, keepdims=True)
        back = inv_std * (grad_hat - mean_one - x_hat * mean_two)
        part[rows] = (grad_one[rows].astype(F32) + back).astype(BF16)

    result = pltpu.make_async_copy(part, grad_x, load_sems.at[12])
    result.start()
    for work, plane in zip(works, planes):
        work.finish()
        plane.start()
    for plane in planes:
        plane.second()
    for plane in planes:
        plane.finish()
    result.wait()
    sender.drain()


def backward(grad_up, grad_down, qkv_t, seg, seg_col, attn, grad_one, w_att, normed, x_rows, gain):
    tokens = (TOKENS, WIDTH)
    return pl.pallas_call(
        back_kernel,
        out_shape=[
            jax.ShapeDtypeStruct(grad_up.shape[1:], BF16),
            jax.ShapeDtypeStruct(grad_down.shape[1:], BF16),
            jax.ShapeDtypeStruct(w_att.shape, BF16),
            jax.ShapeDtypeStruct(tokens, BF16),
            jax.ShapeDtypeStruct((1, WIDTH), F32),
        ],
        in_specs=[ANY_SPEC, ANY_SPEC, ANY_SPEC, VMEM_SPEC, VMEM_SPEC, VMEM_SPEC, ANY_SPEC, ANY_SPEC, ANY_SPEC, ANY_SPEC, VMEM_SPEC],
        out_specs=[ANY_SPEC, ANY_SPEC, ANY_SPEC, ANY_SPEC, VMEM_SPEC],
        scratch_shapes=[
            pltpu.VMEM(qkv_t.shape, BF16),
            pltpu.VMEM(attn.shape, BF16),
            pltpu.VMEM(tokens, BF16),
            pltpu.VMEM(tokens, BF16),
            pltpu.VMEM((RING * QKV_ROWS, WIDTH), BF16),
            pltpu.VMEM((RING * OUT_ROWS, WIDTH), BF16),
            pltpu.VMEM(tokens, BF16),
            pltpu.VMEM(tokens, BF16),
            pltpu.VMEM((2, OUT_ROWS, WIDTH), BF16),
            pltpu.SemaphoreType.DMA((13,)),
            pltpu.SemaphoreType.DMA((2,)),
        ] + comm_scratch(2, MLP_WIDTHS, TOKENS // STEP),
        compiler_params=pltpu.CompilerParams(collective_id=3, has_side_effects=True, vmem_limit_bytes=67043328),
        name="backward",
    )(grad_up, grad_down, qkv_t, seg, seg_col, attn, grad_one, w_att, normed, x_rows, gain)


def solution(mesh):
    batch_spec = P(("pod", "dp"), None, None)
    seg_spec = P(("pod", "dp"), None)

    def local_step(x_in, seg_ids, gain_one, gain_two, w_qkv, w_out, w_up, w_down, grad_y):
        batch_loc, seq_len, hidden = x_in.shape
        heads_loc, head_dim = w_out.shape[:2]
        rows_loc = batch_loc // RING
        tokens = rows_loc * seq_len
        shard_rows = w_up.shape[1]
        qkv_cols = w_qkv.shape[1]
        x_pos = lax.axis_index("tp") // 2

        def own_rows(array):
            return lax.dynamic_slice_in_dim(array, x_pos * rows_loc, rows_loc, axis=0)

        def grid_of(own):
            return own.reshape(RING, RING, PIECE, hidden)

        own_att = grid_of(jnp.concatenate([w_qkv.T, w_out.reshape(heads_loc * head_dim, hidden)], axis=0))
        own_up = grid_of(w_up.T)
        own_down = grid_of(w_down)
        (w_att,) = gather_weights([own_att], 1)
        w_att = w_att.reshape(RING, shard_rows, hidden)
        w_qkv_t = w_att[:, :qkv_cols]
        w_out_all = w_att[:, qkv_cols:].reshape(RING * heads_loc * head_dim, hidden)

        x_rows = own_rows(x_in).reshape(tokens, hidden)
        seg_rows = own_rows(seg_ids)
        grad_rows = own_rows(grad_y).reshape(tokens, hidden)
        seg_row, seg_col = seg_rows[:, None, :], seg_rows[:, :, None]
        normed_a, _, _ = norm_forward(x_rows, gain_one)
        qkv_t = dot_nt(w_qkv_t, normed_a).astype(BF16)
        qkv_t = qkv_t.reshape(RING * qkv_cols, tokens)
        up_t, down, attn_flat = gather_weights([own_up, own_down], 2, (qkv_t, seg_row, seg_col))
        up_t = up_t.reshape(RING * shard_rows, hidden)
        down = down.reshape(RING * shard_rows, hidden)

        def pair_sum(part):
            return part.astype(F32) + core_swap(part).astype(F32)

        part_one = dot_tn(attn_flat, w_out_all).astype(BF16)
        sum_one = pair_sum(part_one).astype(BF16)
        x_one = (x_rows.astype(F32) + sum_one.astype(F32)).astype(BF16)
        normed_b, hat_b, inv_b = norm_forward(x_one, gain_two)
        pre_act = dot_nt(up_t, normed_b)
        act_val, gelu_pull = jax.vjp(gelu_tanh, pre_act)
        hidden_act = act_val.astype(BF16)
        part_two = dot_tn(hidden_act, down).astype(BF16)
        sum_two = pair_sum(part_two).astype(BF16)
        y_rows = (x_one.astype(F32) + sum_two.astype(F32)).astype(BF16)

        grad_hidden = dot_nt(down, grad_rows).astype(BF16)
        grad_pre = gelu_pull(grad_hidden.astype(F32))[0].astype(BF16)

        grid_shape = (RING, RING, RING, PIECE, hidden)
        grad_down_w = dot_nn(hidden_act, grad_rows).astype(BF16).reshape(grid_shape)
        grad_up_w = dot_nn(grad_pre, normed_b).astype(BF16).reshape(grid_shape)
        part_b = dot_tn(grad_pre, up_t).astype(BF16)
        grad_norm_b = pair_sum(part_b).astype(BF16)
        back_b, gain_grad_two = norm_backward(grad_norm_b, hat_b, inv_b, gain_two)
        grad_x_one = (grad_rows.astype(F32) + back_b).astype(BF16)
        grad_up_own, grad_down_own, grad_att, grad_x, gain_grad_one = backward(
            grad_up_w, grad_down_w, qkv_t, seg_row, seg_col, attn_flat, grad_x_one, w_att, normed_a, x_rows, gain_one[None])
        gains = jnp.concatenate([gain_grad_one, gain_grad_two[None], jnp.zeros((6, hidden), F32)], axis=0)
        grad_att_own, gains = scatter_last(grad_att.reshape(grid_shape), gains)
        grad_att_own = grad_att_own.reshape(shard_rows, hidden)

        def spread(rows):
            core = lax.axis_index("tp") % 2
            mine = lax.dynamic_slice_in_dim(rows.reshape(rows_loc, seq_len, hidden), core, 1, axis=0)
            return lax.all_gather(mine, "tp", axis=0, tiled=True)

        return (
            spread(y_rows),
            spread(grad_x),
            gains[0].astype(BF16),
            gains[1].astype(BF16),
            grad_att_own[:qkv_cols].T,
            grad_att_own[qkv_cols:].reshape(heads_loc, head_dim, hidden),
            grad_up_own.reshape(shard_rows, hidden).T,
            grad_down_own.reshape(shard_rows, hidden),
        )

    return jax.shard_map(
        local_step,
        mesh=mesh,
        in_specs=(batch_spec, seg_spec, P(None), P(None), P(None, "tp"), P("tp", None, None), P(None, "tp"), P("tp", None), batch_spec),
        out_specs=(batch_spec, batch_spec, P("pod"), P("pod"), P("pod", "tp"), P(("pod", "tp"), None, None), P("pod", "tp"), P(("pod", "tp"), None)),
        check_vma=False,
    )
```

```python
import functools

import jax
import jax.numpy as jnp
from jax import lax
from jax.experimental import pallas as pl
from jax.experimental.pallas import tpu as pltpu
from jax.sharding import PartitionSpec as P

EPS_NORM = 1e-5
NEG_LARGE = -1e30
F32 = jnp.float32
BF16 = jnp.bfloat16
RING = 4


def gelu_tanh(values):
    return jax.nn.gelu(values, approximate=True)


def dot_nt(lhs, rhs):
    return lax.dot_general(lhs, rhs, (((lhs.ndim - 1,), (rhs.ndim - 1,)), ((), ())), preferred_element_type=F32)


def dot_tn(lhs, rhs):
    return lax.dot_general(lhs, rhs, (((0,), (0,)), ((), ())), preferred_element_type=F32)


def core_swap(array):
    return lax.ppermute(array, "tp", [(i, i ^ 1) for i in range(8)])


THIRD = 512
PIECE = 48
WIDTH = 1536
HALF = WIDTH // 2
MESH_ID = pl.DeviceIdType.MESH


class Place:
    def __init__(self):
        plane = lax.axis_index("dp")
        column = lax.axis_index("tp")
        self.pos = {"z": lax.div(plane, RING), "y": lax.rem(plane, RING), "x": lax.div(column, 2)}
        self.core = lax.rem(column, 2)

    def ahead(self, axis, step):
        return lax.rem(self.pos[axis] + step, RING)

    def peer(self, axis, step):
        if axis == "x":
            return {"tp": self.ahead("x", step) * 2 + self.core}
        if axis == "y":
            return {"dp": self.pos["z"] * RING + self.ahead("y", step)}
        return {"dp": self.ahead("z", step) * RING + self.pos["y"]}

    def block(self, axis, step):
        return step if axis == "x" else self.ahead(axis, step)

    def sibling(self):
        return {"tp": self.pos["x"] * 2 + 1 - self.core}

    def enter(self, core=False):
        barrier = pltpu.get_barrier_semaphore()
        if core:
            pl.semaphore_signal(barrier, inc=1, device_id=self.sibling(), device_id_type=MESH_ID)
        for axis in "xyz":
            for step in range(1, RING):
                pl.semaphore_signal(barrier, inc=1, device_id=self.peer(axis, step), device_id_type=MESH_ID)
        pl.semaphore_wait(barrier, 9 + core)


class Sender:
    def __init__(self, place, send_sems, recv_sems):
        self.place, self.send_sems, self.recv_sems = place, send_sems, recv_sems
        self.used = 0
        self.copies = []

    def ring(self, axis, source, target):
        started = []
        for step in range(1, RING):
            copy = pltpu.make_async_remote_copy(
                src_ref=source(step), dst_ref=target(step),
                send_sem=self.send_sems.at[self.used], recv_sem=self.recv_sems.at[self.used],
                device_id=self.place.peer(axis, step), device_id_type=MESH_ID,
            )
            copy.start()
            self.used += 1
            started.append(copy)
        self.copies += started
        return started

    def swap(self, source, target):
        copy = pltpu.make_async_remote_copy(
            src_ref=source, dst_ref=target,
            send_sem=self.send_sems.at[self.used], recv_sem=self.recv_sems.at[self.used],
            device_id=self.place.sibling(), device_id_type=MESH_ID,
        )
        copy.start()
        self.used += 1
        return copy

    def drain(self):
        for copy in self.copies:
            copy.wait_send()


def wait_all(copies):
    for copy in copies:
        copy.wait_recv()


ANY_SPEC = pl.BlockSpec(memory_space=pl.ANY)
VMEM_SPEC = pl.BlockSpec(memory_space=pltpu.VMEM)
QKV_ROWS = 576
OUT_ROWS = 192
SEQ = 512
TOKENS = 2 * SEQ
STEP = 256
NORM_STEP = 128
BLOCK = 256
HEAD = 96
SCALE = HEAD ** -0.5


def head_slice(ref, index, kind, lo, hi, kinds=3):
    head, row = lax.div(index, 2), lax.rem(index, 2)
    start = pl.multiple_of((head * kinds + kind) * HEAD, 32)
    return ref.at[pl.ds(start, HEAD), pl.ds(pl.multiple_of(row * SEQ + lo, 128), hi - lo)]


def dot_cols(lhs, rhs):
    return lax.dot_general(lhs, rhs, (((0,), (0,)), ((), ())), preferred_element_type=F32)


def dot_rows(lhs, rhs):
    return lax.dot_general(lhs, rhs, (((1,), (1,)), ((), ())), preferred_element_type=F32)


def dot_plain(lhs, rhs):
    return lax.dot_general(lhs, rhs, (((1,), (0,)), ((), ())), preferred_element_type=F32)


def probs_block(k_t, q_t, seg, seg_col, row, first):
    keys = first + BLOCK
    scores = dot_cols(k_t, q_t) * SCALE
    query = lax.broadcasted_iota(jnp.int32, (keys, BLOCK), 1) + first
    key = lax.broadcasted_iota(jnp.int32, (keys, BLOCK), 0)
    same = seg[row, :, first : first + BLOCK] == seg_col[row, :keys, :]
    scores = jnp.where((query >= key) & same, scores, NEG_LARGE)
    weights = jnp.exp(scores - jnp.max(scores, axis=0, keepdims=True))
    return weights * (1.0 / jnp.sum(weights, axis=0, keepdims=True))


def attention_forward(qkv, seg, seg_col, out, start, stop):
    @pl.loop(start, stop)
    def _(index):
        row = lax.rem(index, 2)
        for first in range(0, SEQ, BLOCK):
            keys = first + BLOCK
            probs = probs_block(
                head_slice(qkv, index, 1, 0, keys)[...], head_slice(qkv, index, 0, first, keys)[...], seg, seg_col, row, first)
            value = lax.dot_general(
                head_slice(qkv, index, 2, 0, keys)[...], probs.astype(BF16), (((1,), (0,)), ((), ())), preferred_element_type=F32)
            head_slice(out, index, 0, first, keys, kinds=1)[...] = value.astype(BF16)


def attention_backward(qkv, seg, seg_col, grad, out, start, stop):
    @pl.loop(start, stop)
    def _(index):
        row = lax.rem(index, 2)
        grads = []
        for first in range(0, SEQ, BLOCK):
            keys = first + BLOCK
            q_t = head_slice(qkv, index, 0, first, keys)[...]
            k_t = head_slice(qkv, index, 1, 0, keys)[...]
            g_t = head_slice(grad, index, 0, first, keys, kinds=1)[...]
            probs = probs_block(k_t, q_t, seg, seg_col, row, first)
            grad_probs = dot_cols(head_slice(qkv, index, 2, 0, keys)[...], g_t)
            grad_scores = probs * (grad_probs - jnp.sum(grad_probs * probs, axis=0, keepdims=True))
            low = (grad_scores * SCALE).astype(BF16)
            grad_q = lax.dot_general(k_t, low, (((1,), (0,)), ((), ())), preferred_element_type=F32)
            head_slice(out, index, 0, first, keys)[...] = grad_q.astype(BF16)
            grads.append((dot_rows(q_t, low), dot_rows(g_t, probs.astype(BF16))))
        for i in range(2):
            whole = grads[1][i]
            head_slice(out, index, 1 + i, 0, BLOCK)[...] = (grads[0][i] + whole[:, :BLOCK]).astype(BF16)
            head_slice(out, index, 1 + i, BLOCK, SEQ)[...] = whole[:, BLOCK:].astype(BF16)


class WeightGather:
    COPIES = 21

    def __init__(self, place, sender, own, out):
        self.place, self.sender, self.own, self.out = place, sender, own, out

    def spot(self, cols):
        z, y = self.place.pos["z"], self.place.pos["y"]
        return lambda step: self.out.at[pl.ds(1, 3), z, y, :, cols]

    def start(self):
        z, y = self.place.pos["z"], self.place.pos["y"]
        self.near = []
        for part in range(2):
            cols = pl.ds(part * THIRD, THIRD)
            self.near.append(self.sender.ring(
                "x", lambda step: self.own.at[z, y, :, cols], lambda step: self.out.at[RING - step, z, y, :, cols]))

    def start_whole(self):
        cols = pl.ds(2 * THIRD, THIRD)
        self.whole = self.sender.ring(
            "x", lambda step: self.own.at[:, :, :, cols], lambda step: self.out.at[RING - step, :, :, :, cols])

    def second(self):
        self.mid = []
        for part, axis in enumerate("yz"):
            wait_all(self.near[part])
            spot = self.spot(pl.ds(part * THIRD, THIRD))
            self.mid.append(self.sender.ring(axis, spot, spot))

    def third(self):
        z, y = self.place.pos["z"], self.place.pos["y"]
        wait_all(self.mid[0])
        line = lambda step: self.out.at[pl.ds(1, 3), z, :, :, pl.ds(0, THIRD)]
        self.far = self.sender.ring("z", line, line)
        wait_all(self.mid[1])
        row = lambda step: self.out.at[pl.ds(1, 3), :, y, :, pl.ds(THIRD, THIRD)]
        self.far += self.sender.ring("y", row, row)

    def finish(self):
        wait_all(self.far)
        wait_all(self.whole)


def norm_stats(x_f32):
    centered = x_f32 - jnp.mean(x_f32, axis=-1, keepdims=True)
    inv_std = lax.rsqrt(jnp.mean(centered * centered, axis=-1, keepdims=True) + EPS_NORM)
    return centered * inv_std, inv_std


def token_blocks(body):
    @pl.loop(0, TOKENS // NORM_STEP)
    def _(index):
        body(pl.ds(pl.multiple_of(index * NORM_STEP, NORM_STEP), NORM_STEP))


def front_kernel(
    own_att, own_up, own_down, x_in, gain_a, gain_b, seg, seg_col,
    w_att, w_up, w_down, qkv_out, attn_out, normed_a_out, x_one_out, normed_b_out,
    weights, stage, x_one, normed, qkv, attn, part, other, load_sems, send_sems, recv_sems,
):
    place = Place()
    sender = Sender(place, send_sems, recv_sems)

    def copy(source, target, index):
        started = pltpu.make_async_copy(source, target, load_sems.at[index])
        started.start()
        return started

    loads = [copy(x_in, x_one, 0), copy(own_att, weights.at[0], 1), copy(own_up, stage.at[0], 2), copy(own_down, stage.at[1], 3)]
    place.enter(core=True)
    att = WeightGather(place, sender, own_att, w_att)
    mlp = [WeightGather(place, sender, own_up, w_up), WeightGather(place, sender, own_down, w_down)]
    att.start()
    att.start_whole()
    for gather in mlp:
        gather.start()
    for gather in mlp:
        gather.start_whole()
    loads[0].wait()

    def first_norm(rows):
        x_hat, _ = norm_stats(x_one[rows].astype(F32))
        normed[rows] = (x_hat * gain_a[...].astype(F32)).astype(BF16)

    token_blocks(first_norm)
    results = [copy(normed, normed_a_out, 4)]
    att.second()
    for load in loads[1:]:
        load.wait()
    results += [copy(weights.at[0], w_att.at[0], 5), copy(stage.at[0], w_up.at[0], 6), copy(stage.at[1], w_down.at[0], 7)]

    def project(start, stop):
        @pl.loop(start, stop)
        def _(index):
            block = weights[lax.div(index, 3), lax.rem(index, 3)].reshape(OUT_ROWS, WIDTH)
            qkv[pl.ds(pl.multiple_of(index * OUT_ROWS, OUT_ROWS), OUT_ROWS)] = dot_rows(block, normed[...]).astype(BF16)

    project(0, 3)
    att.third()
    for gather in mlp:
        gather.second()
    att.finish()
    others = [copy(w_att.at[shard], weights.at[shard], 7 + shard) for shard in range(1, RING)]
    for load in others:
        load.wait()
    project(3, 12)
    results.append(copy(qkv, qkv_out, 11))
    attention_forward(qkv, seg, seg_col, attn, 0, 6)
    for gather in mlp:
        gather.third()
    attention_forward(qkv, seg, seg_col, attn, 6, 16)
    results.append(copy(attn, attn_out, 12))
    swaps = []
    for index in range(TOKENS // STEP):
        rows = pl.ds(index * STEP, STEP)
        total = None
        for shard in range(RING):
            block = weights[shard, 3].reshape(OUT_ROWS, WIDTH)
            term = dot_cols(attn[shard * OUT_ROWS : (shard + 1) * OUT_ROWS, index * STEP : (index + 1) * STEP], block)
            total = term if total is None else total + term
        part[rows] = total.astype(BF16)
        swaps.append(sender.swap(part.at[rows], other.at[rows]))
    results[0].wait()
    wait_all(swaps)

    def second_norm(rows):
        summed = (part[rows].astype(F32) + other[rows].astype(F32)).astype(BF16)
        x_new = (x_one[rows].astype(F32) + summed.astype(F32)).astype(BF16)
        x_one[rows] = x_new
        x_hat, _ = norm_stats(x_new.astype(F32))
        normed[rows] = (x_hat * gain_b[...].astype(F32)).astype(BF16)

    token_blocks(second_norm)
    results += [copy(x_one, x_one_out, 13), copy(normed, normed_b_out, 14)]
    for gather in mlp:
        gather.finish()
    for result in results[1:]:
        result.wait()
    for swap in swaps:
        swap.wait_send()
    sender.drain()


def front(own_att, own_up, own_down, x_rows, gain_a, gain_b, seg, seg_col):
    tokens = (TOKENS, WIDTH)
    gathered = jax.ShapeDtypeStruct((RING,) + own_att.shape, BF16)
    rows = jax.ShapeDtypeStruct(tokens, BF16)
    copies = 3 * WeightGather.COPIES + TOKENS // STEP
    return pl.pallas_call(
        front_kernel,
        out_shape=[
            gathered, gathered, gathered,
            jax.ShapeDtypeStruct((RING * QKV_ROWS, TOKENS), BF16), jax.ShapeDtypeStruct((RING * OUT_ROWS, TOKENS), BF16),
            rows, rows, rows,
        ],
        in_specs=[ANY_SPEC] * 4 + [VMEM_SPEC] * 4,
        out_specs=[ANY_SPEC] * 8,
        scratch_shapes=[
            pltpu.VMEM(gathered.shape, BF16),
            pltpu.VMEM((2,) + own_att.shape, BF16),
            pltpu.VMEM(tokens, BF16),
            pltpu.VMEM(tokens, BF16),
            pltpu.VMEM((RING * QKV_ROWS, TOKENS), BF16),
            pltpu.VMEM((RING * OUT_ROWS, TOKENS), BF16),
            pltpu.VMEM(tokens, BF16),
            pltpu.VMEM(tokens, BF16),
            pltpu.SemaphoreType.DMA((15,)),
            pltpu.SemaphoreType.DMA((copies,)),
            pltpu.SemaphoreType.DMA((copies,)),
        ],
        compiler_params=pltpu.CompilerParams(collective_id=1, has_side_effects=True, vmem_limit_bytes=56 << 20),
        name="front",
    )(own_att, own_up, own_down, x_rows, gain_a, gain_b, seg, seg_col)


ORDERS = (("z", "y", "x", 1), ("y", "x", "z", 0), ("x", "z", "y", 0))


class GradScatter:
    def __init__(self, place, sender, grads, widths, bufs, final, local_sems):
        self.place, self.sender, self.grads = place, sender, grads
        self.bufs, self.final, self.local_sems = bufs, final, local_sems
        self.parts = range(len(widths))
        self.cols = [(sum(widths[:part]), widths[part]) for part in self.parts]

    @staticmethod
    def scratch(widths):
        shapes = []
        for width in widths:
            shapes += [
                pltpu.VMEM((RING, RING, PIECE, width), BF16),
                pltpu.VMEM((3, RING, RING, PIECE, width), BF16),
                pltpu.VMEM((RING, RING, PIECE, width), BF16),
                pltpu.VMEM((3, PIECE, width), BF16),
            ]
        return shapes

    def cut(self, part, step):
        axis = ORDERS[part][0]
        index = self.place.block(axis, step)
        cols = pl.ds(*self.cols[part])
        if axis == "x":
            return self.grads.at[index, :, :, :, cols]
        if axis == "z":
            return self.grads.at[:, index, :, :, cols]
        return self.grads.at[:, :, index, :, cols]

    def start(self):
        self.loads, self.one, self.two, self.three = [], [], {}, {}
        for part in self.parts:
            self.one.append(self.sender.ring(
                ORDERS[part][0], lambda step: self.cut(part, step), lambda step: self.bufs[part][1].at[step - 1]))
        for part in self.parts:
            load = pltpu.make_async_copy(self.cut(part, 0), self.bufs[part][0], self.local_sems.at[part])
            load.start()
            self.loads.append(load)

    def second(self):
        for part in self.parts:
            self.loads[part].wait()
            wait_all(self.one[part])
            mine, first, second, _ = self.bufs[part]

            @pl.loop(0, RING)
            def _(a):
                for b in range(RING):
                    total = mine[a, b].astype(F32)
                    for k in range(3):
                        total = total + first[k, a, b].astype(F32)
                    mine[a, b] = total.astype(BF16)

            axis, spot = ORDERS[part][1], ORDERS[part][3]

            def source(step):
                index = self.place.block(axis, step)
                return mine.at[:, index] if spot else mine.at[index]

            self.two[part] = self.sender.ring(axis, source, lambda step: second.at[step - 1])

    def third(self):
        for part in self.parts:
            wait_all(self.two[part])
            mine, _, second, third = self.bufs[part]
            axis, spot = ORDERS[part][1], ORDERS[part][3]
            own = self.place.block(axis, 0)
            for other in range(RING):
                total = mine[(other, own) if spot else (own, other)].astype(F32)
                for k in range(3):
                    total = total + second[k, other].astype(F32)
                second[3, other] = total.astype(BF16)
            axis = ORDERS[part][2]
            self.three[part] = self.sender.ring(
                axis, lambda step: second.at[3, self.place.block(axis, step)], lambda step: third.at[step - 1])

    def finish(self):
        for part in self.parts:
            wait_all(self.three[part])
            _, _, second, third = self.bufs[part]
            total = second[3, self.place.block(ORDERS[part][2], 0)].astype(F32)
            for k in range(3):
                total = total + third[k].astype(F32)
            start, width = self.cols[part]
            self.final[:, start : start + width] = total.astype(BF16)


class PlaneGather:
    COPIES = 12

    def __init__(self, place, sender, final, out, local_sem):
        self.place, self.sender, self.final, self.out, self.local_sem = place, sender, final, out, local_sem

    def start(self):
        z, y = self.place.pos["z"], self.place.pos["y"]
        self.store = pltpu.make_async_copy(self.final, self.out.at[z, y], self.local_sem)
        self.store.start()
        self.near = []
        for part, axis in enumerate("yz"):
            cols = pl.ds(part * HALF, HALF)
            self.near.append(self.sender.ring(
                axis, lambda step: self.final.at[:, cols], lambda step: self.out.at[z, y, :, cols]))

    def second(self):
        z, y = self.place.pos["z"], self.place.pos["y"]
        self.store.wait()
        wait_all(self.near[0])
        line = lambda step: self.out.at[z, :, :, pl.ds(0, HALF)]
        self.far = self.sender.ring("z", line, line)
        wait_all(self.near[1])
        row = lambda step: self.out.at[:, y, :, pl.ds(HALF, HALF)]
        self.far += self.sender.ring("y", row, row)

    def finish(self):
        wait_all(self.far)


def gain_step(place, sender, gains, bufs, index, axis):
    copies = sender.ring(axis, lambda step: gains.at[index], lambda step: bufs.at[index, step - 1])

    def finish():
        wait_all(copies)
        gains[index + 1] = (gains[index] + bufs[index, 1]) + (bufs[index, 0] + bufs[index, 2])

    return finish


def grad_works(place, sender, grads, widths, bufs, finals, outs, local_sems):
    parts = len(widths)
    works, planes = [], []
    for i, grad in enumerate(grads):
        mine = bufs[4 * parts * i : 4 * parts * (i + 1)]
        mine = [mine[4 * part : 4 * part + 4] for part in range(parts)]
        works.append(GradScatter(place, sender, grad, widths, mine, finals.at[i], local_sems.at[i]))
        planes.append(PlaneGather(place, sender, finals.at[i], outs[i], local_sems.at[i, 3]))
    return works, planes


def comm_scratch(count, widths, extra):
    copies = (9 * len(widths) + PlaneGather.COPIES) * count + extra
    scratch = [
        pltpu.VMEM((count, PIECE, WIDTH), BF16),
        pltpu.SemaphoreType.DMA((copies,)),
        pltpu.SemaphoreType.DMA((copies,)),
        pltpu.SemaphoreType.DMA((count, 4)),
    ]
    for _ in range(count):
        scratch += GradScatter.scratch(widths)
    return scratch


ATT_WIDTHS = (768, 768)
MLP_WIDTHS = (640, 512, 384)


def last_kernel(grad, gain_in, out, gain_out, gains, gain_bufs, finals, send_sems, recv_sems, local_sems, *bufs):
    place = Place()
    sender = Sender(place, send_sems, recv_sems)
    place.enter()
    (work,), (plane,) = grad_works(place, sender, [grad], ATT_WIDTHS, bufs, finals, [out], local_sems)
    gains[0] = gain_in[...]
    gain_finish = gain_step(place, sender, gains, gain_bufs, 0, "z")
    work.start()
    gain_finish()
    gain_finish = gain_step(place, sender, gains, gain_bufs, 1, "y")
    work.second()
    gain_finish()
    gain_finish = gain_step(place, sender, gains, gain_bufs, 2, "x")
    work.third()
    work.finish()
    plane.start()
    gain_finish()
    gain_out[...] = gains[3]
    plane.second()
    plane.finish()
    sender.drain()


def scatter_last(grad, gains):
    return pl.pallas_call(
        last_kernel,
        out_shape=[jax.ShapeDtypeStruct(grad.shape[1:], BF16), jax.ShapeDtypeStruct(gains.shape, F32)],
        in_specs=[ANY_SPEC, VMEM_SPEC],
        out_specs=[ANY_SPEC, VMEM_SPEC],
        scratch_shapes=[pltpu.VMEM((4,) + gains.shape, F32), pltpu.VMEM((3, 3) + gains.shape, F32)] + comm_scratch(1, ATT_WIDTHS, 9),
        compiler_params=pltpu.CompilerParams(collective_id=4, has_side_effects=True, vmem_limit_bytes=32 << 20),
        name="scatter_last",
    )(grad, gains)


def back_kernel(
    hidden_act, grad_pre, grad_y, normed_b_in, part_b, x_one_in, qkv_in, seg, seg_col, attn, w_att, normed_a_in, x_in, gain_a, gain_b,
    out_up, out_down, grad_up, grad_down, grad_att, grad_x, gain_grad_a, gain_grad_b,
    lhs, qkv, grad_attn, grad_one, normed, w_qkv, w_out, part, other, stage, load_sems, lhs_sems, stage_sems, free_sem,
    finals, send_sems, recv_sems, local_sems, *bufs,
):
    place = Place()
    sender = Sender(place, send_sems, recv_sems)
    loads = {}

    def load(name, source, target, index):
        copy = pltpu.make_async_copy(source, target, load_sems.at[index])
        copy.start()
        loads.setdefault(name, []).append(copy)

    def ready(name):
        for copy in loads[name]:
            copy.wait()

    load("one", grad_y, grad_one, 0)
    load("part", part_b, part, 13)
    load("normed_b", normed_b_in, normed, 6)
    load("qkv", qkv_in, qkv, 5)
    for shard in range(RING):
        load("out", w_att.at[shard, pl.ds(QKV_ROWS, OUT_ROWS)], w_out.at[pl.ds(shard * OUT_ROWS, OUT_ROWS)], 1 + shard)
    for shard in range(RING):
        load("w", w_att.at[shard, pl.ds(0, QKV_ROWS)], w_qkv.at[pl.ds(shard * QKV_ROWS, QKV_ROWS)], 7 + shard)
    place.enter(core=True)
    works, planes = grad_works(place, sender, [grad_down, grad_up], MLP_WIDTHS, bufs, finals, [out_down, out_up], local_sems)
    ready("part")
    early = sender.swap(part, other)

    blocks = RING * RING

    def fetch(source, index, slot):
        rows = pl.ds(pl.multiple_of(index * OUT_ROWS, OUT_ROWS), OUT_ROWS)
        return pltpu.make_async_copy(source.at[rows], lhs.at[slot], lhs_sems.at[slot])

    def place_block(target, index, slot):
        return pltpu.make_async_copy(stage.at[slot], target.at[lax.div(index, RING), lax.rem(index, RING)], stage_sems.at[slot])

    def weight_grad(source, rhs, target):
        fetch(source, 0, 0).start()

        @pl.loop(0, blocks)
        def _(index):
            slot = lax.rem(index, 2)
            fetch(source, index, slot).wait()

            @pl.when(index + 1 < blocks)
            def _():
                fetch(source, index + 1, 1 - slot).start()

            @pl.when(index >= 2)
            def _():
                place_block(target, index - 2, slot).wait()

            stage[slot] = dot_plain(lhs[slot], rhs[...]).astype(BF16).reshape(RING, PIECE, WIDTH)
            place_block(target, index, slot).start()

        for index in (blocks - 2, blocks - 1):
            place_block(target, index, index % 2).wait()

    ready("one")
    weight_grad(hidden_act, grad_one, grad_down)
    works[0].start()
    ready("normed_b")
    weight_grad(grad_pre, normed, grad_up)
    works[1].start()

    load("x_one", x_one_in, normed, 14)
    gain_grad_a[...] = jnp.zeros_like(gain_grad_a)
    gain_grad_b[...] = jnp.zeros_like(gain_grad_b)
    early.wait_recv()
    early.wait_send()
    ready("x_one")

    def norm_back(rows, gain, gain_grad):
        x_hat, inv_std = norm_stats(normed[rows].astype(F32))
        grad = (part[rows].astype(F32) + other[rows].astype(F32)).astype(BF16).astype(F32)
        gain_grad[...] += jnp.sum(grad * x_hat, axis=0, keepdims=True)
        grad_hat = grad * gain[...].astype(F32)
        mean_one = jnp.mean(grad_hat, axis=-1, keepdims=True)
        mean_two = jnp.mean(grad_hat * x_hat, axis=-1, keepdims=True)
        back = inv_std * (grad_hat - mean_one - x_hat * mean_two)
        return (grad_one[rows].astype(F32) + back).astype(BF16)

    def second_norm(rows):
        grad_one[rows] = norm_back(rows, gain_b, gain_grad_b)

    token_blocks(second_norm)
    pl.semaphore_signal(free_sem, inc=1, device_id=place.sibling(), device_id_type=MESH_ID)
    load("normed_a", normed_a_in, normed, 11)

    ready("out")
    for shard in range(RING):
        rows = pl.ds(shard * OUT_ROWS, OUT_ROWS)
        grad_attn[rows] = dot_rows(w_out[rows], grad_one[...]).astype(BF16)
    ready("qkv")
    attention_backward(qkv, seg, seg_col, grad_attn, qkv, 0, 10)
    works[0].second()
    attention_backward(qkv, seg, seg_col, grad_attn, qkv, 10, 16)

    ready("w")
    pl.semaphore_wait(free_sem, 1)
    swaps = []
    for index in range(TOKENS // STEP):
        rows = pl.ds(index * STEP, STEP)
        part[rows] = dot_cols(qkv[:, index * STEP : (index + 1) * STEP], w_qkv[...]).astype(BF16)
        swaps.append(sender.swap(part.at[rows], other.at[rows]))
    works[1].second()
    works[0].third()

    stores = []

    def put(rows, shard, start):
        slot = len(stores) % 2
        if len(stores) >= 2:
            stores[-2].wait()
        stage[slot] = rows.astype(BF16).reshape(RING, PIECE, WIDTH)
        copy = pltpu.make_async_copy(stage.at[slot], grad_att.at[shard, start // OUT_ROWS], stage_sems.at[slot])
        copy.start()
        stores.append(copy)

    for shard in range(RING):
        put(dot_plain(attn[shard * OUT_ROWS : (shard + 1) * OUT_ROWS], grad_one[...]), shard, QKV_ROWS)
    ready("normed_a")
    for shard in range(RING):
        for block in range(3):
            start = shard * QKV_ROWS + block * OUT_ROWS
            put(dot_plain(qkv[start : start + OUT_ROWS], normed[...]), shard, block * OUT_ROWS)
    for store in stores[-2:]:
        store.wait()
    load("x", x_in, normed, 15)
    works[1].third()
    ready("x")
    wait_all(swaps)
    for copy in swaps:
        copy.wait_send()

    def first_norm(rows):
        part[rows] = norm_back(rows, gain_a, gain_grad_a)

    token_blocks(first_norm)
    result = pltpu.make_async_copy(part, grad_x, load_sems.at[12])
    result.start()
    for work, plane in zip(works, planes):
        work.finish()
        plane.start()
    for plane in planes:
        plane.second()
    for plane in planes:
        plane.finish()
    result.wait()
    sender.drain()


def backward(*operands):
    tokens = (TOKENS, WIDTH)
    piece = jax.ShapeDtypeStruct((RING, RING, PIECE, WIDTH), BF16)
    grid = jax.ShapeDtypeStruct((RING, RING, RING, PIECE, WIDTH), BF16)
    return pl.pallas_call(
        back_kernel,
        out_shape=[
            piece, piece, grid, grid, grid,
            jax.ShapeDtypeStruct(tokens, BF16),
            jax.ShapeDtypeStruct((1, WIDTH), F32), jax.ShapeDtypeStruct((1, WIDTH), F32),
        ],
        in_specs=[ANY_SPEC] * 7 + [VMEM_SPEC] * 3 + [ANY_SPEC] * 3 + [VMEM_SPEC] * 2,
        out_specs=[ANY_SPEC] * 6 + [VMEM_SPEC] * 2,
        scratch_shapes=[
            pltpu.VMEM((2, OUT_ROWS, TOKENS), BF16),
            pltpu.VMEM((RING * QKV_ROWS, TOKENS), BF16),
            pltpu.VMEM((RING * OUT_ROWS, TOKENS), BF16),
            pltpu.VMEM(tokens, BF16),
            pltpu.VMEM(tokens, BF16),
            pltpu.VMEM((RING * QKV_ROWS, WIDTH), BF16),
            pltpu.VMEM((RING * OUT_ROWS, WIDTH), BF16),
            pltpu.VMEM(tokens, BF16),
            pltpu.VMEM(tokens, BF16),
            pltpu.VMEM((2, RING, PIECE, WIDTH), BF16),
            pltpu.SemaphoreType.DMA((16,)),
            pltpu.SemaphoreType.DMA((2,)),
            pltpu.SemaphoreType.DMA((2,)),
            pltpu.SemaphoreType.REGULAR,
        ] + comm_scratch(2, MLP_WIDTHS, TOKENS // STEP + 1),
        compiler_params=pltpu.CompilerParams(collective_id=3, has_side_effects=True, vmem_limit_bytes=67043328),
        name="backward",
    )(*operands)


def solution(mesh):
    batch_spec = P(("pod", "dp"), None, None)
    seg_spec = P(("pod", "dp"), None)

    def local_step(x_in, seg_ids, gain_one, gain_two, w_qkv, w_out, w_up, w_down, grad_y):
        batch_loc, seq_len, hidden = x_in.shape
        heads_loc, head_dim = w_out.shape[:2]
        rows_loc = batch_loc // RING
        tokens = rows_loc * seq_len
        shard_rows = w_up.shape[1]
        qkv_cols = w_qkv.shape[1]
        x_pos = lax.axis_index("tp") // 2

        def own_rows(array):
            return lax.dynamic_slice_in_dim(array, x_pos * rows_loc, rows_loc, axis=0)

        def grid_of(own):
            return own.reshape(RING, RING, PIECE, hidden)

        own_att = grid_of(jnp.concatenate([w_qkv.T, w_out.reshape(heads_loc * head_dim, hidden)], axis=0))
        own_up = grid_of(w_up.T)
        own_down = grid_of(w_down)
        x_rows = own_rows(x_in).reshape(tokens, hidden)
        seg_rows = own_rows(seg_ids)
        seg_row, seg_col = seg_rows[:, None, :], seg_rows[:, :, None]
        grad_rows = own_rows(grad_y).reshape(tokens, hidden)
        w_att, up_t, down, qkv_t, attn_flat, normed_a, x_one, normed_b = front(
            own_att, own_up, own_down, x_rows, gain_one[None], gain_two[None], seg_row, seg_col)
        up_t = up_t.reshape(RING * shard_rows, hidden)
        down = down.reshape(RING * shard_rows, hidden)

        def pair_sum(part):
            return part.astype(F32) + core_swap(part).astype(F32)

        pre_act = dot_nt(up_t, normed_b)
        act_val, gelu_pull = jax.vjp(gelu_tanh, pre_act)
        hidden_act = act_val.astype(BF16)
        part_two = dot_tn(hidden_act, down).astype(BF16)
        sum_two = pair_sum(part_two).astype(BF16)
        y_rows = (x_one.astype(F32) + sum_two.astype(F32)).astype(BF16)

        grad_hidden = dot_nt(down, grad_rows).astype(BF16)
        grad_pre = gelu_pull(grad_hidden.astype(F32))[0].astype(BF16)

        part_b = dot_tn(grad_pre, up_t).astype(BF16)
        grad_up_own, grad_down_own, _, _, grad_att, grad_x, gain_grad_one, gain_grad_two = backward(
            hidden_act, grad_pre, grad_rows, normed_b, part_b, x_one, qkv_t, seg_row, seg_col, attn_flat,
            w_att.reshape(RING, shard_rows, hidden), normed_a, x_rows, gain_one[None], gain_two[None])
        gains = jnp.concatenate([gain_grad_one, gain_grad_two, jnp.zeros((6, hidden), F32)], axis=0)
        grad_att_own, gains = scatter_last(grad_att, gains)
        grad_att_own = grad_att_own.reshape(shard_rows, hidden)

        def spread(rows):
            core = lax.axis_index("tp") % 2
            mine = lax.dynamic_slice_in_dim(rows.reshape(rows_loc, seq_len, hidden), core, 1, axis=0)
            return lax.all_gather(mine, "tp", axis=0, tiled=True)

        return (
            spread(y_rows),
            spread(grad_x),
            gains[0].astype(BF16),
            gains[1].astype(BF16),
            grad_att_own[:qkv_cols].T,
            grad_att_own[qkv_cols:].reshape(heads_loc, head_dim, hidden),
            grad_up_own.reshape(shard_rows, hidden).T,
            grad_down_own.reshape(shard_rows, hidden),
        )

    return jax.shard_map(
        local_step,
        mesh=mesh,
        in_specs=(batch_spec, seg_spec, P(None), P(None), P(None, "tp"), P("tp", None, None), P(None, "tp"), P("tp", None), batch_spec),
        out_specs=(batch_spec, batch_spec, P("pod"), P("pod"), P("pod", "tp"), P(("pod", "tp"), None, None), P("pod", "tp"), P(("pod", "tp"), None)),
        check_vma=False,
    )
```

```python
import functools

import jax
import jax.numpy as jnp
from jax import lax
from jax.experimental import pallas as pl
from jax.experimental.pallas import tpu as pltpu
from jax.sharding import PartitionSpec as P

EPS_NORM = 1e-5
NEG_LARGE = -1e30
F32 = jnp.float32
BF16 = jnp.bfloat16
RING = 4


def gelu_tanh(values):
    return jax.nn.gelu(values, approximate=True)


def dot_nt(lhs, rhs):
    return lax.dot_general(lhs, rhs, (((lhs.ndim - 1,), (rhs.ndim - 1,)), ((), ())), preferred_element_type=F32)


def dot_tn(lhs, rhs):
    return lax.dot_general(lhs, rhs, (((0,), (0,)), ((), ())), preferred_element_type=F32)


def core_swap(array):
    return lax.ppermute(array, "tp", [(i, i ^ 1) for i in range(8)])


THIRD = 512
PIECE = 48
WIDTH = 1536
HALF = WIDTH // 2
MESH_ID = pl.DeviceIdType.MESH


class Place:
    def __init__(self):
        plane = lax.axis_index("dp")
        column = lax.axis_index("tp")
        self.pos = {"z": lax.div(plane, RING), "y": lax.rem(plane, RING), "x": lax.div(column, 2)}
        self.core = lax.rem(column, 2)

    def ahead(self, axis, step):
        return lax.rem(self.pos[axis] + step, RING)

    def peer(self, axis, step):
        if axis == "x":
            return {"tp": self.ahead("x", step) * 2 + self.core}
        if axis == "y":
            return {"dp": self.pos["z"] * RING + self.ahead("y", step)}
        return {"dp": self.ahead("z", step) * RING + self.pos["y"]}

    def block(self, axis, step):
        return step if axis == "x" else self.ahead(axis, step)

    def sibling(self):
        return {"tp": self.pos["x"] * 2 + 1 - self.core}

    def enter(self, core=False):
        barrier = pltpu.get_barrier_semaphore()
        if core:
            pl.semaphore_signal(barrier, inc=1, device_id=self.sibling(), device_id_type=MESH_ID)
        self.signal_rings(barrier)
        pl.semaphore_wait(barrier, 9 + core)

    def signal_rings(self, semaphore):
        for axis in "xyz":
            for step in range(1, RING):
                pl.semaphore_signal(semaphore, inc=1, device_id=self.peer(axis, step), device_id_type=MESH_ID)


class Sender:
    def __init__(self, place, send_sems, recv_sems):
        self.place, self.send_sems, self.recv_sems = place, send_sems, recv_sems
        self.used = 0
        self.copies = []

    def ring(self, axis, source, target):
        started = []
        for step in range(1, RING):
            copy = pltpu.make_async_remote_copy(
                src_ref=source(step), dst_ref=target(step),
                send_sem=self.send_sems.at[self.used], recv_sem=self.recv_sems.at[self.used],
                device_id=self.place.peer(axis, step), device_id_type=MESH_ID,
            )
            copy.start()
            self.used += 1
            started.append(copy)
        self.copies += started
        return started

    def swap(self, source, target):
        copy = pltpu.make_async_remote_copy(
            src_ref=source, dst_ref=target,
            send_sem=self.send_sems.at[self.used], recv_sem=self.recv_sems.at[self.used],
            device_id=self.place.sibling(), device_id_type=MESH_ID,
        )
        copy.start()
        self.used += 1
        return copy

    def settle(self, copies):
        for copy in copies:
            copy.wait_send()
        done = {id(copy) for copy in copies}
        self.copies = [copy for copy in self.copies if id(copy) not in done]

    def drain(self):
        for copy in self.copies:
            copy.wait_send()


def wait_all(copies):
    for copy in copies:
        copy.wait_recv()


ANY_SPEC = pl.BlockSpec(memory_space=pl.ANY)
VMEM_SPEC = pl.BlockSpec(memory_space=pltpu.VMEM)
QKV_ROWS = 576
OUT_ROWS = 192
SEQ = 512
TOKENS = 2 * SEQ
STEP = 256
NORM_STEP = 128
BLOCK = 256
HEAD = 96
SCALE = HEAD ** -0.5


def head_slice(ref, index, kind, lo, hi, kinds=3):
    head, row = lax.div(index, 2), lax.rem(index, 2)
    start = pl.multiple_of((head * kinds + kind) * HEAD, 32)
    return ref.at[pl.ds(start, HEAD), pl.ds(pl.multiple_of(row * SEQ + lo, 128), hi - lo)]


def dot_cols(lhs, rhs):
    return lax.dot_general(lhs, rhs, (((0,), (0,)), ((), ())), preferred_element_type=F32)


def dot_rows(lhs, rhs):
    return lax.dot_general(lhs, rhs, (((1,), (1,)), ((), ())), preferred_element_type=F32)


def dot_plain(lhs, rhs):
    return lax.dot_general(lhs, rhs, (((1,), (0,)), ((), ())), preferred_element_type=F32)


def probs_block(k_t, q_t, seg, seg_col, row, first):
    keys = first + BLOCK
    scores = dot_cols(k_t, q_t) * SCALE
    query = lax.broadcasted_iota(jnp.int32, (keys, BLOCK), 1) + first
    key = lax.broadcasted_iota(jnp.int32, (keys, BLOCK), 0)
    same = seg[row, :, first : first + BLOCK] == seg_col[row, :keys, :]
    scores = jnp.where((query >= key) & same, scores, NEG_LARGE)
    weights = jnp.exp(scores - jnp.max(scores, axis=0, keepdims=True))
    return weights * (1.0 / jnp.sum(weights, axis=0, keepdims=True))


def attention_forward(qkv, seg, seg_col, out, start, stop):
    @pl.loop(start, stop)
    def _(index):
        row = lax.rem(index, 2)
        for first in range(0, SEQ, BLOCK):
            keys = first + BLOCK
            probs = probs_block(
                head_slice(qkv, index, 1, 0, keys)[...], head_slice(qkv, index, 0, first, keys)[...], seg, seg_col, row, first)
            value = lax.dot_general(
                head_slice(qkv, index, 2, 0, keys)[...], probs.astype(BF16), (((1,), (0,)), ((), ())), preferred_element_type=F32)
            head_slice(out, index, 0, first, keys, kinds=1)[...] = value.astype(BF16)


def attention_backward(qkv, seg, seg_col, grad, out, start, stop):
    @pl.loop(start, stop)
    def _(index):
        row = lax.rem(index, 2)
        grads = []
        for first in range(0, SEQ, BLOCK):
            keys = first + BLOCK
            q_t = head_slice(qkv, index, 0, first, keys)[...]
            k_t = head_slice(qkv, index, 1, 0, keys)[...]
            g_t = head_slice(grad, index, 0, first, keys, kinds=1)[...]
            probs = probs_block(k_t, q_t, seg, seg_col, row, first)
            grad_probs = dot_cols(head_slice(qkv, index, 2, 0, keys)[...], g_t)
            grad_scores = probs * (grad_probs - jnp.sum(grad_probs * probs, axis=0, keepdims=True))
            low = (grad_scores * SCALE).astype(BF16)
            grad_q = lax.dot_general(k_t, low, (((1,), (0,)), ((), ())), preferred_element_type=F32)
            head_slice(out, index, 0, first, keys)[...] = grad_q.astype(BF16)
            grads.append((dot_rows(q_t, low), dot_rows(g_t, probs.astype(BF16))))
        for i in range(2):
            whole = grads[1][i]
            head_slice(out, index, 1 + i, 0, BLOCK)[...] = (grads[0][i] + whole[:, :BLOCK]).astype(BF16)
            head_slice(out, index, 1 + i, BLOCK, SEQ)[...] = whole[:, BLOCK:].astype(BF16)


class WeightGather:
    COPIES = 21

    def __init__(self, place, sender, own, out):
        self.place, self.sender, self.own, self.out = place, sender, own, out

    def spot(self, cols):
        z, y = self.place.pos["z"], self.place.pos["y"]
        return lambda step: self.out.at[pl.ds(1, 3), z, y, :, cols]

    def start(self):
        z, y = self.place.pos["z"], self.place.pos["y"]
        self.near = []
        for part in range(2):
            cols = pl.ds(part * THIRD, THIRD)
            self.near.append(self.sender.ring(
                "x", lambda step: self.own.at[z, y, :, cols], lambda step: self.out.at[RING - step, z, y, :, cols]))

    def start_whole(self):
        cols = pl.ds(2 * THIRD, THIRD)
        self.whole = self.sender.ring(
            "x", lambda step: self.own.at[:, :, :, cols], lambda step: self.out.at[RING - step, :, :, :, cols])

    def second(self):
        self.mid = []
        for part, axis in enumerate("yz"):
            wait_all(self.near[part])
            spot = self.spot(pl.ds(part * THIRD, THIRD))
            self.mid.append(self.sender.ring(axis, spot, spot))

    def third(self):
        z, y = self.place.pos["z"], self.place.pos["y"]
        wait_all(self.mid[0])
        line = lambda step: self.out.at[pl.ds(1, 3), z, :, :, pl.ds(0, THIRD)]
        self.far = self.sender.ring("z", line, line)
        wait_all(self.mid[1])
        row = lambda step: self.out.at[pl.ds(1, 3), :, y, :, pl.ds(THIRD, THIRD)]
        self.far += self.sender.ring("y", row, row)

    def finish(self):
        wait_all(self.far)
        wait_all(self.whole)


def norm_stats(x_f32):
    centered = x_f32 - jnp.mean(x_f32, axis=-1, keepdims=True)
    inv_std = lax.rsqrt(jnp.mean(centered * centered, axis=-1, keepdims=True) + EPS_NORM)
    return centered * inv_std, inv_std


def token_blocks(body):
    @pl.loop(0, TOKENS // NORM_STEP)
    def _(index):
        body(pl.ds(pl.multiple_of(index * NORM_STEP, NORM_STEP), NORM_STEP))


def front_kernel(
    own_att, own_up, own_down, x_in, gain_a, gain_b, seg, seg_col,
    w_att, w_up, w_down, qkv_out, attn_out, normed_a_out, x_one_out, normed_b_out,
    weights, stage, x_one, normed, qkv, attn, part, other, load_sems, send_sems, recv_sems,
):
    place = Place()
    sender = Sender(place, send_sems, recv_sems)

    def copy(source, target, index):
        started = pltpu.make_async_copy(source, target, load_sems.at[index])
        started.start()
        return started

    loads = [copy(x_in, x_one, 0), copy(own_att, weights.at[0], 1), copy(own_up, stage.at[0], 2), copy(own_down, stage.at[1], 3)]
    place.enter(core=True)
    att = WeightGather(place, sender, own_att, w_att)
    mlp = [WeightGather(place, sender, own_up, w_up), WeightGather(place, sender, own_down, w_down)]
    att.start()
    att.start_whole()
    for gather in mlp:
        gather.start()
    for gather in mlp:
        gather.start_whole()
    loads[0].wait()

    def first_norm(rows):
        x_hat, _ = norm_stats(x_one[rows].astype(F32))
        normed[rows] = (x_hat * gain_a[...].astype(F32)).astype(BF16)

    token_blocks(first_norm)
    results = [copy(normed, normed_a_out, 4)]
    att.second()
    for load in loads[1:]:
        load.wait()
    results += [copy(weights.at[0], w_att.at[0], 5), copy(stage.at[0], w_up.at[0], 6), copy(stage.at[1], w_down.at[0], 7)]

    def project(start, stop):
        @pl.loop(start, stop)
        def _(index):
            block = weights[lax.div(index, 3), lax.rem(index, 3)].reshape(OUT_ROWS, WIDTH)
            qkv[pl.ds(pl.multiple_of(index * OUT_ROWS, OUT_ROWS), OUT_ROWS)] = dot_rows(block, normed[...]).astype(BF16)

    project(0, 3)
    att.third()
    for gather in mlp:
        gather.second()
    att.finish()
    others = [copy(w_att.at[shard], weights.at[shard], 7 + shard) for shard in range(1, RING)]
    for load in others:
        load.wait()
    project(3, 12)
    results.append(copy(qkv, qkv_out, 11))
    attention_forward(qkv, seg, seg_col, attn, 0, 6)
    for gather in mlp:
        gather.third()
    attention_forward(qkv, seg, seg_col, attn, 6, 16)
    results.append(copy(attn, attn_out, 12))
    swaps = []
    for index in range(TOKENS // STEP):
        rows = pl.ds(index * STEP, STEP)
        total = None
        for shard in range(RING):
            block = weights[shard, 3].reshape(OUT_ROWS, WIDTH)
            term = dot_cols(attn[shard * OUT_ROWS : (shard + 1) * OUT_ROWS, index * STEP : (index + 1) * STEP], block)
            total = term if total is None else total + term
        part[rows] = total.astype(BF16)
        swaps.append(sender.swap(part.at[rows], other.at[rows]))
    results[0].wait()
    wait_all(swaps)

    def second_norm(rows):
        summed = (part[rows].astype(F32) + other[rows].astype(F32)).astype(BF16)
        x_new = (x_one[rows].astype(F32) + summed.astype(F32)).astype(BF16)
        x_one[rows] = x_new
        x_hat, _ = norm_stats(x_new.astype(F32))
        normed[rows] = (x_hat * gain_b[...].astype(F32)).astype(BF16)

    token_blocks(second_norm)
    results += [copy(x_one, x_one_out, 13), copy(normed, normed_b_out, 14)]
    for gather in mlp:
        gather.finish()
    for result in results[1:]:
        result.wait()
    for swap in swaps:
        swap.wait_send()
    sender.drain()


def front(own_att, own_up, own_down, x_rows, gain_a, gain_b, seg, seg_col):
    tokens = (TOKENS, WIDTH)
    gathered = jax.ShapeDtypeStruct((RING,) + own_att.shape, BF16)
    rows = jax.ShapeDtypeStruct(tokens, BF16)
    copies = 3 * WeightGather.COPIES + TOKENS // STEP
    return pl.pallas_call(
        front_kernel,
        out_shape=[
            gathered, gathered, gathered,
            jax.ShapeDtypeStruct((RING * QKV_ROWS, TOKENS), BF16), jax.ShapeDtypeStruct((RING * OUT_ROWS, TOKENS), BF16),
            rows, rows, rows,
        ],
        in_specs=[ANY_SPEC] * 4 + [VMEM_SPEC] * 4,
        out_specs=[ANY_SPEC] * 8,
        scratch_shapes=[
            pltpu.VMEM(gathered.shape, BF16),
            pltpu.VMEM((2,) + own_att.shape, BF16),
            pltpu.VMEM(tokens, BF16),
            pltpu.VMEM(tokens, BF16),
            pltpu.VMEM((RING * QKV_ROWS, TOKENS), BF16),
            pltpu.VMEM((RING * OUT_ROWS, TOKENS), BF16),
            pltpu.VMEM(tokens, BF16),
            pltpu.VMEM(tokens, BF16),
            pltpu.SemaphoreType.DMA((15,)),
            pltpu.SemaphoreType.DMA((copies,)),
            pltpu.SemaphoreType.DMA((copies,)),
        ],
        compiler_params=pltpu.CompilerParams(collective_id=1, has_side_effects=True, vmem_limit_bytes=56 << 20),
        name="front",
    )(own_att, own_up, own_down, x_rows, gain_a, gain_b, seg, seg_col)


ORDERS = (("z", "y", "x", 1), ("y", "x", "z", 0), ("x", "z", "y", 0))


class GradScatter:
    def __init__(self, place, sender, grads, widths, bufs, final, local_sems):
        self.place, self.sender, self.grads = place, sender, grads
        self.bufs, self.final, self.local_sems = bufs, final, local_sems
        self.parts = range(len(widths))
        self.cols = [(sum(widths[:part]), widths[part]) for part in self.parts]

    @staticmethod
    def scratch(widths):
        shapes = []
        for width in widths:
            shapes += [
                pltpu.VMEM((RING, RING, PIECE, width), BF16),
                pltpu.VMEM((3, RING, RING, PIECE, width), BF16),
                pltpu.VMEM((RING, RING, PIECE, width), BF16),
                pltpu.VMEM((3, PIECE, width), BF16),
            ]
        return shapes

    def cut(self, part, step):
        axis = ORDERS[part][0]
        index = self.place.block(axis, step)
        cols = pl.ds(*self.cols[part])
        if axis == "x":
            return self.grads.at[index, :, :, :, cols]
        if axis == "z":
            return self.grads.at[:, index, :, :, cols]
        return self.grads.at[:, :, index, :, cols]

    def start(self):
        self.loads, self.one, self.two, self.three = [], [], {}, {}
        for part in self.parts:
            self.one.append(self.sender.ring(
                ORDERS[part][0], lambda step: self.cut(part, step), lambda step: self.bufs[part][1].at[step - 1]))
        for part in self.parts:
            load = pltpu.make_async_copy(self.cut(part, 0), self.bufs[part][0], self.local_sems.at[part])
            load.start()
            self.loads.append(load)

    def second(self):
        for part in self.parts:
            self.loads[part].wait()
            wait_all(self.one[part])
            mine, first, second, _ = self.bufs[part]

            @pl.loop(0, RING)
            def _(a):
                for b in range(RING):
                    total = mine[a, b].astype(F32)
                    for k in range(3):
                        total = total + first[k, a, b].astype(F32)
                    mine[a, b] = total.astype(BF16)

            axis, spot = ORDERS[part][1], ORDERS[part][3]

            def source(step):
                index = self.place.block(axis, step)
                return mine.at[:, index] if spot else mine.at[index]

            self.two[part] = self.sender.ring(axis, source, lambda step: second.at[step - 1])

    def third(self):
        for part in self.parts:
            wait_all(self.two[part])
            mine, _, second, third = self.bufs[part]
            axis, spot = ORDERS[part][1], ORDERS[part][3]
            own = self.place.block(axis, 0)
            for other in range(RING):
                total = mine[(other, own) if spot else (own, other)].astype(F32)
                for k in range(3):
                    total = total + second[k, other].astype(F32)
                second[3, other] = total.astype(BF16)
            axis = ORDERS[part][2]
            self.three[part] = self.sender.ring(
                axis, lambda step: second.at[3, self.place.block(axis, step)], lambda step: third.at[step - 1])

    def finish(self):
        for part in self.parts:
            wait_all(self.three[part])
            _, _, second, third = self.bufs[part]
            total = second[3, self.place.block(ORDERS[part][2], 0)].astype(F32)
            for k in range(3):
                total = total + third[k].astype(F32)
            start, width = self.cols[part]
            self.final[:, start : start + width] = total.astype(BF16)


class PlaneGather:
    COPIES = 12

    def __init__(self, place, sender, final, out, local_sem):
        self.place, self.sender, self.final, self.out, self.local_sem = place, sender, final, out, local_sem

    def start(self):
        z, y = self.place.pos["z"], self.place.pos["y"]
        self.store = pltpu.make_async_copy(self.final, self.out.at[z, y], self.local_sem)
        self.store.start()
        self.near = []
        for part, axis in enumerate("yz"):
            cols = pl.ds(part * HALF, HALF)
            self.near.append(self.sender.ring(
                axis, lambda step: self.final.at[:, cols], lambda step: self.out.at[z, y, :, cols]))

    def second(self):
        z, y = self.place.pos["z"], self.place.pos["y"]
        self.store.wait()
        wait_all(self.near[0])
        line = lambda step: self.out.at[z, :, :, pl.ds(0, HALF)]
        self.far = self.sender.ring("z", line, line)
        wait_all(self.near[1])
        row = lambda step: self.out.at[:, y, :, pl.ds(HALF, HALF)]
        self.far += self.sender.ring("y", row, row)

    def finish(self):
        wait_all(self.far)


def gain_step(place, sender, gains, bufs, index, axis):
    copies = sender.ring(axis, lambda step: gains.at[index], lambda step: bufs.at[index, step - 1])

    def finish():
        wait_all(copies)
        gains[index + 1] = (gains[index] + bufs[index, 1]) + (bufs[index, 0] + bufs[index, 2])

    return finish


def grad_works(place, sender, grads, widths, bufs, finals, outs, local_sems):
    parts = len(widths)
    works, planes = [], []
    for i, grad in enumerate(grads):
        mine = bufs[4 * parts * i : 4 * parts * (i + 1)]
        mine = [mine[4 * part : 4 * part + 4] for part in range(parts)]
        works.append(GradScatter(place, sender, grad, widths, mine, finals.at[i], local_sems.at[i]))
        planes.append(PlaneGather(place, sender, finals.at[i], outs[i], local_sems.at[i, 3]))
    return works, planes


WIDTHS = (640, 640, 256)


def back_kernel(
    hidden_act, grad_pre, grad_y, normed_b_in, part_b, x_one_in, qkv_in, seg, seg_col, attn, w_att, normed_a_in, x_in, gain_a, gain_b,
    out_up, out_down, out_att, grad_up, grad_down, grad_att, grad_x, gain_out,
    lhs, qkv, grad_attn, grad_one, normed, w_qkv, w_out, part, other, stage, load_sems, lhs_sems, stage_sems, free_sem, ring_sem,
    gain_grad_a, gain_grad_b, gains, gain_bufs, finals, send_sems, recv_sems, local_sems, *bufs,
):
    place = Place()
    sender = Sender(place, send_sems, recv_sems)
    loads = {}

    def load(name, source, target, index):
        copy = pltpu.make_async_copy(source, target, load_sems.at[index])
        copy.start()
        loads.setdefault(name, []).append(copy)

    def ready(name):
        for copy in loads[name]:
            copy.wait()

    load("one", grad_y, grad_one, 0)
    load("part", part_b, part, 13)
    load("normed_b", normed_b_in, normed, 6)
    load("qkv", qkv_in, qkv, 5)
    for shard in range(RING):
        load("out", w_att.at[shard, pl.ds(QKV_ROWS, OUT_ROWS)], w_out.at[pl.ds(shard * OUT_ROWS, OUT_ROWS)], 1 + shard)
    for shard in range(RING):
        load("w", w_att.at[shard, pl.ds(0, QKV_ROWS)], w_qkv.at[pl.ds(shard * QKV_ROWS, QKV_ROWS)], 7 + shard)
    place.enter(core=True)
    works, planes = grad_works(place, sender, [grad_down, grad_up], WIDTHS, bufs, finals, [out_down, out_up], local_sems)
    tail = bufs[8 * len(WIDTHS) :]
    reused = [(works[0].bufs[part][0], works[0].bufs[part][1]) + tuple(tail[2 * part : 2 * part + 2]) for part in range(len(WIDTHS))]
    att_work = GradScatter(place, sender, grad_att, WIDTHS, reused, finals.at[2], local_sems.at[2])
    att_plane = PlaneGather(place, sender, finals.at[2], out_att, local_sems.at[2, 3])
    ready("part")
    early = sender.swap(part, other)

    blocks = RING * RING

    def fetch(source, index, slot):
        rows = pl.ds(pl.multiple_of(index * OUT_ROWS, OUT_ROWS), OUT_ROWS)
        return pltpu.make_async_copy(source.at[rows], lhs.at[slot], lhs_sems.at[slot])

    def place_block(target, index, slot):
        return pltpu.make_async_copy(stage.at[slot], target.at[lax.div(index, RING), lax.rem(index, RING)], stage_sems.at[slot])

    def weight_grad(source, rhs, target):
        fetch(source, 0, 0).start()

        @pl.loop(0, blocks)
        def _(index):
            slot = lax.rem(index, 2)
            fetch(source, index, slot).wait()

            @pl.when(index + 1 < blocks)
            def _():
                fetch(source, index + 1, 1 - slot).start()

            @pl.when(index >= 2)
            def _():
                place_block(target, index - 2, slot).wait()

            stage[slot] = dot_plain(lhs[slot], rhs[...]).astype(BF16).reshape(RING, PIECE, WIDTH)
            place_block(target, index, slot).start()

        for index in (blocks - 2, blocks - 1):
            place_block(target, index, index % 2).wait()

    ready("one")
    weight_grad(hidden_act, grad_one, grad_down)
    works[0].start()
    ready("normed_b")
    weight_grad(grad_pre, normed, grad_up)
    works[1].start()

    load("x_one", x_one_in, normed, 14)
    gain_grad_a[...] = jnp.zeros_like(gain_grad_a)
    gain_grad_b[...] = jnp.zeros_like(gain_grad_b)
    early.wait_recv()
    early.wait_send()
    ready("x_one")

    def norm_back(rows, gain, gain_grad):
        x_hat, inv_std = norm_stats(normed[rows].astype(F32))
        grad = (part[rows].astype(F32) + other[rows].astype(F32)).astype(BF16).astype(F32)
        gain_grad[...] += jnp.sum(grad * x_hat, axis=0, keepdims=True)
        grad_hat = grad * gain[...].astype(F32)
        mean_one = jnp.mean(grad_hat, axis=-1, keepdims=True)
        mean_two = jnp.mean(grad_hat * x_hat, axis=-1, keepdims=True)
        back = inv_std * (grad_hat - mean_one - x_hat * mean_two)
        return (grad_one[rows].astype(F32) + back).astype(BF16)

    def second_norm(rows):
        grad_one[rows] = norm_back(rows, gain_b, gain_grad_b)

    token_blocks(second_norm)
    pl.semaphore_signal(free_sem, inc=1, device_id=place.sibling(), device_id_type=MESH_ID)
    load("normed_a", normed_a_in, normed, 11)

    ready("out")
    for shard in range(RING):
        rows = pl.ds(shard * OUT_ROWS, OUT_ROWS)
        grad_attn[rows] = dot_rows(w_out[rows], grad_one[...]).astype(BF16)
    ready("qkv")
    attention_backward(qkv, seg, seg_col, grad_attn, qkv, 0, 10)
    works[0].second()
    place.signal_rings(ring_sem)
    attention_backward(qkv, seg, seg_col, grad_attn, qkv, 10, 16)

    ready("w")
    pl.semaphore_wait(free_sem, 1)
    swaps = []
    for index in range(TOKENS // STEP):
        rows = pl.ds(index * STEP, STEP)
        part[rows] = dot_cols(qkv[:, index * STEP : (index + 1) * STEP], w_qkv[...]).astype(BF16)
        swaps.append(sender.swap(part.at[rows], other.at[rows]))
    works[1].second()
    works[0].third()

    stores = []

    def put(rows, shard, start):
        slot = len(stores) % 2
        if len(stores) >= 2:
            stores[-2].wait()
        stage[slot] = rows.astype(BF16).reshape(RING, PIECE, WIDTH)
        copy = pltpu.make_async_copy(stage.at[slot], grad_att.at[shard, start // OUT_ROWS], stage_sems.at[slot])
        copy.start()
        stores.append(copy)

    for shard in range(RING):
        put(dot_plain(attn[shard * OUT_ROWS : (shard + 1) * OUT_ROWS], grad_one[...]), shard, QKV_ROWS)
    ready("normed_a")
    for shard in range(RING):
        for block in range(3):
            start = shard * QKV_ROWS + block * OUT_ROWS
            put(dot_plain(qkv[start : start + OUT_ROWS], normed[...]), shard, block * OUT_ROWS)
    for store in stores[-2:]:
        store.wait()
    load("x", x_in, normed, 15)
    sender.settle([copy for copies in works[0].two.values() for copy in copies])
    pl.semaphore_wait(ring_sem, 9)
    att_work.start()
    works[1].third()
    ready("x")
    wait_all(swaps)
    for copy in swaps:
        copy.wait_send()

    def first_norm(rows):
        part[rows] = norm_back(rows, gain_a, gain_grad_a)

    token_blocks(first_norm)
    row_of = lambda step: 2 * place.ahead("x", RING - step) + place.core
    mine = part.at[pl.ds(pl.multiple_of(place.core * SEQ, SEQ), SEQ)]
    rows_sent = sender.ring("x", lambda step: mine, lambda step: grad_x.at[row_of(0)])
    results = []
    for i in range(2):
        result = pltpu.make_async_copy(part.at[pl.ds(i * SEQ, SEQ)], grad_x.at[2 * place.pos["x"] + i], load_sems.at[12 + 4 * i])
        result.start()
        results.append(result)
    gains[0] = jnp.zeros_like(gain_out)
    gains[0, 0:1] = gain_grad_a[...]
    gains[0, 1:2] = gain_grad_b[...]
    gain_finish = gain_step(place, sender, gains, gain_bufs, 0, "z")
    for work, plane in zip(works, planes):
        work.finish()
        plane.start()
    gain_finish()
    gain_finish = gain_step(place, sender, gains, gain_bufs, 1, "y")
    att_work.second()
    for plane in planes:
        plane.second()
    gain_finish()
    gain_finish = gain_step(place, sender, gains, gain_bufs, 2, "x")
    att_work.third()
    passed = []
    for step, copy in zip(range(1, RING), rows_sent):
        copy.wait_recv()
        row = grad_x.at[row_of(step)]
        passed.append(sender.swap(row, row))
    att_work.finish()
    att_plane.start()
    gain_finish()
    gain_out[...] = gains[3]
    for plane in planes:
        plane.finish()
    att_plane.second()
    att_plane.finish()
    wait_all(passed)
    for copy in passed:
        copy.wait_send()
    for result in results:
        result.wait()
    sender.drain()


def backward(*operands):
    tokens = (TOKENS, WIDTH)
    piece = jax.ShapeDtypeStruct((RING, RING, PIECE, WIDTH), BF16)
    grid = jax.ShapeDtypeStruct((RING, RING, RING, PIECE, WIDTH), BF16)
    copies = 3 * (9 * len(WIDTHS) + PlaneGather.COPIES) + TOKENS // STEP + 1 + 9 + 6
    tail = [shape for part in range(len(WIDTHS)) for shape in GradScatter.scratch(WIDTHS)[4 * part + 2 : 4 * part + 4]]
    return pl.pallas_call(
        back_kernel,
        out_shape=[
            piece, piece, piece, grid, grid, grid,
            jax.ShapeDtypeStruct((2 * RING, SEQ, WIDTH), BF16),
            jax.ShapeDtypeStruct((8, WIDTH), F32),
        ],
        in_specs=[ANY_SPEC] * 7 + [VMEM_SPEC] * 3 + [ANY_SPEC] * 3 + [VMEM_SPEC] * 2,
        out_specs=[ANY_SPEC] * 7 + [VMEM_SPEC],
        scratch_shapes=[
            pltpu.VMEM((2, OUT_ROWS, TOKENS), BF16),
            pltpu.VMEM((RING * QKV_ROWS, TOKENS), BF16),
            pltpu.VMEM((RING * OUT_ROWS, TOKENS), BF16),
            pltpu.VMEM(tokens, BF16),
            pltpu.VMEM(tokens, BF16),
            pltpu.VMEM((RING * QKV_ROWS, WIDTH), BF16),
            pltpu.VMEM((RING * OUT_ROWS, WIDTH), BF16),
            pltpu.VMEM(tokens, BF16),
            pltpu.VMEM(tokens, BF16),
            pltpu.VMEM((2, RING, PIECE, WIDTH), BF16),
            pltpu.SemaphoreType.DMA((17,)),
            pltpu.SemaphoreType.DMA((2,)),
            pltpu.SemaphoreType.DMA((2,)),
            pltpu.SemaphoreType.REGULAR,
            pltpu.SemaphoreType.REGULAR,
            pltpu.VMEM((1, WIDTH), F32),
            pltpu.VMEM((1, WIDTH), F32),
            pltpu.VMEM((4, 8, WIDTH), F32),
            pltpu.VMEM((3, 3, 8, WIDTH), F32),
            pltpu.VMEM((3, PIECE, WIDTH), BF16),
            pltpu.SemaphoreType.DMA((copies,)),
            pltpu.SemaphoreType.DMA((copies,)),
            pltpu.SemaphoreType.DMA((3, 4)),
        ] + GradScatter.scratch(WIDTHS) + GradScatter.scratch(WIDTHS) + tail,
        compiler_params=pltpu.CompilerParams(collective_id=3, has_side_effects=True, vmem_limit_bytes=67043328),
        name="backward",
    )(*operands)


def solution(mesh):
    batch_spec = P(("pod", "dp"), None, None)
    seg_spec = P(("pod", "dp"), None)

    def local_step(x_in, seg_ids, gain_one, gain_two, w_qkv, w_out, w_up, w_down, grad_y):
        batch_loc, seq_len, hidden = x_in.shape
        heads_loc, head_dim = w_out.shape[:2]
        rows_loc = batch_loc // RING
        tokens = rows_loc * seq_len
        shard_rows = w_up.shape[1]
        qkv_cols = w_qkv.shape[1]
        x_pos = lax.axis_index("tp") // 2

        def own_rows(array):
            return lax.dynamic_slice_in_dim(array, x_pos * rows_loc, rows_loc, axis=0)

        def grid_of(own):
            return own.reshape(RING, RING, PIECE, hidden)

        own_att = grid_of(jnp.concatenate([w_qkv.T, w_out.reshape(heads_loc * head_dim, hidden)], axis=0))
        own_up = grid_of(w_up.T)
        own_down = grid_of(w_down)
        x_rows = own_rows(x_in).reshape(tokens, hidden)
        seg_rows = own_rows(seg_ids)
        seg_row, seg_col = seg_rows[:, None, :], seg_rows[:, :, None]
        grad_rows = own_rows(grad_y).reshape(tokens, hidden)
        w_att, up_t, down, qkv_t, attn_flat, normed_a, x_one, normed_b = front(
            own_att, own_up, own_down, x_rows, gain_one[None], gain_two[None], seg_row, seg_col)
        up_t = up_t.reshape(RING * shard_rows, hidden)
        down = down.reshape(RING * shard_rows, hidden)

        def pair_sum(part):
            return part.astype(F32) + core_swap(part).astype(F32)

        pre_act = dot_nt(up_t, normed_b)
        act_val, gelu_pull = jax.vjp(gelu_tanh, pre_act)
        hidden_act = act_val.astype(BF16)
        part_two = dot_tn(hidden_act, down).astype(BF16)
        sum_two = pair_sum(part_two).astype(BF16)
        y_rows = (x_one.astype(F32) + sum_two.astype(F32)).astype(BF16)

        grad_hidden = dot_nt(down, grad_rows).astype(BF16)
        grad_pre = gelu_pull(grad_hidden.astype(F32))[0].astype(BF16)

        part_b = dot_tn(grad_pre, up_t).astype(BF16)
        part_b, y_rows = lax.optimization_barrier((part_b, y_rows))
        grad_up_own, grad_down_own, grad_att_own, _, _, _, grad_x, gains = backward(
            hidden_act, grad_pre, grad_rows, normed_b, part_b, x_one, qkv_t, seg_row, seg_col, attn_flat,
            w_att.reshape(RING, shard_rows, hidden), normed_a, x_rows, gain_one[None], gain_two[None])
        grad_att_own = grad_att_own.reshape(shard_rows, hidden)

        def spread(rows):
            core = lax.axis_index("tp") % 2
            mine = lax.dynamic_slice_in_dim(rows.reshape(rows_loc, seq_len, hidden), core, 1, axis=0)
            return lax.all_gather(mine, "tp", axis=0, tiled=True)

        return (
            spread(y_rows),
            grad_x,
            gains[0].astype(BF16),
            gains[1].astype(BF16),
            grad_att_own[:qkv_cols].T,
            grad_att_own[qkv_cols:].reshape(heads_loc, head_dim, hidden),
            grad_up_own.reshape(shard_rows, hidden).T,
            grad_down_own.reshape(shard_rows, hidden),
        )

    return jax.shard_map(
        local_step,
        mesh=mesh,
        in_specs=(batch_spec, seg_spec, P(None), P(None), P(None, "tp"), P("tp", None, None), P(None, "tp"), P("tp", None), batch_spec),
        out_specs=(batch_spec, batch_spec, P("pod"), P("pod"), P("pod", "tp"), P(("pod", "tp"), None, None), P("pod", "tp"), P(("pod", "tp"), None)),
        check_vma=False,
    )
```

```python
import functools

import jax
import jax.numpy as jnp
from jax import lax
from jax.experimental import pallas as pl
from jax.experimental.pallas import tpu as pltpu
from jax.sharding import PartitionSpec as P

EPS_NORM = 1e-5
NEG_LARGE = -1e30
F32 = jnp.float32
BF16 = jnp.bfloat16
RING = 4


def gelu_tanh(values):
    return jax.nn.gelu(values, approximate=True)


def dot_nt(lhs, rhs):
    return lax.dot_general(lhs, rhs, (((lhs.ndim - 1,), (rhs.ndim - 1,)), ((), ())), preferred_element_type=F32)


def dot_tn(lhs, rhs):
    return lax.dot_general(lhs, rhs, (((0,), (0,)), ((), ())), preferred_element_type=F32)


def core_swap(array):
    return lax.ppermute(array, "tp", [(i, i ^ 1) for i in range(8)])


THIRD = 512
PIECE = 48
WIDTH = 1536
HALF = WIDTH // 2
MESH_ID = pl.DeviceIdType.MESH


class Place:
    def __init__(self):
        plane = lax.axis_index("dp")
        column = lax.axis_index("tp")
        self.pos = {"z": lax.div(plane, RING), "y": lax.rem(plane, RING), "x": lax.div(column, 2)}
        self.core = lax.rem(column, 2)

    def ahead(self, axis, step):
        return lax.rem(self.pos[axis] + step, RING)

    def peer(self, axis, step):
        if axis == "x":
            return {"tp": self.ahead("x", step) * 2 + self.core}
        if axis == "y":
            return {"dp": self.pos["z"] * RING + self.ahead("y", step)}
        return {"dp": self.ahead("z", step) * RING + self.pos["y"]}

    def block(self, axis, step):
        return step if axis == "x" else self.ahead(axis, step)

    def sibling(self):
        return {"tp": self.pos["x"] * 2 + 1 - self.core}

    def enter(self, core=False):
        barrier = pltpu.get_barrier_semaphore()
        if core:
            pl.semaphore_signal(barrier, inc=1, device_id=self.sibling(), device_id_type=MESH_ID)
        self.signal_rings(barrier)
        pl.semaphore_wait(barrier, 9 + core)

    def signal_rings(self, semaphore):
        for axis in "xyz":
            for step in range(1, RING):
                pl.semaphore_signal(semaphore, inc=1, device_id=self.peer(axis, step), device_id_type=MESH_ID)


class Sender:
    def __init__(self, place, send_sems, recv_sems):
        self.place, self.send_sems, self.recv_sems = place, send_sems, recv_sems
        self.used = 0
        self.copies = []

    def ring(self, axis, source, target):
        started = []
        for step in range(1, RING):
            copy = pltpu.make_async_remote_copy(
                src_ref=source(step), dst_ref=target(step),
                send_sem=self.send_sems.at[self.used], recv_sem=self.recv_sems.at[self.used],
                device_id=self.place.peer(axis, step), device_id_type=MESH_ID,
            )
            copy.start()
            self.used += 1
            started.append(copy)
        self.copies += started
        return started

    def send(self, axis, step, source, target):
        copy = pltpu.make_async_remote_copy(
            src_ref=source, dst_ref=target,
            send_sem=self.send_sems.at[self.used], recv_sem=self.recv_sems.at[self.used],
            device_id=self.place.peer(axis, step), device_id_type=MESH_ID,
        )
        copy.start()
        self.used += 1
        self.copies.append(copy)
        return copy

    def swap(self, source, target):
        copy = pltpu.make_async_remote_copy(
            src_ref=source, dst_ref=target,
            send_sem=self.send_sems.at[self.used], recv_sem=self.recv_sems.at[self.used],
            device_id=self.place.sibling(), device_id_type=MESH_ID,
        )
        copy.start()
        self.used += 1
        return copy

    def settle(self, copies):
        for copy in copies:
            copy.wait_send()
        done = {id(copy) for copy in copies}
        self.copies = [copy for copy in self.copies if id(copy) not in done]

    def drain(self):
        for copy in self.copies:
            copy.wait_send()


def wait_all(copies):
    for copy in copies:
        copy.wait_recv()


ANY_SPEC = pl.BlockSpec(memory_space=pl.ANY)
VMEM_SPEC = pl.BlockSpec(memory_space=pltpu.VMEM)
QKV_ROWS = 576
OUT_ROWS = 192
SEQ = 512
TOKENS = 2 * SEQ
STEP = 256
NORM_STEP = 128
BLOCK = 256
HEAD = 96
SCALE = HEAD ** -0.5


def head_slice(ref, index, kind, lo, hi, kinds=3):
    head, row = lax.div(index, 2), lax.rem(index, 2)
    start = pl.multiple_of((head * kinds + kind) * HEAD, 32)
    return ref.at[pl.ds(start, HEAD), pl.ds(pl.multiple_of(row * SEQ + lo, 128), hi - lo)]


def dot_cols(lhs, rhs):
    return lax.dot_general(lhs, rhs, (((0,), (0,)), ((), ())), preferred_element_type=F32)


def dot_rows(lhs, rhs):
    return lax.dot_general(lhs, rhs, (((1,), (1,)), ((), ())), preferred_element_type=F32)


def dot_plain(lhs, rhs):
    return lax.dot_general(lhs, rhs, (((1,), (0,)), ((), ())), preferred_element_type=F32)


def probs_block(k_t, q_t, seg, seg_col, row, first):
    keys = first + BLOCK
    scores = dot_cols(k_t, q_t) * SCALE
    query = lax.broadcasted_iota(jnp.int32, (keys, BLOCK), 1) + first
    key = lax.broadcasted_iota(jnp.int32, (keys, BLOCK), 0)
    same = seg[row, :, first : first + BLOCK] == seg_col[row, :keys, :]
    scores = jnp.where((query >= key) & same, scores, NEG_LARGE)
    weights = jnp.exp(scores - jnp.max(scores, axis=0, keepdims=True))
    return weights * (1.0 / jnp.sum(weights, axis=0, keepdims=True))


def attention_forward(qkv, seg, seg_col, out, start, stop):
    @pl.loop(start, stop)
    def _(index):
        row = lax.rem(index, 2)
        for first in range(0, SEQ, BLOCK):
            keys = first + BLOCK
            probs = probs_block(
                head_slice(qkv, index, 1, 0, keys)[...], head_slice(qkv, index, 0, first, keys)[...], seg, seg_col, row, first)
            value = lax.dot_general(
                head_slice(qkv, index, 2, 0, keys)[...], probs.astype(BF16), (((1,), (0,)), ((), ())), preferred_element_type=F32)
            head_slice(out, index, 0, first, keys, kinds=1)[...] = value.astype(BF16)


def attention_backward(qkv, seg, seg_col, grad, out, start, stop):
    @pl.loop(start, stop)
    def _(index):
        row = lax.rem(index, 2)
        grads = []
        for first in range(0, SEQ, BLOCK):
            keys = first + BLOCK
            q_t = head_slice(qkv, index, 0, first, keys)[...]
            k_t = head_slice(qkv, index, 1, 0, keys)[...]
            g_t = head_slice(grad, index, 0, first, keys, kinds=1)[...]
            probs = probs_block(k_t, q_t, seg, seg_col, row, first)
            grad_probs = dot_cols(head_slice(qkv, index, 2, 0, keys)[...], g_t)
            grad_scores = probs * (grad_probs - jnp.sum(grad_probs * probs, axis=0, keepdims=True))
            low = (grad_scores * SCALE).astype(BF16)
            grad_q = lax.dot_general(k_t, low, (((1,), (0,)), ((), ())), preferred_element_type=F32)
            head_slice(out, index, 0, first, keys)[...] = grad_q.astype(BF16)
            grads.append((dot_rows(q_t, low), dot_rows(g_t, probs.astype(BF16))))
        for i in range(2):
            whole = grads[1][i]
            head_slice(out, index, 1 + i, 0, BLOCK)[...] = (grads[0][i] + whole[:, :BLOCK]).astype(BF16)
            head_slice(out, index, 1 + i, BLOCK, SEQ)[...] = whole[:, BLOCK:].astype(BF16)


class Relay:
    COPIES = 6

    def __init__(self, sender, axis, own, up, down, on_up, on_down):
        self.sender, self.axis = sender, axis
        self.on_up, self.on_down = on_up, on_down
        self.ups = [sender.send(axis, 1, own(half), up(half)) for half in range(2)]
        self.downs = [sender.send(axis, 3, own(half), down(half)) for half in range(2)]

    @classmethod
    def at_place(cls, sender, axis, region, own=None):
        place = sender.place
        here = lambda half: region(place.pos[axis], half)
        behind, ahead = region(place.ahead(axis, 3), 0), region(place.ahead(axis, 1), 1)
        return cls(sender, axis, own or here, here, here, (behind, behind), (ahead, ahead))

    def pass_on(self):
        self.ups[0].wait_recv()
        self.passed = [self.sender.send(self.axis, 1, *self.on_up)]
        self.downs[1].wait_recv()
        self.passed.append(self.sender.send(self.axis, 3, *self.on_down))

    def finish(self):
        wait_all([self.ups[1], self.downs[0]] + self.passed)


class WeightGather:
    COPIES = 12 + 3 * Relay.COPIES

    def __init__(self, place, sender, own, out):
        self.place, self.sender, self.own, self.out = place, sender, own, out

    def spot(self, cols):
        z, y = self.place.pos["z"], self.place.pos["y"]
        return lambda step: self.out.at[pl.ds(1, 3), z, y, :, cols]

    def start(self):
        z, y = self.place.pos["z"], self.place.pos["y"]
        self.near = []
        for part in range(2):
            cols = pl.ds(part * THIRD, THIRD)
            self.near.append(self.sender.ring(
                "x", lambda step: self.own.at[z, y, :, cols], lambda step: self.out.at[RING - step, z, y, :, cols]))

    def start_whole(self):
        cols = pl.ds(2 * THIRD, THIRD)
        spot = lambda shard, half: self.out.at[shard, pl.ds(2 * half, 2), :, :, cols]
        self.whole = Relay(
            self.sender, "x", lambda half: self.own.at[pl.ds(2 * half, 2), :, :, cols],
            lambda half: spot(3, half), lambda half: spot(1, half), (spot(3, 0), spot(2, 0)), (spot(1, 1), spot(2, 1)))

    def second(self):
        self.mid = []
        for part, axis in enumerate("yz"):
            wait_all(self.near[part])
            spot = self.spot(pl.ds(part * THIRD, THIRD))
            self.mid.append(self.sender.ring(axis, spot, spot))

    def third(self):
        shards = pl.ds(1, 3)
        wait_all(self.mid[0])
        line = lambda pos, half: self.out.at[shards, pos, pl.ds(2 * half, 2), :, pl.ds(0, THIRD)]
        self.far = [Relay.at_place(self.sender, "z", line)]
        wait_all(self.mid[1])
        row = lambda pos, half: self.out.at[shards, pl.ds(2 * half, 2), pos, :, pl.ds(THIRD, THIRD)]
        self.far.append(Relay.at_place(self.sender, "y", row))

    def pass_on(self):
        for far in self.far:
            far.pass_on()

    def finish(self):
        for far in self.far:
            far.finish()
        self.whole.finish()


def norm_stats(x_f32):
    centered = x_f32 - jnp.mean(x_f32, axis=-1, keepdims=True)
    inv_std = lax.rsqrt(jnp.mean(centered * centered, axis=-1, keepdims=True) + EPS_NORM)
    return centered * inv_std, inv_std


def token_blocks(body):
    @pl.loop(0, TOKENS // NORM_STEP)
    def _(index):
        body(pl.ds(pl.multiple_of(index * NORM_STEP, NORM_STEP), NORM_STEP))


def front_kernel(
    own_att, own_up, own_down, x_in, gain_a, gain_b, seg, seg_col,
    w_att, w_up, w_down, qkv_out, attn_out, normed_a_out, x_one_out, normed_b_out,
    weights, stage, x_one, normed, qkv, attn, part, other, load_sems, send_sems, recv_sems,
):
    place = Place()
    sender = Sender(place, send_sems, recv_sems)

    def copy(source, target, index):
        started = pltpu.make_async_copy(source, target, load_sems.at[index])
        started.start()
        return started

    loads = [copy(x_in, x_one, 0), copy(own_att, weights.at[0], 1), copy(own_up, stage.at[0], 2), copy(own_down, stage.at[1], 3)]
    place.enter(core=True)
    att = WeightGather(place, sender, own_att, w_att)
    mlp = [WeightGather(place, sender, own_up, w_up), WeightGather(place, sender, own_down, w_down)]
    att.start()
    att.start_whole()
    for gather in mlp:
        gather.start()
    loads[0].wait()

    def first_norm(rows):
        x_hat, _ = norm_stats(x_one[rows].astype(F32))
        normed[rows] = (x_hat * gain_a[...].astype(F32)).astype(BF16)

    token_blocks(first_norm)
    results = [copy(normed, normed_a_out, 4)]
    att.second()
    for load in loads[1:]:
        load.wait()
    results += [copy(weights.at[0], w_att.at[0], 5), copy(stage.at[0], w_up.at[0], 6), copy(stage.at[1], w_down.at[0], 7)]

    def project(start, stop):
        @pl.loop(start, stop)
        def _(index):
            block = weights[lax.div(index, 3), lax.rem(index, 3)].reshape(OUT_ROWS, WIDTH)
            qkv[pl.ds(pl.multiple_of(index * OUT_ROWS, OUT_ROWS), OUT_ROWS)] = dot_rows(block, normed[...]).astype(BF16)

    project(0, 3)
    att.third()
    for gather in mlp:
        gather.second()
    att.whole.pass_on()
    for gather in mlp:
        gather.start_whole()
    att.pass_on()
    att.finish()
    others = [copy(w_att.at[shard], weights.at[shard], 7 + shard) for shard in range(1, RING)]
    for load in others:
        load.wait()
    project(3, 12)
    results.append(copy(qkv, qkv_out, 11))
    for gather in mlp:
        gather.third()
    attention_forward(qkv, seg, seg_col, attn, 0, 10)
    mlp[0].whole.pass_on()
    mlp[0].pass_on()
    attention_forward(qkv, seg, seg_col, attn, 10, 16)
    mlp[1].whole.pass_on()
    mlp[1].pass_on()
    results.append(copy(attn, attn_out, 12))
    swaps = []
    for index in range(TOKENS // STEP):
        rows = pl.ds(index * STEP, STEP)
        total = None
        for shard in range(RING):
            block = weights[shard, 3].reshape(OUT_ROWS, WIDTH)
            term = dot_cols(attn[shard * OUT_ROWS : (shard + 1) * OUT_ROWS, index * STEP : (index + 1) * STEP], block)
            total = term if total is None else total + term
        part[rows] = total.astype(BF16)
        swaps.append(sender.swap(part.at[rows], other.at[rows]))
    results[0].wait()
    wait_all(swaps)

    def second_norm(rows):
        summed = (part[rows].astype(F32) + other[rows].astype(F32)).astype(BF16)
        x_new = (x_one[rows].astype(F32) + summed.astype(F32)).astype(BF16)
        x_one[rows] = x_new
        x_hat, _ = norm_stats(x_new.astype(F32))
        normed[rows] = (x_hat * gain_b[...].astype(F32)).astype(BF16)

    token_blocks(second_norm)
    results += [copy(x_one, x_one_out, 13), copy(normed, normed_b_out, 14)]
    for gather in mlp:
        gather.finish()
    for result in results[1:]:
        result.wait()
    for swap in swaps:
        swap.wait_send()
    sender.drain()


def front(own_att, own_up, own_down, x_rows, gain_a, gain_b, seg, seg_col):
    tokens = (TOKENS, WIDTH)
    gathered = jax.ShapeDtypeStruct((RING,) + own_att.shape, BF16)
    rows = jax.ShapeDtypeStruct(tokens, BF16)
    copies = 3 * WeightGather.COPIES + TOKENS // STEP
    return pl.pallas_call(
        front_kernel,
        out_shape=[
            gathered, gathered, gathered,
            jax.ShapeDtypeStruct((RING * QKV_ROWS, TOKENS), BF16), jax.ShapeDtypeStruct((RING * OUT_ROWS, TOKENS), BF16),
            rows, rows, rows,
        ],
        in_specs=[ANY_SPEC] * 4 + [VMEM_SPEC] * 4,
        out_specs=[ANY_SPEC] * 8,
        scratch_shapes=[
            pltpu.VMEM(gathered.shape, BF16),
            pltpu.VMEM((2,) + own_att.shape, BF16),
            pltpu.VMEM(tokens, BF16),
            pltpu.VMEM(tokens, BF16),
            pltpu.VMEM((RING * QKV_ROWS, TOKENS), BF16),
            pltpu.VMEM((RING * OUT_ROWS, TOKENS), BF16),
            pltpu.VMEM(tokens, BF16),
            pltpu.VMEM(tokens, BF16),
            pltpu.SemaphoreType.DMA((15,)),
            pltpu.SemaphoreType.DMA((copies,)),
            pltpu.SemaphoreType.DMA((copies,)),
        ],
        compiler_params=pltpu.CompilerParams(collective_id=1, has_side_effects=True, vmem_limit_bytes=56 << 20),
        name="front",
    )(own_att, own_up, own_down, x_rows, gain_a, gain_b, seg, seg_col)


ORDERS = (("z", "y", "x", 1), ("y", "x", "z", 0), ("x", "z", "y", 0))


class GradScatter:
    def __init__(self, place, sender, grads, widths, bufs, final, local_sems):
        self.place, self.sender, self.grads = place, sender, grads
        self.bufs, self.final, self.local_sems = bufs, final, local_sems
        self.parts = range(len(widths))
        self.cols = [(sum(widths[:part]), widths[part]) for part in self.parts]

    @staticmethod
    def scratch(widths):
        shapes = []
        for width in widths:
            shapes += [
                pltpu.VMEM((RING, RING, PIECE, width), BF16),
                pltpu.VMEM((3, RING, RING, PIECE, width), BF16),
                pltpu.VMEM((RING, RING, PIECE, width), BF16),
                pltpu.VMEM((3, PIECE, width), BF16),
            ]
        return shapes

    def cut(self, part, step):
        axis = ORDERS[part][0]
        index = self.place.block(axis, step)
        cols = pl.ds(*self.cols[part])
        if axis == "x":
            return self.grads.at[index, :, :, :, cols]
        if axis == "z":
            return self.grads.at[:, index, :, :, cols]
        return self.grads.at[:, :, index, :, cols]

    def start(self):
        self.loads, self.one, self.two, self.three = [], [], {}, {}
        for part in self.parts:
            self.one.append(self.sender.ring(
                ORDERS[part][0], lambda step: self.cut(part, step), lambda step: self.bufs[part][1].at[step - 1]))
        for part in self.parts:
            load = pltpu.make_async_copy(self.cut(part, 0), self.bufs[part][0], self.local_sems.at[part])
            load.start()
            self.loads.append(load)

    def second(self):
        for part in self.parts:
            self.loads[part].wait()
            wait_all(self.one[part])
            mine, first, second, _ = self.bufs[part]

            @pl.loop(0, RING)
            def _(a):
                for b in range(RING):
                    total = mine[a, b].astype(F32)
                    for k in range(3):
                        total = total + first[k, a, b].astype(F32)
                    mine[a, b] = total.astype(BF16)

            axis, spot = ORDERS[part][1], ORDERS[part][3]

            def source(step):
                index = self.place.block(axis, step)
                return mine.at[:, index] if spot else mine.at[index]

            self.two[part] = self.sender.ring(axis, source, lambda step: second.at[step - 1])

    def third(self):
        for part in self.parts:
            wait_all(self.two[part])
            mine, _, second, third = self.bufs[part]
            axis, spot = ORDERS[part][1], ORDERS[part][3]
            own = self.place.block(axis, 0)
            for other in range(RING):
                total = mine[(other, own) if spot else (own, other)].astype(F32)
                for k in range(3):
                    total = total + second[k, other].astype(F32)
                second[3, other] = total.astype(BF16)
            axis = ORDERS[part][2]
            self.three[part] = self.sender.ring(
                axis, lambda step: second.at[3, self.place.block(axis, step)], lambda step: third.at[step - 1])

    def finish(self):
        for part in self.parts:
            wait_all(self.three[part])
            _, _, second, third = self.bufs[part]
            total = second[3, self.place.block(ORDERS[part][2], 0)].astype(F32)
            for k in range(3):
                total = total + third[k].astype(F32)
            start, width = self.cols[part]
            self.final[:, start : start + width] = total.astype(BF16)


class PlaneGather:
    COPIES = 6 + 2 * Relay.COPIES

    def __init__(self, place, sender, final, out, local_sem):
        self.place, self.sender, self.final, self.out, self.local_sem = place, sender, final, out, local_sem

    def start(self):
        z, y = self.place.pos["z"], self.place.pos["y"]
        self.store = pltpu.make_async_copy(self.final, self.out.at[z, y], self.local_sem)
        self.store.start()
        self.near = []
        for part, axis in enumerate("yz"):
            cols = pl.ds(part * HALF, HALF)
            self.near.append(self.sender.ring(
                axis, lambda step: self.final.at[:, cols], lambda step: self.out.at[z, y, :, cols]))

    def second(self):
        self.store.wait()
        wait_all(self.near[0])
        line = lambda pos, half: self.out.at[pos, pl.ds(2 * half, 2), :, pl.ds(0, HALF)]
        self.far = [Relay.at_place(self.sender, "z", line)]
        wait_all(self.near[1])
        row = lambda pos, half: self.out.at[pl.ds(2 * half, 2), pos, :, pl.ds(HALF, HALF)]
        self.far.append(Relay.at_place(self.sender, "y", row))

    def pass_on(self):
        for far in self.far:
            far.pass_on()

    def finish(self):
        for far in self.far:
            far.finish()


def gain_step(place, sender, gains, bufs, index, axis):
    copies = sender.ring(axis, lambda step: gains.at[index], lambda step: bufs.at[index, step - 1])

    def finish():
        wait_all(copies)
        gains[index + 1] = (gains[index] + bufs[index, 1]) + (bufs[index, 0] + bufs[index, 2])

    return finish


def grad_works(place, sender, grads, widths, bufs, finals, outs, local_sems):
    parts = len(widths)
    works, planes = [], []
    for i, grad in enumerate(grads):
        mine = bufs[4 * parts * i : 4 * parts * (i + 1)]
        mine = [mine[4 * part : 4 * part + 4] for part in range(parts)]
        works.append(GradScatter(place, sender, grad, widths, mine, finals.at[i], local_sems.at[i]))
        planes.append(PlaneGather(place, sender, finals.at[i], outs[i], local_sems.at[i, 3]))
    return works, planes


WIDTHS = (640, 640, 256)


def back_kernel(
    hidden_act, grad_pre, grad_y, normed_b_in, part_b, x_one_in, qkv_in, seg, seg_col, attn, w_att, normed_a_in, x_in, gain_a, gain_b,
    out_up, out_down, out_att, grad_up, grad_down, grad_att, grad_x, gain_out,
    lhs, qkv, grad_attn, grad_one, normed, w_qkv, w_out, part, other, stage, load_sems, lhs_sems, stage_sems, free_sem, ring_sem,
    gain_grad_a, gain_grad_b, gains, gain_bufs, finals, send_sems, recv_sems, local_sems, *bufs,
):
    place = Place()
    sender = Sender(place, send_sems, recv_sems)
    loads = {}

    def load(name, source, target, index):
        copy = pltpu.make_async_copy(source, target, load_sems.at[index])
        copy.start()
        loads.setdefault(name, []).append(copy)

    def ready(name):
        for copy in loads[name]:
            copy.wait()

    load("one", grad_y, grad_one, 0)
    load("part", part_b, part, 13)
    load("normed_b", normed_b_in, normed, 6)
    load("qkv", qkv_in, qkv, 5)
    for shard in range(RING):
        load("out", w_att.at[shard, pl.ds(QKV_ROWS, OUT_ROWS)], w_out.at[pl.ds(shard * OUT_ROWS, OUT_ROWS)], 1 + shard)
    for shard in range(RING):
        load("w", w_att.at[shard, pl.ds(0, QKV_ROWS)], w_qkv.at[pl.ds(shard * QKV_ROWS, QKV_ROWS)], 7 + shard)
    place.enter(core=True)
    works, planes = grad_works(place, sender, [grad_down, grad_up], WIDTHS, bufs, finals, [out_down, out_up], local_sems)
    tail = bufs[8 * len(WIDTHS) :]
    reused = [(works[0].bufs[part][0], works[0].bufs[part][1]) + tuple(tail[2 * part : 2 * part + 2]) for part in range(len(WIDTHS))]
    att_work = GradScatter(place, sender, grad_att, WIDTHS, reused, finals.at[2], local_sems.at[2])
    att_plane = PlaneGather(place, sender, finals.at[2], out_att, local_sems.at[2, 3])
    ready("part")
    early = sender.swap(part, other)

    blocks = RING * RING

    def fetch(source, index, slot):
        rows = pl.ds(pl.multiple_of(index * OUT_ROWS, OUT_ROWS), OUT_ROWS)
        return pltpu.make_async_copy(source.at[rows], lhs.at[slot], lhs_sems.at[slot])

    def place_block(target, index, slot):
        return pltpu.make_async_copy(stage.at[slot], target.at[lax.div(index, RING), lax.rem(index, RING)], stage_sems.at[slot])

    def weight_grad(source, rhs, target):
        fetch(source, 0, 0).start()

        @pl.loop(0, blocks)
        def _(index):
            slot = lax.rem(index, 2)
            fetch(source, index, slot).wait()

            @pl.when(index + 1 < blocks)
            def _():
                fetch(source, index + 1, 1 - slot).start()

            @pl.when(index >= 2)
            def _():
                place_block(target, index - 2, slot).wait()

            stage[slot] = dot_plain(lhs[slot], rhs[...]).astype(BF16).reshape(RING, PIECE, WIDTH)
            place_block(target, index, slot).start()

        for index in (blocks - 2, blocks - 1):
            place_block(target, index, index % 2).wait()

    ready("one")
    weight_grad(hidden_act, grad_one, grad_down)
    works[0].start()
    ready("normed_b")
    weight_grad(grad_pre, normed, grad_up)
    works[1].start()

    load("x_one", x_one_in, normed, 14)
    gain_grad_a[...] = jnp.zeros_like(gain_grad_a)
    gain_grad_b[...] = jnp.zeros_like(gain_grad_b)
    early.wait_recv()
    early.wait_send()
    ready("x_one")

    def norm_back(rows, gain, gain_grad):
        x_hat, inv_std = norm_stats(normed[rows].astype(F32))
        grad = (part[rows].astype(F32) + other[rows].astype(F32)).astype(BF16).astype(F32)
        gain_grad[...] += jnp.sum(grad * x_hat, axis=0, keepdims=True)
        grad_hat = grad * gain[...].astype(F32)
        mean_one = jnp.mean(grad_hat, axis=-1, keepdims=True)
        mean_two = jnp.mean(grad_hat * x_hat, axis=-1, keepdims=True)
        back = inv_std * (grad_hat - mean_one - x_hat * mean_two)
        return (grad_one[rows].astype(F32) + back).astype(BF16)

    def second_norm(rows):
        grad_one[rows] = norm_back(rows, gain_b, gain_grad_b)

    token_blocks(second_norm)
    pl.semaphore_signal(free_sem, inc=1, device_id=place.sibling(), device_id_type=MESH_ID)
    load("normed_a", normed_a_in, normed, 11)

    ready("out")
    for shard in range(RING):
        rows = pl.ds(shard * OUT_ROWS, OUT_ROWS)
        grad_attn[rows] = dot_rows(w_out[rows], grad_one[...]).astype(BF16)
    ready("qkv")
    attention_backward(qkv, seg, seg_col, grad_attn, qkv, 0, 10)
    works[0].second()
    place.signal_rings(ring_sem)
    attention_backward(qkv, seg, seg_col, grad_attn, qkv, 10, 16)

    ready("w")
    pl.semaphore_wait(free_sem, 1)
    swaps = []
    for index in range(TOKENS // STEP):
        rows = pl.ds(index * STEP, STEP)
        part[rows] = dot_cols(qkv[:, index * STEP : (index + 1) * STEP], w_qkv[...]).astype(BF16)
        swaps.append(sender.swap(part.at[rows], other.at[rows]))
    works[1].second()
    works[0].third()

    stores = []

    def put(rows, shard, start):
        slot = len(stores) % 2
        if len(stores) >= 2:
            stores[-2].wait()
        stage[slot] = rows.astype(BF16).reshape(RING, PIECE, WIDTH)
        copy = pltpu.make_async_copy(stage.at[slot], grad_att.at[shard, start // OUT_ROWS], stage_sems.at[slot])
        copy.start()
        stores.append(copy)

    for shard in range(RING):
        put(dot_plain(attn[shard * OUT_ROWS : (shard + 1) * OUT_ROWS], grad_one[...]), shard, QKV_ROWS)
    ready("normed_a")
    for shard in range(RING):
        for block in range(3):
            start = shard * QKV_ROWS + block * OUT_ROWS
            put(dot_plain(qkv[start : start + OUT_ROWS], normed[...]), shard, block * OUT_ROWS)
    for store in stores[-2:]:
        store.wait()
    load("x", x_in, normed, 15)
    sender.settle([copy for copies in works[0].two.values() for copy in copies])
    pl.semaphore_wait(ring_sem, 9)
    att_work.start()
    works[1].third()
    ready("x")
    wait_all(swaps)
    for copy in swaps:
        copy.wait_send()

    def first_norm(rows):
        part[rows] = norm_back(rows, gain_a, gain_grad_a)

    token_blocks(first_norm)
    row_of = lambda pos: 2 * pos + place.core
    part_rows = SEQ // 2
    mine = lambda half: part.at[pl.ds(pl.multiple_of(place.core * SEQ + half * part_rows, part_rows), part_rows)]
    rows_sent = Relay.at_place(sender, "x", lambda pos, half: grad_x.at[row_of(pos), pl.ds(half * part_rows, part_rows)], mine)
    results = []
    for i in range(2):
        result = pltpu.make_async_copy(part.at[pl.ds(i * SEQ, SEQ)], grad_x.at[2 * place.pos["x"] + i], load_sems.at[12 + 4 * i])
        result.start()
        results.append(result)
    gains[0] = jnp.zeros_like(gain_out)
    gains[0, 0:1] = gain_grad_a[...]
    gains[0, 1:2] = gain_grad_b[...]
    gain_finish = gain_step(place, sender, gains, gain_bufs, 0, "z")
    for work, plane in zip(works, planes):
        work.finish()
        plane.start()
    gain_finish()
    gain_finish = gain_step(place, sender, gains, gain_bufs, 1, "y")
    att_work.second()
    for plane in planes:
        plane.second()
    gain_finish()
    gain_finish = gain_step(place, sender, gains, gain_bufs, 2, "x")
    rows_sent.pass_on()
    att_work.third()
    for plane in planes:
        plane.pass_on()
    att_work.finish()
    att_plane.start()
    rows_sent.finish()
    passed = []
    for step in range(1, RING):
        row = grad_x.at[row_of(place.ahead("x", step))]
        passed.append(sender.swap(row, row))
    gain_finish()
    gain_out[...] = gains[3]
    for plane in planes:
        plane.finish()
    att_plane.second()
    att_plane.pass_on()
    att_plane.finish()
    wait_all(passed)
    for copy in passed:
        copy.wait_send()
    for result in results:
        result.wait()
    sender.drain()


def backward(*operands):
    tokens = (TOKENS, WIDTH)
    piece = jax.ShapeDtypeStruct((RING, RING, PIECE, WIDTH), BF16)
    grid = jax.ShapeDtypeStruct((RING, RING, RING, PIECE, WIDTH), BF16)
    copies = 3 * (9 * len(WIDTHS) + PlaneGather.COPIES) + TOKENS // STEP + 1 + 9 + Relay.COPIES + 3
    tail = [shape for part in range(len(WIDTHS)) for shape in GradScatter.scratch(WIDTHS)[4 * part + 2 : 4 * part + 4]]
    return pl.pallas_call(
        back_kernel,
        out_shape=[
            piece, piece, piece, grid, grid, grid,
            jax.ShapeDtypeStruct((2 * RING, SEQ, WIDTH), BF16),
            jax.ShapeDtypeStruct((8, WIDTH), F32),
        ],
        in_specs=[ANY_SPEC] * 7 + [VMEM_SPEC] * 3 + [ANY_SPEC] * 3 + [VMEM_SPEC] * 2,
        out_specs=[ANY_SPEC] * 7 + [VMEM_SPEC],
        scratch_shapes=[
            pltpu.VMEM((2, OUT_ROWS, TOKENS), BF16),
            pltpu.VMEM((RING * QKV_ROWS, TOKENS), BF16),
            pltpu.VMEM((RING * OUT_ROWS, TOKENS), BF16),
            pltpu.VMEM(tokens, BF16),
            pltpu.VMEM(tokens, BF16),
            pltpu.VMEM((RING * QKV_ROWS, WIDTH), BF16),
            pltpu.VMEM((RING * OUT_ROWS, WIDTH), BF16),
            pltpu.VMEM(tokens, BF16),
            pltpu.VMEM(tokens, BF16),
            pltpu.VMEM((2, RING, PIECE, WIDTH), BF16),
            pltpu.SemaphoreType.DMA((17,)),
            pltpu.SemaphoreType.DMA((2,)),
            pltpu.SemaphoreType.DMA((2,)),
            pltpu.SemaphoreType.REGULAR,
            pltpu.SemaphoreType.REGULAR,
            pltpu.VMEM((1, WIDTH), F32),
            pltpu.VMEM((1, WIDTH), F32),
            pltpu.VMEM((4, 8, WIDTH), F32),
            pltpu.VMEM((3, 3, 8, WIDTH), F32),
            pltpu.VMEM((3, PIECE, WIDTH), BF16),
            pltpu.SemaphoreType.DMA((copies,)),
            pltpu.SemaphoreType.DMA((copies,)),
            pltpu.SemaphoreType.DMA((3, 4)),
        ] + GradScatter.scratch(WIDTHS) + GradScatter.scratch(WIDTHS) + tail,
        compiler_params=pltpu.CompilerParams(collective_id=3, has_side_effects=True, vmem_limit_bytes=67043328),
        name="backward",
    )(*operands)


def solution(mesh):
    batch_spec = P(("pod", "dp"), None, None)
    seg_spec = P(("pod", "dp"), None)

    def local_step(x_in, seg_ids, gain_one, gain_two, w_qkv, w_out, w_up, w_down, grad_y):
        batch_loc, seq_len, hidden = x_in.shape
        heads_loc, head_dim = w_out.shape[:2]
        rows_loc = batch_loc // RING
        tokens = rows_loc * seq_len
        shard_rows = w_up.shape[1]
        qkv_cols = w_qkv.shape[1]
        x_pos = lax.axis_index("tp") // 2

        def own_rows(array):
            return lax.dynamic_slice_in_dim(array, x_pos * rows_loc, rows_loc, axis=0)

        def grid_of(own):
            return own.reshape(RING, RING, PIECE, hidden)

        own_att = grid_of(jnp.concatenate([w_qkv.T, w_out.reshape(heads_loc * head_dim, hidden)], axis=0))
        own_up = grid_of(w_up.T)
        own_down = grid_of(w_down)
        x_rows = own_rows(x_in).reshape(tokens, hidden)
        seg_rows = own_rows(seg_ids)
        seg_row, seg_col = seg_rows[:, None, :], seg_rows[:, :, None]
        grad_rows = own_rows(grad_y).reshape(tokens, hidden)
        w_att, up_t, down, qkv_t, attn_flat, normed_a, x_one, normed_b = front(
            own_att, own_up, own_down, x_rows, gain_one[None], gain_two[None], seg_row, seg_col)
        up_t = up_t.reshape(RING * shard_rows, hidden)
        down = down.reshape(RING * shard_rows, hidden)

        def pair_sum(part):
            return part.astype(F32) + core_swap(part).astype(F32)

        pre_act = dot_nt(up_t, normed_b)
        act_val, gelu_pull = jax.vjp(gelu_tanh, pre_act)
        hidden_act = act_val.astype(BF16)
        part_two = dot_tn(hidden_act, down).astype(BF16)
        sum_two = pair_sum(part_two).astype(BF16)
        y_rows = (x_one.astype(F32) + sum_two.astype(F32)).astype(BF16)

        grad_hidden = dot_nt(down, grad_rows).astype(BF16)
        grad_pre = gelu_pull(grad_hidden.astype(F32))[0].astype(BF16)

        part_b = dot_tn(grad_pre, up_t).astype(BF16)
        part_b, y_rows = lax.optimization_barrier((part_b, y_rows))
        grad_up_own, grad_down_own, grad_att_own, _, _, _, grad_x, gains = backward(
            hidden_act, grad_pre, grad_rows, normed_b, part_b, x_one, qkv_t, seg_row, seg_col, attn_flat,
            w_att.reshape(RING, shard_rows, hidden), normed_a, x_rows, gain_one[None], gain_two[None])
        grad_att_own = grad_att_own.reshape(shard_rows, hidden)

        def spread(rows):
            core = lax.axis_index("tp") % 2
            mine = lax.dynamic_slice_in_dim(rows.reshape(rows_loc, seq_len, hidden), core, 1, axis=0)
            return lax.all_gather(mine, "tp", axis=0, tiled=True)

        return (
            spread(y_rows),
            grad_x,
            gains[0].astype(BF16),
            gains[1].astype(BF16),
            grad_att_own[:qkv_cols].T,
            grad_att_own[qkv_cols:].reshape(heads_loc, head_dim, hidden),
            grad_up_own.reshape(shard_rows, hidden).T,
            grad_down_own.reshape(shard_rows, hidden),
        )

    return jax.shard_map(
        local_step,
        mesh=mesh,
        in_specs=(batch_spec, seg_spec, P(None), P(None), P(None, "tp"), P("tp", None, None), P(None, "tp"), P("tp", None), batch_spec),
        out_specs=(batch_spec, batch_spec, P("pod"), P("pod"), P("pod", "tp"), P(("pod", "tp"), None, None), P("pod", "tp"), P(("pod", "tp"), None)),
        check_vma=False,
    )
```

```python
import functools

import jax
import jax.numpy as jnp
from jax import lax
from jax.experimental import pallas as pl
from jax.experimental.pallas import tpu as pltpu
from jax.sharding import PartitionSpec as P

EPS_NORM = 1e-5
NEG_LARGE = -1e30
F32 = jnp.float32
BF16 = jnp.bfloat16
RING = 4


def gelu_tanh(values):
    return jax.nn.gelu(values, approximate=True)


def dot_nt(lhs, rhs):
    return lax.dot_general(lhs, rhs, (((lhs.ndim - 1,), (rhs.ndim - 1,)), ((), ())), preferred_element_type=F32)


def dot_tn(lhs, rhs):
    return lax.dot_general(lhs, rhs, (((0,), (0,)), ((), ())), preferred_element_type=F32)


def core_swap(array):
    return lax.ppermute(array, "tp", [(i, i ^ 1) for i in range(8)])


THIRD = 512
PIECE = 48
WIDTH = 1536
HALF = WIDTH // 2
MESH_ID = pl.DeviceIdType.MESH


class Place:
    def __init__(self):
        plane = lax.axis_index("dp")
        column = lax.axis_index("tp")
        self.pos = {"z": lax.div(plane, RING), "y": lax.rem(plane, RING), "x": lax.div(column, 2)}
        self.core = lax.rem(column, 2)

    def ahead(self, axis, step):
        return lax.rem(self.pos[axis] + step, RING)

    def peer(self, axis, step):
        if axis == "x":
            return {"tp": self.ahead("x", step) * 2 + self.core}
        if axis == "y":
            return {"dp": self.pos["z"] * RING + self.ahead("y", step)}
        return {"dp": self.ahead("z", step) * RING + self.pos["y"]}

    def block(self, axis, step):
        return step if axis == "x" else self.ahead(axis, step)

    def sibling(self):
        return {"tp": self.pos["x"] * 2 + 1 - self.core}

    def enter(self, core=False):
        barrier = pltpu.get_barrier_semaphore()
        if core:
            pl.semaphore_signal(barrier, inc=1, device_id=self.sibling(), device_id_type=MESH_ID)
        self.signal_rings(barrier)
        pl.semaphore_wait(barrier, 9 + core)

    def signal_rings(self, semaphore):
        for axis in "xyz":
            for step in range(1, RING):
                pl.semaphore_signal(semaphore, inc=1, device_id=self.peer(axis, step), device_id_type=MESH_ID)


class Sender:
    def __init__(self, place, send_sems, recv_sems):
        self.place, self.send_sems, self.recv_sems = place, send_sems, recv_sems
        self.used = 0
        self.copies = []

    def ring(self, axis, source, target):
        started = []
        for step in range(1, RING):
            copy = pltpu.make_async_remote_copy(
                src_ref=source(step), dst_ref=target(step),
                send_sem=self.send_sems.at[self.used], recv_sem=self.recv_sems.at[self.used],
                device_id=self.place.peer(axis, step), device_id_type=MESH_ID,
            )
            copy.start()
            self.used += 1
            started.append(copy)
        self.copies += started
        return started

    def send(self, axis, step, source, target):
        copy = pltpu.make_async_remote_copy(
            src_ref=source, dst_ref=target,
            send_sem=self.send_sems.at[self.used], recv_sem=self.recv_sems.at[self.used],
            device_id=self.place.peer(axis, step), device_id_type=MESH_ID,
        )
        copy.start()
        self.used += 1
        self.copies.append(copy)
        return copy

    def swap(self, source, target):
        copy = pltpu.make_async_remote_copy(
            src_ref=source, dst_ref=target,
            send_sem=self.send_sems.at[self.used], recv_sem=self.recv_sems.at[self.used],
            device_id=self.place.sibling(), device_id_type=MESH_ID,
        )
        copy.start()
        self.used += 1
        return copy

    def settle(self, copies):
        for copy in copies:
            copy.wait_send()
        done = {id(copy) for copy in copies}
        self.copies = [copy for copy in self.copies if id(copy) not in done]

    def drain(self):
        for copy in self.copies:
            copy.wait_send()


def wait_all(copies):
    for copy in copies:
        copy.wait_recv()


ANY_SPEC = pl.BlockSpec(memory_space=pl.ANY)
VMEM_SPEC = pl.BlockSpec(memory_space=pltpu.VMEM)
QKV_ROWS = 576
OUT_ROWS = 192
SEQ = 512
TOKENS = 2 * SEQ
STEP = 256
NORM_STEP = 128
BLOCK = 256
HEAD = 96
SCALE = HEAD ** -0.5


def head_slice(ref, index, kind, lo, hi, kinds=3):
    head, row = lax.div(index, 2), lax.rem(index, 2)
    start = pl.multiple_of((head * kinds + kind) * HEAD, 32)
    return ref.at[pl.ds(start, HEAD), pl.ds(pl.multiple_of(row * SEQ + lo, 128), hi - lo)]


def dot_cols(lhs, rhs):
    return lax.dot_general(lhs, rhs, (((0,), (0,)), ((), ())), preferred_element_type=F32)


def dot_rows(lhs, rhs):
    return lax.dot_general(lhs, rhs, (((1,), (1,)), ((), ())), preferred_element_type=F32)


def dot_plain(lhs, rhs):
    return lax.dot_general(lhs, rhs, (((1,), (0,)), ((), ())), preferred_element_type=F32)


def probs_block(k_t, q_t, seg, seg_col, row, first):
    keys = first + BLOCK
    scores = dot_cols(k_t, q_t) * SCALE
    query = lax.broadcasted_iota(jnp.int32, (keys, BLOCK), 1) + first
    key = lax.broadcasted_iota(jnp.int32, (keys, BLOCK), 0)
    same = seg[row, :, first : first + BLOCK] == seg_col[row, :keys, :]
    scores = jnp.where((query >= key) & same, scores, NEG_LARGE)
    weights = jnp.exp(scores - jnp.max(scores, axis=0, keepdims=True))
    return weights * (1.0 / jnp.sum(weights, axis=0, keepdims=True))


def attention_forward(qkv, seg, seg_col, out, start, stop):
    @pl.loop(start, stop)
    def _(index):
        row = lax.rem(index, 2)
        for first in range(0, SEQ, BLOCK):
            keys = first + BLOCK
            probs = probs_block(
                head_slice(qkv, index, 1, 0, keys)[...], head_slice(qkv, index, 0, first, keys)[...], seg, seg_col, row, first)
            value = lax.dot_general(
                head_slice(qkv, index, 2, 0, keys)[...], probs.astype(BF16), (((1,), (0,)), ((), ())), preferred_element_type=F32)
            head_slice(out, index, 0, first, keys, kinds=1)[...] = value.astype(BF16)


def attention_backward(qkv, seg, seg_col, grad, out, start, stop):
    @pl.loop(start, stop)
    def _(index):
        row = lax.rem(index, 2)
        grads = []
        for first in range(0, SEQ, BLOCK):
            keys = first + BLOCK
            q_t = head_slice(qkv, index, 0, first, keys)[...]
            k_t = head_slice(qkv, index, 1, 0, keys)[...]
            g_t = head_slice(grad, index, 0, first, keys, kinds=1)[...]
            probs = probs_block(k_t, q_t, seg, seg_col, row, first)
            grad_probs = dot_cols(head_slice(qkv, index, 2, 0, keys)[...], g_t)
            grad_scores = probs * (grad_probs - jnp.sum(grad_probs * probs, axis=0, keepdims=True))
            low = (grad_scores * SCALE).astype(BF16)
            grad_q = lax.dot_general(k_t, low, (((1,), (0,)), ((), ())), preferred_element_type=F32)
            head_slice(out, index, 0, first, keys)[...] = grad_q.astype(BF16)
            grads.append((dot_rows(q_t, low), dot_rows(g_t, probs.astype(BF16))))
        for i in range(2):
            whole = grads[1][i]
            head_slice(out, index, 1 + i, 0, BLOCK)[...] = (grads[0][i] + whole[:, :BLOCK]).astype(BF16)
            head_slice(out, index, 1 + i, BLOCK, SEQ)[...] = whole[:, BLOCK:].astype(BF16)


class Relay:
    COPIES = 6

    def __init__(self, sender, axis, own, up, down, on_up, on_down):
        self.sender, self.axis = sender, axis
        self.on_up, self.on_down = on_up, on_down
        self.ups = [sender.send(axis, 1, own(half), up(half)) for half in range(2)]
        self.downs = [sender.send(axis, 3, own(half), down(half)) for half in range(2)]

    @classmethod
    def at_place(cls, sender, axis, region, own=None):
        place = sender.place
        here = lambda half: region(place.pos[axis], half)
        behind, ahead = region(place.ahead(axis, 3), 0), region(place.ahead(axis, 1), 1)
        return cls(sender, axis, own or here, here, here, (behind, behind), (ahead, ahead))

    def pass_on(self):
        self.ups[0].wait_recv()
        self.passed = [self.sender.send(self.axis, 1, *self.on_up)]
        self.downs[1].wait_recv()
        self.passed.append(self.sender.send(self.axis, 3, *self.on_down))

    def finish(self):
        wait_all([self.ups[1], self.downs[0]] + self.passed)


class WeightGather:
    COPIES = 12 + 3 * Relay.COPIES

    def __init__(self, place, sender, own, out):
        self.place, self.sender, self.own, self.out = place, sender, own, out

    def spot(self, cols):
        z, y = self.place.pos["z"], self.place.pos["y"]
        return lambda step: self.out.at[pl.ds(1, 3), z, y, :, cols]

    def start(self):
        z, y = self.place.pos["z"], self.place.pos["y"]
        self.near = []
        for part in range(2):
            cols = pl.ds(part * THIRD, THIRD)
            self.near.append(self.sender.ring(
                "x", lambda step: self.own.at[z, y, :, cols], lambda step: self.out.at[RING - step, z, y, :, cols]))

    def start_whole(self):
        cols = pl.ds(2 * THIRD, THIRD)
        spot = lambda shard, half: self.out.at[shard, pl.ds(2 * half, 2), :, :, cols]
        self.whole = Relay(
            self.sender, "x", lambda half: self.own.at[pl.ds(2 * half, 2), :, :, cols],
            lambda half: spot(3, half), lambda half: spot(1, half), (spot(3, 0), spot(2, 0)), (spot(1, 1), spot(2, 1)))

    def second(self):
        self.mid = []
        for part, axis in enumerate("yz"):
            wait_all(self.near[part])
            spot = self.spot(pl.ds(part * THIRD, THIRD))
            self.mid.append(self.sender.ring(axis, spot, spot))

    def third(self):
        shards = pl.ds(1, 3)
        wait_all(self.mid[0])
        line = lambda pos, half: self.out.at[shards, pos, pl.ds(2 * half, 2), :, pl.ds(0, THIRD)]
        self.far = [Relay.at_place(self.sender, "z", line)]
        wait_all(self.mid[1])
        row = lambda pos, half: self.out.at[shards, pl.ds(2 * half, 2), pos, :, pl.ds(THIRD, THIRD)]
        self.far.append(Relay.at_place(self.sender, "y", row))

    def pass_on(self):
        for far in self.far:
            far.pass_on()

    def finish(self):
        for far in self.far:
            far.finish()
        self.whole.finish()


def norm_stats(x_f32):
    centered = x_f32 - jnp.mean(x_f32, axis=-1, keepdims=True)
    inv_std = lax.rsqrt(jnp.mean(centered * centered, axis=-1, keepdims=True) + EPS_NORM)
    return centered * inv_std, inv_std


def token_blocks(body):
    @pl.loop(0, TOKENS // NORM_STEP)
    def _(index):
        body(pl.ds(pl.multiple_of(index * NORM_STEP, NORM_STEP), NORM_STEP))


def front_kernel(
    own_att, own_up, own_down, x_in, gain_a, gain_b, seg, seg_col,
    w_att, w_up, w_down, qkv_out, attn_out, normed_a_out, x_one_out, normed_b_out,
    weights, stage, x_one, normed, qkv, attn, part, other, load_sems, send_sems, recv_sems,
):
    place = Place()
    sender = Sender(place, send_sems, recv_sems)

    def copy(source, target, index):
        started = pltpu.make_async_copy(source, target, load_sems.at[index])
        started.start()
        return started

    loads = [copy(x_in, x_one, 0), copy(own_att, weights.at[0], 1), copy(own_up, stage.at[0], 2), copy(own_down, stage.at[1], 3)]
    place.enter(core=True)
    att = WeightGather(place, sender, own_att, w_att)
    mlp = [WeightGather(place, sender, own_up, w_up), WeightGather(place, sender, own_down, w_down)]
    att.start()
    att.start_whole()
    for gather in mlp:
        gather.start()
    loads[0].wait()

    def first_norm(rows):
        x_hat, _ = norm_stats(x_one[rows].astype(F32))
        normed[rows] = (x_hat * gain_a[...].astype(F32)).astype(BF16)

    token_blocks(first_norm)
    results = [copy(normed, normed_a_out, 4)]
    att.second()
    for load in loads[1:]:
        load.wait()
    results += [copy(weights.at[0], w_att.at[0], 5), copy(stage.at[0], w_up.at[0], 6), copy(stage.at[1], w_down.at[0], 7)]

    def project(start, stop):
        @pl.loop(start, stop)
        def _(index):
            block = weights[lax.div(index, 3), lax.rem(index, 3)].reshape(OUT_ROWS, WIDTH)
            qkv[pl.ds(pl.multiple_of(index * OUT_ROWS, OUT_ROWS), OUT_ROWS)] = dot_rows(block, normed[...]).astype(BF16)

    project(0, 3)
    att.third()
    for gather in mlp:
        gather.second()
    att.whole.pass_on()
    for gather in mlp:
        gather.start_whole()
    att.pass_on()
    att.finish()
    others = [copy(w_att.at[shard], weights.at[shard], 7 + shard) for shard in range(1, RING)]
    for load in others:
        load.wait()
    project(3, 12)
    results.append(copy(qkv, qkv_out, 11))
    for gather in mlp:
        gather.third()
    attention_forward(qkv, seg, seg_col, attn, 0, 10)
    mlp[0].whole.pass_on()
    mlp[0].pass_on()
    attention_forward(qkv, seg, seg_col, attn, 10, 16)
    mlp[1].whole.pass_on()
    mlp[1].pass_on()
    results.append(copy(attn, attn_out, 12))
    swaps = []
    for index in range(TOKENS // STEP):
        rows = pl.ds(index * STEP, STEP)
        total = None
        for shard in range(RING):
            block = weights[shard, 3].reshape(OUT_ROWS, WIDTH)
            term = dot_cols(attn[shard * OUT_ROWS : (shard + 1) * OUT_ROWS, index * STEP : (index + 1) * STEP], block)
            total = term if total is None else total + term
        part[rows] = total.astype(BF16)
        swaps.append(sender.swap(part.at[rows], other.at[rows]))
    results[0].wait()
    wait_all(swaps)

    def second_norm(rows):
        summed = (part[rows].astype(F32) + other[rows].astype(F32)).astype(BF16)
        x_new = (x_one[rows].astype(F32) + summed.astype(F32)).astype(BF16)
        x_one[rows] = x_new
        x_hat, _ = norm_stats(x_new.astype(F32))
        normed[rows] = (x_hat * gain_b[...].astype(F32)).astype(BF16)

    token_blocks(second_norm)
    results += [copy(x_one, x_one_out, 13), copy(normed, normed_b_out, 14)]
    for gather in mlp:
        gather.finish()
    for result in results[1:]:
        result.wait()
    for swap in swaps:
        swap.wait_send()
    sender.drain()


def front(own_att, own_up, own_down, x_rows, gain_a, gain_b, seg, seg_col):
    tokens = (TOKENS, WIDTH)
    gathered = jax.ShapeDtypeStruct((RING,) + own_att.shape, BF16)
    rows = jax.ShapeDtypeStruct(tokens, BF16)
    copies = 3 * WeightGather.COPIES + TOKENS // STEP
    return pl.pallas_call(
        front_kernel,
        out_shape=[
            gathered, gathered, gathered,
            jax.ShapeDtypeStruct((RING * QKV_ROWS, TOKENS), BF16), jax.ShapeDtypeStruct((RING * OUT_ROWS, TOKENS), BF16),
            rows, rows, rows,
        ],
        in_specs=[ANY_SPEC] * 4 + [VMEM_SPEC] * 4,
        out_specs=[ANY_SPEC] * 8,
        scratch_shapes=[
            pltpu.VMEM(gathered.shape, BF16),
            pltpu.VMEM((2,) + own_att.shape, BF16),
            pltpu.VMEM(tokens, BF16),
            pltpu.VMEM(tokens, BF16),
            pltpu.VMEM((RING * QKV_ROWS, TOKENS), BF16),
            pltpu.VMEM((RING * OUT_ROWS, TOKENS), BF16),
            pltpu.VMEM(tokens, BF16),
            pltpu.VMEM(tokens, BF16),
            pltpu.SemaphoreType.DMA((15,)),
            pltpu.SemaphoreType.DMA((copies,)),
            pltpu.SemaphoreType.DMA((copies,)),
        ],
        compiler_params=pltpu.CompilerParams(collective_id=1, has_side_effects=True, vmem_limit_bytes=56 << 20),
        name="front",
    )(own_att, own_up, own_down, x_rows, gain_a, gain_b, seg, seg_col)


ORDERS = (("z", "y", "x", 1), ("y", "x", "z", 0), ("x", "z", "y", 0))


class GradScatter:
    def __init__(self, place, sender, grads, widths, bufs, final, local_sems):
        self.place, self.sender, self.grads = place, sender, grads
        self.bufs, self.final, self.local_sems = bufs, final, local_sems
        self.parts = range(len(widths))
        self.cols = [(sum(widths[:part]), widths[part]) for part in self.parts]

    @staticmethod
    def scratch(widths):
        shapes = []
        for width in widths:
            shapes += [
                pltpu.VMEM((RING, RING, PIECE, width), BF16),
                pltpu.VMEM((3, RING, RING, PIECE, width), BF16),
                pltpu.VMEM((RING, RING, PIECE, width), BF16),
                pltpu.VMEM((3, PIECE, width), BF16),
            ]
        return shapes

    def cut(self, part, step, half=None):
        axis = ORDERS[part][0]
        index = self.place.block(axis, step)
        cols = pl.ds(*self.cols[part])
        lead = pl.ds(0, RING) if half is None else pl.ds(2 * half, 2)
        if axis == "x":
            return self.grads.at[index, lead, :, :, cols]
        if axis == "z":
            return self.grads.at[lead, index, :, :, cols]
        return self.grads.at[lead, :, index, :, cols]

    def load(self, source, target, index):
        copy = pltpu.make_async_copy(source, target, self.local_sems.at[index])
        copy.start()
        return copy

    def start(self):
        self.loads, self.far, self.raw, self.sums, self.two, self.three = [], [], [], [], {}, {}
        low, high = pl.ds(0, 2), pl.ds(2, 2)
        for part in self.parts:
            axis, first = ORDERS[part][0], self.bufs[part][1]
            self.far.append([
                self.sender.send(axis, 1, self.cut(part, 2, 0), first.at[1, low]),
                self.sender.send(axis, 3, self.cut(part, 2, 1), first.at[1, high])])
        for part in self.parts:
            axis, first = ORDERS[part][0], self.bufs[part][1]
            self.raw.append([
                self.sender.send(axis, 1, self.cut(part, 1, 1), first.at[0, high]),
                self.sender.send(axis, 3, self.cut(part, 3, 0), first.at[2, low])])
        for part in self.parts:
            mine = self.bufs[part][0]
            self.loads.append([
                self.load(self.cut(part, 1, 0), mine.at[low], part), self.load(self.cut(part, 3, 1), mine.at[high], 4 + part)])

    def relay(self):
        low, high = pl.ds(0, 2), pl.ds(2, 2)
        for part in self.parts:
            for load in self.loads[part]:
                load.wait()
            wait_all(self.far[part])
            axis, mine, first = ORDERS[part][0], self.bufs[part][0], self.bufs[part][1]

            @pl.loop(0, RING)
            def _(a):
                for b in range(RING):
                    mine[a, b] = (mine[a, b].astype(F32) + first[1, a, b].astype(F32)).astype(BF16)

            self.sums.append([
                self.sender.send(axis, 1, mine.at[low], first.at[0, low]),
                self.sender.send(axis, 3, mine.at[high], first.at[2, high])])

    def second(self):
        own = []
        for part in self.parts:
            self.sender.settle(self.sums[part])
            own.append(self.load(self.cut(part, 0), self.bufs[part][0], part))
        for part in self.parts:
            own[part].wait()
            wait_all(self.raw[part] + self.sums[part])
            mine, first, second, _ = self.bufs[part]

            @pl.loop(0, RING)
            def _(a):
                for b in range(RING):
                    total = mine[a, b].astype(F32)
                    for k in (0, 2):
                        total = total + first[k, a, b].astype(F32)
                    mine[a, b] = total.astype(BF16)

            axis, spot = ORDERS[part][1], ORDERS[part][3]

            def source(step):
                index = self.place.block(axis, step)
                return mine.at[:, index] if spot else mine.at[index]

            self.two[part] = self.sender.ring(axis, source, lambda step: second.at[step - 1])

    def third(self):
        for part in self.parts:
            wait_all(self.two[part])
            mine, _, second, third = self.bufs[part]
            axis, spot = ORDERS[part][1], ORDERS[part][3]
            own = self.place.block(axis, 0)
            for other in range(RING):
                total = mine[(other, own) if spot else (own, other)].astype(F32)
                for k in range(3):
                    total = total + second[k, other].astype(F32)
                second[3, other] = total.astype(BF16)
            axis = ORDERS[part][2]
            self.three[part] = self.sender.ring(
                axis, lambda step: second.at[3, self.place.block(axis, step)], lambda step: third.at[step - 1])

    def finish(self):
        for part in self.parts:
            wait_all(self.three[part])
            _, _, second, third = self.bufs[part]
            total = second[3, self.place.block(ORDERS[part][2], 0)].astype(F32)
            for k in range(3):
                total = total + third[k].astype(F32)
            start, width = self.cols[part]
            self.final[:, start : start + width] = total.astype(BF16)


class PlaneGather:
    COPIES = 6 + 2 * Relay.COPIES

    def __init__(self, place, sender, final, out, local_sem):
        self.place, self.sender, self.final, self.out, self.local_sem = place, sender, final, out, local_sem

    def start(self):
        z, y = self.place.pos["z"], self.place.pos["y"]
        self.store = pltpu.make_async_copy(self.final, self.out.at[z, y], self.local_sem)
        self.store.start()
        self.near = []
        for part, axis in enumerate("yz"):
            cols = pl.ds(part * HALF, HALF)
            self.near.append(self.sender.ring(
                axis, lambda step: self.final.at[:, cols], lambda step: self.out.at[z, y, :, cols]))

    def second(self):
        self.store.wait()
        wait_all(self.near[0])
        line = lambda pos, half: self.out.at[pos, pl.ds(2 * half, 2), :, pl.ds(0, HALF)]
        self.far = [Relay.at_place(self.sender, "z", line)]
        wait_all(self.near[1])
        row = lambda pos, half: self.out.at[pl.ds(2 * half, 2), pos, :, pl.ds(HALF, HALF)]
        self.far.append(Relay.at_place(self.sender, "y", row))

    def pass_on(self):
        for far in self.far:
            far.pass_on()

    def finish(self):
        for far in self.far:
            far.finish()


def gain_step(place, sender, gains, bufs, index, axis):
    copies = sender.ring(axis, lambda step: gains.at[index], lambda step: bufs.at[index, step - 1])

    def finish():
        wait_all(copies)
        gains[index + 1] = (gains[index] + bufs[index, 1]) + (bufs[index, 0] + bufs[index, 2])

    return finish


def grad_works(place, sender, grads, widths, bufs, finals, outs, local_sems):
    parts = len(widths)
    works, planes = [], []
    for i, grad in enumerate(grads):
        mine = bufs[4 * parts * i : 4 * parts * (i + 1)]
        mine = [mine[4 * part : 4 * part + 4] for part in range(parts)]
        works.append(GradScatter(place, sender, grad, widths, mine, finals.at[i], local_sems.at[i]))
        planes.append(PlaneGather(place, sender, finals.at[i], outs[i], local_sems.at[i, 3]))
    return works, planes


WIDTHS = (640, 640, 256)


def back_kernel(
    hidden_act, grad_pre, grad_y, normed_b_in, part_b, x_one_in, qkv_in, seg, seg_col, attn, w_att, normed_a_in, x_in, gain_a, gain_b,
    out_up, out_down, out_att, grad_up, grad_down, grad_att, grad_x, gain_out,
    lhs, qkv, grad_attn, grad_one, normed, w_qkv, w_out, part, other, stage, load_sems, lhs_sems, stage_sems, free_sem, ring_sem,
    gain_grad_a, gain_grad_b, gains, gain_bufs, finals, send_sems, recv_sems, local_sems, *bufs,
):
    place = Place()
    sender = Sender(place, send_sems, recv_sems)
    loads = {}

    def load(name, source, target, index):
        copy = pltpu.make_async_copy(source, target, load_sems.at[index])
        copy.start()
        loads.setdefault(name, []).append(copy)

    def ready(name):
        for copy in loads[name]:
            copy.wait()

    load("one", grad_y, grad_one, 0)
    load("part", part_b, part, 13)
    load("normed_b", normed_b_in, normed, 6)
    load("qkv", qkv_in, qkv, 5)
    for shard in range(RING):
        load("out", w_att.at[shard, pl.ds(QKV_ROWS, OUT_ROWS)], w_out.at[pl.ds(shard * OUT_ROWS, OUT_ROWS)], 1 + shard)
    for shard in range(RING):
        load("w", w_att.at[shard, pl.ds(0, QKV_ROWS)], w_qkv.at[pl.ds(shard * QKV_ROWS, QKV_ROWS)], 7 + shard)
    place.enter(core=True)
    works, planes = grad_works(place, sender, [grad_down, grad_up], WIDTHS, bufs, finals, [out_down, out_up], local_sems)
    tail = bufs[8 * len(WIDTHS) :]
    reused = [(works[0].bufs[part][0], works[0].bufs[part][1]) + tuple(tail[2 * part : 2 * part + 2]) for part in range(len(WIDTHS))]
    att_work = GradScatter(place, sender, grad_att, WIDTHS, reused, finals.at[2], local_sems.at[2])
    att_plane = PlaneGather(place, sender, finals.at[2], out_att, local_sems.at[2, 3])
    ready("part")
    early = sender.swap(part, other)

    blocks = RING * RING

    def fetch(source, index, slot):
        rows = pl.ds(pl.multiple_of(index * OUT_ROWS, OUT_ROWS), OUT_ROWS)
        return pltpu.make_async_copy(source.at[rows], lhs.at[slot], lhs_sems.at[slot])

    def place_block(target, index, slot):
        return pltpu.make_async_copy(stage.at[slot], target.at[lax.div(index, RING), lax.rem(index, RING)], stage_sems.at[slot])

    def weight_grad(source, rhs, target):
        fetch(source, 0, 0).start()

        @pl.loop(0, blocks)
        def _(index):
            slot = lax.rem(index, 2)
            fetch(source, index, slot).wait()

            @pl.when(index + 1 < blocks)
            def _():
                fetch(source, index + 1, 1 - slot).start()

            @pl.when(index >= 2)
            def _():
                place_block(target, index - 2, slot).wait()

            stage[slot] = dot_plain(lhs[slot], rhs[...]).astype(BF16).reshape(RING, PIECE, WIDTH)
            place_block(target, index, slot).start()

        for index in (blocks - 2, blocks - 1):
            place_block(target, index, index % 2).wait()

    ready("one")
    weight_grad(hidden_act, grad_one, grad_down)
    works[0].start()
    ready("normed_b")
    weight_grad(grad_pre, normed, grad_up)
    works[0].relay()
    works[1].start()

    load("x_one", x_one_in, normed, 14)
    gain_grad_a[...] = jnp.zeros_like(gain_grad_a)
    gain_grad_b[...] = jnp.zeros_like(gain_grad_b)
    early.wait_recv()
    early.wait_send()
    ready("x_one")

    def norm_back(rows, gain, gain_grad):
        x_hat, inv_std = norm_stats(normed[rows].astype(F32))
        grad = (part[rows].astype(F32) + other[rows].astype(F32)).astype(BF16).astype(F32)
        gain_grad[...] += jnp.sum(grad * x_hat, axis=0, keepdims=True)
        grad_hat = grad * gain[...].astype(F32)
        mean_one = jnp.mean(grad_hat, axis=-1, keepdims=True)
        mean_two = jnp.mean(grad_hat * x_hat, axis=-1, keepdims=True)
        back = inv_std * (grad_hat - mean_one - x_hat * mean_two)
        return (grad_one[rows].astype(F32) + back).astype(BF16)

    def second_norm(rows):
        grad_one[rows] = norm_back(rows, gain_b, gain_grad_b)

    token_blocks(second_norm)
    pl.semaphore_signal(free_sem, inc=1, device_id=place.sibling(), device_id_type=MESH_ID)
    load("normed_a", normed_a_in, normed, 11)

    ready("out")
    for shard in range(RING):
        rows = pl.ds(shard * OUT_ROWS, OUT_ROWS)
        grad_attn[rows] = dot_rows(w_out[rows], grad_one[...]).astype(BF16)
    ready("qkv")
    attention_backward(qkv, seg, seg_col, grad_attn, qkv, 0, 6)
    works[1].relay()
    attention_backward(qkv, seg, seg_col, grad_attn, qkv, 6, 10)
    works[0].second()
    place.signal_rings(ring_sem)
    attention_backward(qkv, seg, seg_col, grad_attn, qkv, 10, 16)

    ready("w")
    pl.semaphore_wait(free_sem, 1)
    swaps = []
    for index in range(TOKENS // STEP):
        rows = pl.ds(index * STEP, STEP)
        part[rows] = dot_cols(qkv[:, index * STEP : (index + 1) * STEP], w_qkv[...]).astype(BF16)
        swaps.append(sender.swap(part.at[rows], other.at[rows]))
    works[1].second()
    works[0].third()

    stores = []

    def put(rows, shard, start):
        slot = len(stores) % 2
        if len(stores) >= 2:
            stores[-2].wait()
        stage[slot] = rows.astype(BF16).reshape(RING, PIECE, WIDTH)
        copy = pltpu.make_async_copy(stage.at[slot], grad_att.at[shard, start // OUT_ROWS], stage_sems.at[slot])
        copy.start()
        stores.append(copy)

    for shard in range(RING):
        put(dot_plain(attn[shard * OUT_ROWS : (shard + 1) * OUT_ROWS], grad_one[...]), shard, QKV_ROWS)
    ready("normed_a")
    for shard in range(RING):
        for block in range(3):
            start = shard * QKV_ROWS + block * OUT_ROWS
            put(dot_plain(qkv[start : start + OUT_ROWS], normed[...]), shard, block * OUT_ROWS)
    for store in stores[-2:]:
        store.wait()
    load("x", x_in, normed, 15)
    sender.settle([copy for copies in works[0].two.values() for copy in copies])
    pl.semaphore_wait(ring_sem, 9)
    att_work.start()
    works[1].third()
    ready("x")
    wait_all(swaps)
    for copy in swaps:
        copy.wait_send()

    def first_norm(rows):
        part[rows] = norm_back(rows, gain_a, gain_grad_a)

    token_blocks(first_norm)
    row_of = lambda pos: 2 * pos + place.core
    part_rows = SEQ // 2
    mine = lambda half: part.at[pl.ds(pl.multiple_of(place.core * SEQ + half * part_rows, part_rows), part_rows)]
    rows_sent = Relay.at_place(sender, "x", lambda pos, half: grad_x.at[row_of(pos), pl.ds(half * part_rows, part_rows)], mine)
    results = []
    for i in range(2):
        result = pltpu.make_async_copy(part.at[pl.ds(i * SEQ, SEQ)], grad_x.at[2 * place.pos["x"] + i], load_sems.at[12 + 4 * i])
        result.start()
        results.append(result)
    gains[0] = jnp.zeros_like(gain_out)
    gains[0, 0:1] = gain_grad_a[...]
    gains[0, 1:2] = gain_grad_b[...]
    gain_finish = gain_step(place, sender, gains, gain_bufs, 0, "z")
    att_work.relay()
    for work, plane in zip(works, planes):
        work.finish()
        plane.start()
    gain_finish()
    gain_finish = gain_step(place, sender, gains, gain_bufs, 1, "y")
    att_work.second()
    for plane in planes:
        plane.second()
    gain_finish()
    gain_finish = gain_step(place, sender, gains, gain_bufs, 2, "x")
    rows_sent.pass_on()
    att_work.third()
    for plane in planes:
        plane.pass_on()
    att_work.finish()
    att_plane.start()
    rows_sent.finish()
    passed = []
    for step in range(1, RING):
        row = grad_x.at[row_of(place.ahead("x", step))]
        passed.append(sender.swap(row, row))
    gain_finish()
    gain_out[...] = gains[3]
    for plane in planes:
        plane.finish()
    att_plane.second()
    att_plane.pass_on()
    att_plane.finish()
    wait_all(passed)
    for copy in passed:
        copy.wait_send()
    for result in results:
        result.wait()
    sender.drain()


def backward(*operands):
    tokens = (TOKENS, WIDTH)
    piece = jax.ShapeDtypeStruct((RING, RING, PIECE, WIDTH), BF16)
    grid = jax.ShapeDtypeStruct((RING, RING, RING, PIECE, WIDTH), BF16)
    copies = 3 * (12 * len(WIDTHS) + PlaneGather.COPIES) + TOKENS // STEP + 1 + 9 + Relay.COPIES + 3
    tail = [shape for part in range(len(WIDTHS)) for shape in GradScatter.scratch(WIDTHS)[4 * part + 2 : 4 * part + 4]]
    return pl.pallas_call(
        back_kernel,
        out_shape=[
            piece, piece, piece, grid, grid, grid,
            jax.ShapeDtypeStruct((2 * RING, SEQ, WIDTH), BF16),
            jax.ShapeDtypeStruct((8, WIDTH), F32),
        ],
        in_specs=[ANY_SPEC] * 7 + [VMEM_SPEC] * 3 + [ANY_SPEC] * 3 + [VMEM_SPEC] * 2,
        out_specs=[ANY_SPEC] * 7 + [VMEM_SPEC],
        scratch_shapes=[
            pltpu.VMEM((2, OUT_ROWS, TOKENS), BF16),
            pltpu.VMEM((RING * QKV_ROWS, TOKENS), BF16),
            pltpu.VMEM((RING * OUT_ROWS, TOKENS), BF16),
            pltpu.VMEM(tokens, BF16),
            pltpu.VMEM(tokens, BF16),
            pltpu.VMEM((RING * QKV_ROWS, WIDTH), BF16),
            pltpu.VMEM((RING * OUT_ROWS, WIDTH), BF16),
            pltpu.VMEM(tokens, BF16),
            pltpu.VMEM(tokens, BF16),
            pltpu.VMEM((2, RING, PIECE, WIDTH), BF16),
            pltpu.SemaphoreType.DMA((17,)),
            pltpu.SemaphoreType.DMA((2,)),
            pltpu.SemaphoreType.DMA((2,)),
            pltpu.SemaphoreType.REGULAR,
            pltpu.SemaphoreType.REGULAR,
            pltpu.VMEM((1, WIDTH), F32),
            pltpu.VMEM((1, WIDTH), F32),
            pltpu.VMEM((4, 8, WIDTH), F32),
            pltpu.VMEM((3, 3, 8, WIDTH), F32),
            pltpu.VMEM((3, PIECE, WIDTH), BF16),
            pltpu.SemaphoreType.DMA((copies,)),
            pltpu.SemaphoreType.DMA((copies,)),
            pltpu.SemaphoreType.DMA((3, 8)),
        ] + GradScatter.scratch(WIDTHS) + GradScatter.scratch(WIDTHS) + tail,
        compiler_params=pltpu.CompilerParams(collective_id=3, has_side_effects=True, vmem_limit_bytes=67043328),
        name="backward",
    )(*operands)


def solution(mesh):
    batch_spec = P(("pod", "dp"), None, None)
    seg_spec = P(("pod", "dp"), None)

    def local_step(x_in, seg_ids, gain_one, gain_two, w_qkv, w_out, w_up, w_down, grad_y):
        batch_loc, seq_len, hidden = x_in.shape
        heads_loc, head_dim = w_out.shape[:2]
        rows_loc = batch_loc // RING
        tokens = rows_loc * seq_len
        shard_rows = w_up.shape[1]
        qkv_cols = w_qkv.shape[1]
        x_pos = lax.axis_index("tp") // 2

        def own_rows(array):
            return lax.dynamic_slice_in_dim(array, x_pos * rows_loc, rows_loc, axis=0)

        def grid_of(own):
            return own.reshape(RING, RING, PIECE, hidden)

        own_att = grid_of(jnp.concatenate([w_qkv.T, w_out.reshape(heads_loc * head_dim, hidden)], axis=0))
        own_up = grid_of(w_up.T)
        own_down = grid_of(w_down)
        x_rows = own_rows(x_in).reshape(tokens, hidden)
        seg_rows = own_rows(seg_ids)
        seg_row, seg_col = seg_rows[:, None, :], seg_rows[:, :, None]
        grad_rows = own_rows(grad_y).reshape(tokens, hidden)
        w_att, up_t, down, qkv_t, attn_flat, normed_a, x_one, normed_b = front(
            own_att, own_up, own_down, x_rows, gain_one[None], gain_two[None], seg_row, seg_col)
        up_t = up_t.reshape(RING * shard_rows, hidden)
        down = down.reshape(RING * shard_rows, hidden)

        def pair_sum(part):
            return part.astype(F32) + core_swap(part).astype(F32)

        pre_act = dot_nt(up_t, normed_b)
        act_val, gelu_pull = jax.vjp(gelu_tanh, pre_act)
        hidden_act = act_val.astype(BF16)
        part_two = dot_tn(hidden_act, down).astype(BF16)
        sum_two = pair_sum(part_two).astype(BF16)
        y_rows = (x_one.astype(F32) + sum_two.astype(F32)).astype(BF16)

        grad_hidden = dot_nt(down, grad_rows).astype(BF16)
        grad_pre = gelu_pull(grad_hidden.astype(F32))[0].astype(BF16)

        part_b = dot_tn(grad_pre, up_t).astype(BF16)
        part_b, y_rows = lax.optimization_barrier((part_b, y_rows))
        grad_up_own, grad_down_own, grad_att_own, _, _, _, grad_x, gains = backward(
            hidden_act, grad_pre, grad_rows, normed_b, part_b, x_one, qkv_t, seg_row, seg_col, attn_flat,
            w_att.reshape(RING, shard_rows, hidden), normed_a, x_rows, gain_one[None], gain_two[None])
        grad_att_own = grad_att_own.reshape(shard_rows, hidden)

        def spread(rows):
            core = lax.axis_index("tp") % 2
            mine = lax.dynamic_slice_in_dim(rows.reshape(rows_loc, seq_len, hidden), core, 1, axis=0)
            return lax.all_gather(mine, "tp", axis=0, tiled=True)

        return (
            spread(y_rows),
            grad_x,
            gains[0].astype(BF16),
            gains[1].astype(BF16),
            grad_att_own[:qkv_cols].T,
            grad_att_own[qkv_cols:].reshape(heads_loc, head_dim, hidden),
            grad_up_own.reshape(shard_rows, hidden).T,
            grad_down_own.reshape(shard_rows, hidden),
        )

    return jax.shard_map(
        local_step,
        mesh=mesh,
        in_specs=(batch_spec, seg_spec, P(None), P(None), P(None, "tp"), P("tp", None, None), P(None, "tp"), P("tp", None), batch_spec),
        out_specs=(batch_spec, batch_spec, P("pod"), P("pod"), P("pod", "tp"), P(("pod", "tp"), None, None), P("pod", "tp"), P(("pod", "tp"), None)),
        check_vma=False,
    )
```
